16 devices in a mesh: dp: 2 (over y, z), tp: 8 (over x, core).
Axes of the slice: x: 4, y: 2, z: 1, core: 2. Of those that a mesh axis runs over, the one named last changes fastest.
The devices are a block of a 4x4x8 slice.
Arguments:
- hidden: bfloat16 [512, 3, 4096], P(('dp', 'tp')), parts along dimension 0
- w_head: bfloat16 [4096, 32000], P(None, 'tp')
- q_draft: float32 [512, 2, 32000], P(('dp', 'tp')), parts along dimension 0
- draft_tok: int32 [512, 2], P('dp'), parts along dimension 0
Outputs:
- output 1: float32 [512, 2], P('dp'), parts along dimension 0
- output 2: float32 [512], P('dp'), parts along dimension 0
- output 3: float32 [512, 2, 32000], P('dp', None, 'tp'), parts along dimension 0
- output 4: float32 [512, 32000], P('dp', 'tp'), parts along dimension 0
There are 2 independent parts. The reference program is written for one: setup_inputs(seed, part) draws one part's arguments, and reference() takes and returns one part's arrays. A program takes and returns all parts, laid end to end along the dimension named above; an argument that names none is the same for every part.
All inputs are finite; a program needn't handle non-finite values.
Results may differ from the reference program's by a relative error of at most 0.001.
Values are sent between devices in bfloat16 or wider.
A program may use at most 768 MiB of HBM per device.

```python
import jax
import jax.numpy as jnp

SEQ_DEV = 32
GROUP_SIZE = 8
DRAFT_LEN = 2
MODEL_DIM = 4096
VOCAB_SIZE = 32000
BATCH = SEQ_DEV * GROUP_SIZE
INV_TEMP = 1.25
HEAD_SCALE = MODEL_DIM ** -0.5


def setup_inputs(seed: int = 0, part: int = 0) -> dict:
    part_key = jax.random.fold_in(jax.random.key(seed), part)
    key_hid, key_noise, key_tok = jax.random.split(part_key, 3)
    key_head = jax.random.key(seed + 1)
    hidden = jax.random.normal(key_hid, (BATCH, DRAFT_LEN + 1, MODEL_DIM), jnp.float32).astype(jnp.bfloat16)
    w_head = (jax.random.normal(key_head, (MODEL_DIM, VOCAB_SIZE), jnp.float32) * HEAD_SCALE).astype(jnp.bfloat16)
    target = jnp.dot(hidden[:, :DRAFT_LEN].reshape(BATCH * DRAFT_LEN, MODEL_DIM), w_head, preferred_element_type=jnp.float32)
    target = target.reshape(BATCH, DRAFT_LEN, VOCAB_SIZE) * INV_TEMP
    draft_noise = jax.random.normal(key_noise, (BATCH, DRAFT_LEN, VOCAB_SIZE), jnp.float32)
    q_draft = jax.nn.softmax(0.8 * target + 0.6 * draft_noise, axis=-1)
    draft_tok = jax.random.randint(key_tok, (BATCH, DRAFT_LEN), 0, VOCAB_SIZE, jnp.int32)
    draft_tok = draft_tok.at[0, 0].set(0).at[BATCH - 1, DRAFT_LEN - 1].set(VOCAB_SIZE - 1)
    return {'hidden': hidden, 'w_head': w_head, 'q_draft': q_draft, 'draft_tok': draft_tok}


def reference(hidden, w_head, q_draft, draft_tok):
    logits = jnp.dot(hidden.reshape(BATCH * (DRAFT_LEN + 1), MODEL_DIM), w_head, preferred_element_type=jnp.float32)
    logits = logits.reshape(BATCH, DRAFT_LEN + 1, VOCAB_SIZE) * INV_TEMP
    target_prob = jax.nn.softmax(logits, axis=-1)
    draft_part = target_prob[:, :DRAFT_LEN]
    p_pick = jnp.take_along_axis(draft_part, draft_tok[:, :, None], axis=2)[:, :, 0]
    q_pick = jnp.take_along_axis(q_draft, draft_tok[:, :, None], axis=2)[:, :, 0]
    accept = jnp.minimum(p_pick / q_pick, 1.0)
    expected = jnp.sum(jnp.cumprod(accept, axis=1), axis=1)
    excess = jnp.maximum(draft_part - q_draft, 0.0)
    residual = excess / jnp.sum(excess, axis=-1, keepdims=True)
    return accept, expected, residual, target_prob[:, DRAFT_LEN]
```

```python
import functools

import jax
import jax.numpy as jnp
from jax import lax
from jax.experimental import pallas as pl
from jax.experimental.pallas import tpu as pltpu
from jax.experimental.layout import Layout, with_layout_constraint
from jax.sharding import PartitionSpec as P

INV_TEMP = 1.25
TOP = 65535.0
HALF = 32768
LANES = 128
SEGS = 4
STEPS = 10
F32 = jnp.float32
MESH = pl.DeviceIdType.MESH


def kernel(
    n, tok_ref, hid_ref, w_ref, q_ref,
    ex_ref, bonus_ref, small_ref,
    hall, z, stage, scode, qall, rbuf, wbuf, msgs, mass, rowc,
    h_send, h_fwd, h_recv, q_send, q_recv, r_send, r_recv,
    m_send, m_recv, x_send, x_recv, loc, wsem, osem,
):
    k = lax.axis_index("tp")
    x, c = k // 2, k % 2
    chips = n // 2
    right, left = (x + 1) % chips, (x + chips - 1) % chips
    far = (x + 2) % chips
    mate = 2 * x + 1 - c
    positions, batch, dim = hall.shape
    drafts = positions - 1
    rows = batch // n
    vocab = w_ref.shape[0]
    width = qall.shape[2]
    seg = width // SEGS
    tiles = width // LANES
    pitch = q_ref.shape[0] // rows
    all_tiles = pitch // drafts
    off = (k * vocab) % LANES
    hcol = dim // 2
    wrows = vocab // STEPS

    def remote(src, dst, ssem, rsem, who):
        return pltpu.make_async_remote_copy(
            src_ref=src, dst_ref=dst, send_sem=ssem, recv_sem=rsem,
            device_id={"tp": who}, device_id_type=MESH,
        )

    hid_cp = pltpu.make_async_copy(hid_ref, hall.at[:, pl.ds(k * rows, rows), :], loc.at[0])
    hid_cp.start()

    def stage_cp(g):
        part = pl.ds(g * 8 * pitch, 8 * pitch)
        return pltpu.make_async_copy(q_ref.at[part], stage.at[part], loc.at[1 + g])

    for g in range(rows // 8):
        stage_cp(g).start()

    def w_cp(t, slot):
        return pltpu.make_async_copy(
            w_ref.at[pl.ds(pl.multiple_of(t * wrows, 8), wrows)], wbuf.at[slot], wsem.at[slot]
        )

    barrier = pltpu.get_barrier_semaphore()
    for p in range(1, n):
        pl.semaphore_signal(barrier, inc=1, device_id={"tp": (k + p) % n}, device_id_type=MESH)
    pl.semaphore_wait(barrier, n - 1)

    def hpiece(src, half):
        return hall.at[:, pl.ds(pl.multiple_of(src * rows, rows), rows), pl.ds(half * hcol, hcol)]

    def hcopy(src, half, ssem, who):
        return remote(hpiece(src, half), hpiece(src, half), ssem, h_recv.at[src * 2 + half], who)

    def hwait(src, half):
        hcopy(src, half, h_send.at[0], mate).wait_recv()

    hid_cp.wait()
    own_sends = []
    for idx, (who, half) in enumerate(
        [(2 * right + c, 0), (2 * left + c, 1), (2 * right + c, 1), (2 * left + c, 0), (mate, 0), (mate, 1)]
    ):
        cp = hcopy(k, half, h_send.at[idx], who)
        cp.start()
        own_sends.append(cp)
    w_cp(0, 0).start()
    w_cp(1, 1).start()

    z[:, 0:96, :] = jnp.zeros((positions, 96, batch), F32)
    z[:, width - 96:width, :] = jnp.zeros((positions, 96, batch), F32)

    for g in range(rows // 8):
        stage_cp(g).wait()

    def qrows(g, i, j):
        return stage[pl.ds(g * 8 * pitch + drafts * j + i, 8, stride=pitch), :]

    groups = [(i, g) for i in range(drafts) for g in range(rows // 8)]
    lane_b = lax.broadcasted_iota(jnp.int32, (8, batch), 1)
    sub_b = lax.broadcasted_iota(jnp.int32, (8, batch), 0)
    lane_t = lax.broadcasted_iota(jnp.int32, (8, LANES), 1)
    mine = [lane_b == k * rows + 8 * g + sub_b for g in range(rows // 8)]
    tok_col = []
    for i, g in groups:
        t = jnp.where(mine[g], jnp.broadcast_to(tok_ref[i:i + 1, :].astype(F32), (8, batch)), 0.0)
        tok_col.append(jnp.broadcast_to(jnp.sum(t, axis=1, keepdims=True), (8, LANES)).astype(jnp.int32))

    def scan(j, carry):
        top, got = carry
        new_top, new_got = [], []
        col = lane_t + j * LANES
        for a, (i, g) in enumerate(groups):
            v = qrows(g, i, j)
            new_top.append(jnp.maximum(top[a], v))
            new_got.append(jnp.where(col == tok_col[a], v, got[a]))
        return tuple(new_top), tuple(new_got)

    zero8 = tuple(jnp.zeros((8, LANES), F32) for _ in groups)
    top, got = lax.fori_loop(0, all_tiles, scan, (zero8, zero8))
    qtop_row, qgot_row = [], []
    for i in range(drafts):
        acc_t = jnp.zeros((8, batch), F32)
        acc_g = jnp.zeros((8, batch), F32)
        for a, (ii, g) in enumerate(groups):
            if ii != i:
                continue
            tcol = jnp.max(top[a], axis=1, keepdims=True)
            gcol = jnp.sum(got[a], axis=1, keepdims=True)
            rowc[a] = jnp.broadcast_to(jnp.log(TOP) - 0.25 * jnp.log(tcol), (8, LANES))
            acc_t = acc_t + jnp.where(mine[g], jnp.broadcast_to(tcol, (8, batch)), 0.0)
            acc_g = acc_g + jnp.where(mine[g], jnp.broadcast_to(gcol, (8, batch)), 0.0)
        qtop_row.append(jnp.sum(acc_t, axis=0, keepdims=True))
        qgot_row.append(jnp.sum(acc_g, axis=0, keepdims=True))
    msgs[k] = jnp.zeros(msgs.shape[1:], F32)
    for i in range(drafts):
        msgs[k, 8 + i:9 + i, :] = qgot_row[i]
        msgs[k, 10 + i:11 + i, :] = qtop_row[i]

    def encode(dest, put):
        first = (dest * vocab) // LANES

        def body(j, _):
            for i in range(drafts):
                for gg in range(rows // 16):
                    parts = []
                    for g in (2 * gg, 2 * gg + 1):
                        v = qrows(g, i, first + j)
                        y = jnp.exp(0.25 * jnp.log(v) + rowc[i * (rows // 8) + g])
                        parts.append((y + 0.5).astype(jnp.int32) - HALF)
                    code = jnp.concatenate(parts, axis=0).astype(jnp.int16)
                    put(i, gg, pl.ds(pl.multiple_of(j * LANES, LANES), LANES), code)
            return 0

        lax.fori_loop(0, tiles, body, 0)

    def to_slot(r):
        def put(i, gg, cols, code):
            scode[r, i, 16 * gg:16 * gg + 16, cols] = code

        return put

    def to_self(i, gg, cols, code):
        qall[i, pl.ds(pl.multiple_of(k * rows + 16 * gg, 16), 16), cols] = code

    encode(2 * far, to_slot(0))
    encode(2 * far + 1, to_slot(1))

    fwd = []

    def forward(src, half):
        cp = hcopy(src, half, h_fwd.at[len(fwd)], mate)
        cp.start()
        fwd.append(cp)

    hwait(2 * left + c, 0)
    rel_r = hcopy(2 * left + c, 0, h_send.at[6], 2 * right + c)
    rel_r.start()
    forward(2 * left + c, 0)
    hwait(2 * right + c, 1)
    rel_l = hcopy(2 * right + c, 1, h_send.at[7], 2 * left + c)
    rel_l.start()
    forward(2 * right + c, 1)

    def unit(buf_i, i, s):
        return buf_i.at[i, :, pl.ds(pl.multiple_of(s * seg, LANES), seg)]

    def landing(src, i, s):
        return qall.at[
            i, pl.ds(pl.multiple_of(src * rows, rows), rows), pl.ds(pl.multiple_of(s * seg, LANES), seg)
        ]

    def direct(slot, i, s, who):
        return remote(
            unit(scode.at[slot], i, s), landing(k, i, s),
            q_send.at[slot * 8 + i * SEGS + s], q_recv.at[k * 8 + i * SEGS + s], who,
        )

    def out_far(way, v):
        i, s, cc = v // 4, 2 * ((v // 2) % 2) + way, v % 2
        who = 2 * (right if way == 0 else left) + c
        return remote(
            unit(scode.at[cc], i, s), rbuf.at[way, v],
            q_send.at[cc * 8 + i * SEGS + s], r_recv.at[way * 8 + v], who,
        )

    def relay(way, v):
        i, s, cc = v // 4, 2 * ((v // 2) % 2) + way, v % 2
        src = 2 * (left if way == 0 else right) + c
        who = 2 * (right if way == 0 else left) + cc
        return remote(
            rbuf.at[way, v], landing(src, i, s),
            r_send.at[way * 8 + v], q_recv.at[src * 8 + i * SEGS + s], who,
        )

    def near(way, u):
        i, s, cc = u // 8, (u // 2) % SEGS, u % 2
        who = 2 * (right if way == 0 else left) + cc
        return direct(2 + 2 * way + cc, i, s, who)

    def send_far(v):
        out_far(0, v).start()
        out_far(1, v).start()

    def send_near(u):
        near(0, u).start()
        near(1, u).start()

    def pass_on(v):
        for way in range(2):
            out_far(way, v).wait_recv()
            relay(way, v).start()

    encode(2 * right, to_slot(2))
    encode(2 * right + 1, to_slot(3))
    encode(2 * left, to_slot(4))
    encode(2 * left + 1, to_slot(5))

    hwait(2 * left + c, 1)
    forward(2 * left + c, 1)
    hwait(2 * right + c, 0)
    forward(2 * right + c, 0)

    def first_far(v, _):
        send_far(v)
        return 0

    def first_near(u, _):
        send_near(u)
        return 0

    lax.fori_loop(0, 4, first_far, 0)
    lax.fori_loop(0, 8, first_near, 0)
    encode(mate, to_slot(6))
    encode(k, to_self)

    def to_mate(u, _):
        direct(6, u // SEGS, u % SEGS, mate).start()
        return 0

    lax.fori_loop(0, drafts * SEGS, to_mate, 0)

    hwait(2 * far + c, 0)
    forward(2 * far + c, 0)
    hwait(2 * far + c, 1)
    forward(2 * far + c, 1)
    for chip in (x, left, right, far):
        for half in range(2):
            hwait(2 * chip + 1 - c, half)

    def step(t, top):
        slot = t % 2

        @pl.when((t >= 2) & (t < 4))
        def _():
            pass_on(2 * (t - 2))
            pass_on(2 * (t - 2) + 1)

        @pl.when((t >= 4) & (t < 6))
        def _():
            send_far(4 + 2 * (t - 4))
            send_far(4 + 2 * (t - 4) + 1)

        @pl.when(t >= 8)
        def _():
            send_near(8 + 2 * (t - 8))
            send_near(8 + 2 * (t - 8) + 1)

        w_cp(t, slot).wait()
        prod = INV_TEMP * lax.dot_general(
            wbuf[slot], hall[...].reshape(positions * batch, dim), (((1,), (1,)), ((), ())), preferred_element_type=F32
        )
        base = pl.multiple_of(off + t * wrows, 8)
        for i in range(positions):
            z[i, pl.ds(base, wrows), :] = prod[:, i * batch:(i + 1) * batch]

        @pl.when(t + 2 < STEPS)
        def _():
            w_cp(t + 2, slot).start()

        return jnp.maximum(top, jnp.max(prod.reshape(wrows // 8, 8, positions * batch), axis=0))

    top = lax.fori_loop(0, STEPS, step, jnp.full((8, positions * batch), -jnp.inf, F32))
    own_max = jnp.max(top, axis=0, keepdims=True)

    chunk = 160
    row_i = lax.broadcasted_iota(jnp.int32, (chunk, batch), 0)
    for i in range(positions):
        m_i = own_max[:, i * batch:(i + 1) * batch]
        want = tok_ref[i:i + 1, :] - k * vocab if i < drafts else None

        def expo(t, carry, i=i, m_i=m_i, want=want):
            total, got = carry
            at = pl.ds(pl.multiple_of(off + t * chunk, 8), chunk)
            e = jnp.exp(z[i, at, :] - m_i)
            z[i, at, :] = e
            total = total + jnp.sum(e.reshape(chunk // 8, 8, batch), axis=0)
            if want is not None:
                pick = jnp.where(row_i + t * chunk == want, e, 0.0)
                got = got + jnp.sum(pick.reshape(chunk // 8, 8, batch), axis=0)
            return total, got

        zero = jnp.zeros((8, batch), F32)
        total, got = lax.fori_loop(0, vocab // chunk, expo, (zero, zero))
        msgs[k, i:i + 1, :] = m_i
        msgs[k, 3 + i:4 + i, :] = jnp.sum(total, axis=0, keepdims=True)
        if i < drafts:
            msgs[k, 6 + i:7 + i, :] = jnp.sum(got, axis=0, keepdims=True)

    def msg(p, src):
        return remote(msgs.at[src], msgs.at[src], m_send.at[p], m_recv.at[src], (k + p) % n)

    for p in range(1, n):
        msg(p, k).start()

    def rest_near(u, _):
        send_near(u)
        return 0

    lax.fori_loop(12, 16, rest_near, 0)
    for v in range(4, 8):
        pass_on(v)
    for p in range(1, n):
        msg(p, (k + p) % n).wait_recv()

    allm = msgs[...]
    peak = jnp.max(allm[:, 0:3, :], axis=0)
    part = jnp.exp(allm[:, 0:3, :] - peak[None])
    inv = 1.0 / jnp.sum(part * allm[:, 3:6, :], axis=0)
    p_pick = jnp.sum(part[:, 0:drafts, :] * allm[:, 6:8, :], axis=0) * inv[0:drafts]
    q_pick = jnp.sum(allm[:, 8:10, :], axis=0)
    q_scale = jnp.sum(allm[:, 10:12, :], axis=0) * (1.0 / (TOP * TOP * TOP * TOP))
    fac = jnp.exp(msgs[k, 0:3, :] - peak) * inv

    def scale(t, _):
        at = pl.ds(pl.multiple_of(off + t * chunk, 8), chunk)
        z[drafts, at, :] = z[drafts, at, :] * fac[drafts:drafts + 1, :]
        return 0

    lax.fori_loop(0, vocab // chunk, scale, 0)

    def out_cp(i, dst):
        return pltpu.make_async_copy(z.at[i, pl.ds(pl.multiple_of(off, 8), vocab), :], dst, osem.at[i])

    out_cp(drafts, bonus_ref).start()

    def xmsg(p, i, src):
        return remote(mass.at[i, src], mass.at[i, src], x_send.at[i * n + p], x_recv.at[i * n + src], (k + p) % n)

    for i in range(drafts):
        acc = [jnp.zeros((8, LANES), F32) for _ in range(batch // LANES)]
        for s in range(SEGS):
            for p in range(1, n):
                src = (k + p) % n
                remote(
                    landing(src, i, s), landing(src, i, s), q_send.at[0],
                    q_recv.at[src * 8 + i * SEGS + s], mate,
                ).wait_recv()

            def body(t, acc, i=i, s=s):
                at = pl.ds(pl.multiple_of((s * (tiles // SEGS) + t) * LANES, LANES), LANES)
                out = []
                for h in range(batch // LANES):
                    ls = slice(h * LANES, (h + 1) * LANES)
                    code = qall[i, ls, at].astype(jnp.int32).astype(F32)
                    y = code.T + float(HALF)
                    y = y * y
                    qt = y * y * q_scale[i:i + 1, ls]
                    ex = jnp.maximum(z[i, at, ls] * fac[i:i + 1, ls] - qt, 0.0)
                    z[i, at, ls] = ex
                    out.append(acc[h] + jnp.sum(ex.reshape(LANES // 8, 8, LANES), axis=0))
                return tuple(out)

            acc = lax.fori_loop(0, tiles // SEGS, body, tuple(acc))
        out_cp(i, ex_ref.at[i]).start()
        for h in range(batch // LANES):
            mass[i, k, :, h * LANES:(h + 1) * LANES] = acc[h]
        for p in range(1, n):
            xmsg(p, i, k).start()
    small_ref[...] = jnp.zeros(small_ref.shape, F32)
    small_ref[2:4, :] = p_pick
    small_ref[4:6, :] = q_pick
    for i in range(drafts):
        for p in range(1, n):
            xmsg(p, i, (k + p) % n).wait_recv()
        total = jnp.sum(jnp.sum(mass[i], axis=0), axis=0, keepdims=True)
        small_ref[i:i + 1, :] = 1.0 / total

    for cp in own_sends + [rel_r, rel_l] + fwd:
        cp.wait_send()
    for p in range(1, n):
        msg(p, k).wait_send()
        for i in range(drafts):
            xmsg(p, i, k).wait_send()

    def drain(u, _):
        direct(u // 8, (u % 8) // SEGS, u % SEGS, mate).wait_send()
        return 0

    lax.fori_loop(0, 7 * 8, drain, 0)

    def drain_relay(v, _):
        relay(0, v).wait_send()
        relay(1, v).wait_send()
        return 0

    lax.fori_loop(0, 8, drain_relay, 0)
    out_cp(drafts, bonus_ref).wait()
    for i in range(drafts):
        out_cp(i, ex_ref.at[i]).wait()


def solution(mesh):
    n = mesh.shape["tp"]

    def local(hid, w, q, tok):
        rows, positions, dim = hid.shape
        vocab = w.shape[1]
        drafts = positions - 1
        batch = rows * n
        q_tiles = q.shape[2] // LANES
        width = -(-vocab // LANES) * LANES
        q_view = q.reshape(rows, drafts, q_tiles, LANES).transpose(0, 2, 1, 3)
        q_view = with_layout_constraint(q_view, Layout((0, 1, 2, 3))).reshape(-1, LANES)
        dma = pltpu.SemaphoreType.DMA
        ex, bonus, small = pl.pallas_call(
            functools.partial(kernel, n),
            out_shape=(
                jax.ShapeDtypeStruct((drafts, vocab, batch), F32),
                jax.ShapeDtypeStruct((vocab, batch), F32),
                jax.ShapeDtypeStruct((8, batch), F32),
            ),
            in_specs=[pl.BlockSpec(memory_space=pltpu.VMEM)] + [pl.BlockSpec(memory_space=pl.ANY)] * 3,
            out_specs=(
                pl.BlockSpec(memory_space=pl.ANY),
                pl.BlockSpec(memory_space=pl.ANY),
                pl.BlockSpec(memory_space=pltpu.VMEM),
            ),
            scratch_shapes=[
                pltpu.VMEM((positions, batch, dim), jnp.bfloat16),
                pltpu.VMEM((positions, width, batch), F32),
                pltpu.VMEM((rows * q_tiles * drafts, LANES), F32),
                pltpu.VMEM((n - 1, drafts, rows, width), jnp.int16),
                pltpu.VMEM((drafts, batch, width), jnp.int16),
                pltpu.VMEM((2, 8, rows, width // SEGS), jnp.int16),
                pltpu.VMEM((2, vocab // STEPS, dim), jnp.bfloat16),
                pltpu.VMEM((n, 16, batch), F32),
                pltpu.VMEM((drafts, n, 8, batch), F32),
                pltpu.VMEM((drafts * (rows // 8), 8, LANES), F32),
                dma((8,)), dma((8,)), dma((2 * n,)),
                dma((7 * 8,)), dma((8 * 8,)), dma((16,)), dma((16,)),
                dma((n,)), dma((n,)), dma((2 * n,)), dma((2 * n,)),
                dma((8,)), dma((2,)), dma((3,)),
            ],
            compiler_params=pltpu.CompilerParams(
                collective_id=0, has_side_effects=True, vmem_limit_bytes=60 * 2**20
            ),
        )(tok.T, hid.transpose(1, 0, 2), w.T, q_view)
        residual = (ex * small[0:drafts][:, None, :]).transpose(2, 0, 1)
        accept = jnp.minimum(small[2:4] / small[4:6], 1.0)
        expected = accept[0] + accept[0] * accept[1]
        return accept.T, expected, residual, bonus.T

    return jax.shard_map(
        local,
        mesh=mesh,
        in_specs=(P(("dp", "tp"), None, None), P(None, "tp"), P(("dp", "tp"), None, None), P("dp", None)),
        out_specs=(P("dp", None), P("dp"), P("dp", None, "tp"), P("dp", "tp")),
        check_vma=False,
    )
```

```python
import functools

import jax
import jax.numpy as jnp
from jax import lax
from jax.experimental import pallas as pl
from jax.experimental.pallas import tpu as pltpu
from jax.experimental.layout import Layout, with_layout_constraint
from jax.sharding import PartitionSpec as P

INV_TEMP = 1.25
TOP = 65535.0
HALF = 32768
LANES = 128
SEGS = 4
STEPS = 10
PARTS = 5
F32 = jnp.float32
MESH = pl.DeviceIdType.MESH


def kernel(
    n, tok_in, hid_ref, w_ref, q_ref,
    z, small_ref,
    tok_ref, hall, stage, scode, qall, rbuf, wbuf, msgs, mass, rowc,
    h_send, h_fwd, h_recv, q_send, q_recv, r_send, r_recv,
    m_send, m_recv, x_send, x_recv, loc, wsem,
):
    k = lax.axis_index("tp")
    x, c = k // 2, k % 2
    chips = n // 2
    right, left = (x + 1) % chips, (x + chips - 1) % chips
    far = (x + 2) % chips
    mate = 2 * x + 1 - c
    positions, batch, dim = hall.shape
    drafts = positions - 1
    rows = batch // n
    vocab = w_ref.shape[0]
    width = qall.shape[2]
    seg = width // SEGS
    tiles = width // LANES
    pitch = q_ref.shape[0] // rows
    all_tiles = pitch // drafts
    off = (k * vocab) % LANES
    hcol = dim // 2
    wrows = vocab // STEPS

    def remote(src, dst, ssem, rsem, who):
        return pltpu.make_async_remote_copy(
            src_ref=src, dst_ref=dst, send_sem=ssem, recv_sem=rsem,
            device_id={"tp": who}, device_id_type=MESH,
        )

    hid_cp = pltpu.make_async_copy(hid_ref, hall.at[:, pl.ds(k * rows, rows), :], loc.at[0])
    hid_cp.start()
    tok_cp = pltpu.make_async_copy(tok_in, tok_ref, loc.at[6])
    tok_cp.start()

    def stage_cp(g):
        part = pl.ds(g * 8 * pitch, 8 * pitch)
        return pltpu.make_async_copy(q_ref.at[part], stage.at[part], loc.at[1 + g])

    for g in range(rows // 8):
        stage_cp(g).start()

    def w_cp(t, slot):
        return pltpu.make_async_copy(
            w_ref.at[pl.ds(pl.multiple_of(t * wrows, 8), wrows)], wbuf.at[slot], wsem.at[slot]
        )

    barrier = pltpu.get_barrier_semaphore()
    for p in range(1, n):
        pl.semaphore_signal(barrier, inc=1, device_id={"tp": (k + p) % n}, device_id_type=MESH)
    pl.semaphore_wait(barrier, n - 1)

    def hpiece(src, half):
        return hall.at[:, pl.ds(pl.multiple_of(src * rows, rows), rows), pl.ds(half * hcol, hcol)]

    def hcopy(src, half, ssem, who):
        return remote(hpiece(src, half), hpiece(src, half), ssem, h_recv.at[src * 2 + half], who)

    def hwait(src, half):
        hcopy(src, half, h_send.at[0], mate).wait_recv()

    hid_cp.wait()
    own_sends = []
    for idx, (who, half) in enumerate(
        [(2 * right + c, 0), (2 * left + c, 1), (2 * right + c, 1), (2 * left + c, 0), (mate, 0), (mate, 1)]
    ):
        cp = hcopy(k, half, h_send.at[idx], who)
        cp.start()
        own_sends.append(cp)
    w_cp(0, 0).start()
    w_cp(1, 1).start()

    z[:, 0:96, :] = jnp.zeros((positions, 96, batch), F32)
    z[:, width - 96:width, :] = jnp.zeros((positions, 96, batch), F32)

    tok_cp.wait()
    for g in range(rows // 8):
        stage_cp(g).wait()

    def qrows(g, i, j):
        return stage[pl.ds(g * 8 * pitch + drafts * j + i, 8, stride=pitch), :]

    groups = [(i, g) for i in range(drafts) for g in range(rows // 8)]
    lane_b = lax.broadcasted_iota(jnp.int32, (8, batch), 1)
    sub_b = lax.broadcasted_iota(jnp.int32, (8, batch), 0)
    lane_t = lax.broadcasted_iota(jnp.int32, (8, LANES), 1)
    mine = [lane_b == k * rows + 8 * g + sub_b for g in range(rows // 8)]
    tok_col = []
    for i, g in groups:
        t = jnp.where(mine[g], jnp.broadcast_to(tok_ref[i:i + 1, :].astype(F32), (8, batch)), 0.0)
        tok_col.append(jnp.broadcast_to(jnp.sum(t, axis=1, keepdims=True), (8, LANES)).astype(jnp.int32))

    def scan(j, carry):
        top, got = carry
        new_top, new_got = [], []
        col = lane_t + j * LANES
        for a, (i, g) in enumerate(groups):
            v = qrows(g, i, j)
            new_top.append(jnp.maximum(top[a], v))
            new_got.append(jnp.where(col == tok_col[a], v, got[a]))
        return tuple(new_top), tuple(new_got)

    zero8 = tuple(jnp.zeros((8, LANES), F32) for _ in groups)
    top, got = lax.fori_loop(0, all_tiles, scan, (zero8, zero8))
    qtop_row, qgot_row = [], []
    for i in range(drafts):
        acc_t = jnp.zeros((8, batch), F32)
        acc_g = jnp.zeros((8, batch), F32)
        for a, (ii, g) in enumerate(groups):
            if ii != i:
                continue
            tcol = jnp.max(top[a], axis=1, keepdims=True)
            gcol = jnp.sum(got[a], axis=1, keepdims=True)
            rowc[a] = jnp.broadcast_to(jnp.log(TOP) - 0.25 * jnp.log(tcol), (8, LANES))
            acc_t = acc_t + jnp.where(mine[g], jnp.broadcast_to(tcol, (8, batch)), 0.0)
            acc_g = acc_g + jnp.where(mine[g], jnp.broadcast_to(gcol, (8, batch)), 0.0)
        qtop_row.append(jnp.sum(acc_t, axis=0, keepdims=True))
        qgot_row.append(jnp.sum(acc_g, axis=0, keepdims=True))
    msgs[k] = jnp.zeros(msgs.shape[1:], F32)
    for i in range(drafts):
        msgs[k, 8 + i:9 + i, :] = qgot_row[i]
        msgs[k, 10 + i:11 + i, :] = qtop_row[i]

    def encode(dest, put):
        first = (dest * vocab) // LANES

        def body(j, _):
            for i in range(drafts):
                for gg in range(rows // 16):
                    parts = []
                    for g in (2 * gg, 2 * gg + 1):
                        v = qrows(g, i, first + j)
                        y = jnp.exp(0.25 * jnp.log(v) + rowc[i * (rows // 8) + g])
                        parts.append((y + 0.5).astype(jnp.int32) - HALF)
                    code = jnp.concatenate(parts, axis=0).astype(jnp.int16)
                    put(i, gg, pl.ds(pl.multiple_of(j * LANES, LANES), LANES), code)
            return 0

        lax.fori_loop(0, tiles, body, 0)

    def to_slot(r):
        def put(i, gg, cols, code):
            scode[r, i, 16 * gg:16 * gg + 16, cols] = code

        return put

    def to_self(i, gg, cols, code):
        qall[i, pl.ds(pl.multiple_of(k * rows + 16 * gg, 16), 16), cols] = code

    encode(2 * far, to_slot(0))
    encode(2 * far + 1, to_slot(1))

    fwd = []

    def forward(src, half):
        cp = hcopy(src, half, h_fwd.at[len(fwd)], mate)
        cp.start()
        fwd.append(cp)

    hwait(2 * left + c, 0)
    rel_r = hcopy(2 * left + c, 0, h_send.at[6], 2 * right + c)
    rel_r.start()
    forward(2 * left + c, 0)
    hwait(2 * right + c, 1)
    rel_l = hcopy(2 * right + c, 1, h_send.at[7], 2 * left + c)
    rel_l.start()
    forward(2 * right + c, 1)

    def unit(buf_i, i, s):
        return buf_i.at[i, :, pl.ds(pl.multiple_of(s * seg, LANES), seg)]

    def landing(src, i, s):
        return qall.at[
            i, pl.ds(pl.multiple_of(src * rows, rows), rows), pl.ds(pl.multiple_of(s * seg, LANES), seg)
        ]

    def direct(slot, i, s, who):
        return remote(
            unit(scode.at[slot], i, s), landing(k, i, s),
            q_send.at[slot * 8 + i * SEGS + s], q_recv.at[k * 8 + i * SEGS + s], who,
        )

    def out_far(way, v):
        i, s, cc = v // 4, 2 * ((v // 2) % 2) + way, v % 2
        who = 2 * (right if way == 0 else left) + c
        return remote(
            unit(scode.at[cc], i, s), rbuf.at[way, v],
            q_send.at[cc * 8 + i * SEGS + s], r_recv.at[way * 8 + v], who,
        )

    def relay(way, v):
        i, s, cc = v // 4, 2 * ((v // 2) % 2) + way, v % 2
        src = 2 * (left if way == 0 else right) + c
        who = 2 * (right if way == 0 else left) + cc
        return remote(
            rbuf.at[way, v], landing(src, i, s),
            r_send.at[way * 8 + v], q_recv.at[src * 8 + i * SEGS + s], who,
        )

    def near(way, u):
        i, s, cc = u // 8, (u // 2) % SEGS, u % 2
        who = 2 * (right if way == 0 else left) + cc
        return direct(2 + 2 * way + cc, i, s, who)

    def send_far(v):
        out_far(0, v).start()
        out_far(1, v).start()

    def send_near(u):
        near(0, u).start()
        near(1, u).start()

    def pass_on(v):
        for way in range(2):
            out_far(way, v).wait_recv()
            relay(way, v).start()

    encode(2 * right, to_slot(2))
    encode(2 * right + 1, to_slot(3))
    encode(2 * left, to_slot(4))
    encode(2 * left + 1, to_slot(5))

    hwait(2 * left + c, 1)
    forward(2 * left + c, 1)
    hwait(2 * right + c, 0)
    forward(2 * right + c, 0)

    def first_far(v, _):
        send_far(v)
        return 0

    def first_near(u, _):
        send_near(u)
        return 0

    lax.fori_loop(0, 4, first_far, 0)
    lax.fori_loop(0, 8, first_near, 0)
    encode(mate, to_slot(6))
    encode(k, to_self)

    def to_mate(u, _):
        direct(6, u // SEGS, u % SEGS, mate).start()
        return 0

    lax.fori_loop(0, drafts * SEGS, to_mate, 0)

    hwait(2 * far + c, 0)
    forward(2 * far + c, 0)
    hwait(2 * far + c, 1)
    forward(2 * far + c, 1)
    for chip in (x, left, right, far):
        for half in range(2):
            hwait(2 * chip + 1 - c, half)

    def step(t, top):
        slot = t % 2

        @pl.when((t >= 2) & (t < 4))
        def _():
            pass_on(2 * (t - 2))
            pass_on(2 * (t - 2) + 1)

        @pl.when((t >= 4) & (t < 6))
        def _():
            send_far(4 + 2 * (t - 4))
            send_far(4 + 2 * (t - 4) + 1)

        @pl.when(t >= 8)
        def _():
            send_near(8 + 2 * (t - 8))
            send_near(8 + 2 * (t - 8) + 1)

        w_cp(t, slot).wait()
        prod = INV_TEMP * lax.dot_general(
            wbuf[slot], hall[...].reshape(positions * batch, dim), (((1,), (1,)), ((), ())), preferred_element_type=F32
        )
        base = pl.multiple_of(off + t * wrows, 8)
        for i in range(positions):
            z[i, pl.ds(base, wrows), :] = prod[:, i * batch:(i + 1) * batch]

        @pl.when(t + 2 < STEPS)
        def _():
            w_cp(t + 2, slot).start()

        return jnp.maximum(top, jnp.max(prod.reshape(wrows // 8, 8, positions * batch), axis=0))

    top = lax.fori_loop(0, STEPS, step, jnp.full((8, positions * batch), -jnp.inf, F32))
    own_max = jnp.max(top, axis=0, keepdims=True)

    chunk = 160
    row_i = lax.broadcasted_iota(jnp.int32, (chunk, batch), 0)
    for i in range(positions):
        m_i = own_max[:, i * batch:(i + 1) * batch]
        want = tok_ref[i:i + 1, :] - k * vocab if i < drafts else None

        def expo(t, carry, i=i, m_i=m_i, want=want):
            total, got = carry
            at = pl.ds(pl.multiple_of(off + t * chunk, 8), chunk)
            e = jnp.exp(z[i, at, :] - m_i)
            z[i, at, :] = e
            total = total + jnp.sum(e.reshape(chunk // 8, 8, batch), axis=0)
            if want is not None:
                pick = jnp.where(row_i + t * chunk == want, e, 0.0)
                got = got + jnp.sum(pick.reshape(chunk // 8, 8, batch), axis=0)
            return total, got

        zero = jnp.zeros((8, batch), F32)
        total, got = lax.fori_loop(0, vocab // chunk, expo, (zero, zero))
        msgs[k, i:i + 1, :] = m_i
        msgs[k, 3 + i:4 + i, :] = jnp.sum(total, axis=0, keepdims=True)
        if i < drafts:
            msgs[k, 6 + i:7 + i, :] = jnp.sum(got, axis=0, keepdims=True)

    def msg(p, src):
        return remote(msgs.at[src], msgs.at[src], m_send.at[p], m_recv.at[src], (k + p) % n)

    for p in range(1, n):
        msg(p, k).start()

    def rest_near(u, _):
        send_near(u)
        return 0

    lax.fori_loop(12, 16, rest_near, 0)
    for v in range(4, 8):
        pass_on(v)
    for p in range(1, n):
        msg(p, (k + p) % n).wait_recv()

    allm = msgs[...]
    peak = jnp.max(allm[:, 0:3, :], axis=0)
    part = jnp.exp(allm[:, 0:3, :] - peak[None])
    inv = 1.0 / jnp.sum(part * allm[:, 3:6, :], axis=0)
    p_pick = jnp.sum(part[:, 0:drafts, :] * allm[:, 6:8, :], axis=0) * inv[0:drafts]
    q_pick = jnp.sum(allm[:, 8:10, :], axis=0)
    q_scale = jnp.sum(allm[:, 10:12, :], axis=0) * (1.0 / (TOP * TOP * TOP * TOP))
    fac = jnp.exp(msgs[k, 0:3, :] - peak) * inv

    def scale(t, _):
        at = pl.ds(pl.multiple_of(off + t * chunk, 8), chunk)
        z[drafts, at, :] = z[drafts, at, :] * fac[drafts:drafts + 1, :]
        return 0

    lax.fori_loop(0, vocab // chunk, scale, 0)

    def xmsg(p, i, src):
        return remote(mass.at[i, src], mass.at[i, src], x_send.at[i * n + p], x_recv.at[i * n + src], (k + p) % n)

    for i in range(drafts):
        acc = [jnp.zeros((8, LANES), F32) for _ in range(batch // LANES)]
        for s in range(SEGS):
            for p in range(1, n):
                src = (k + p) % n
                remote(
                    landing(src, i, s), landing(src, i, s), q_send.at[0],
                    q_recv.at[src * 8 + i * SEGS + s], mate,
                ).wait_recv()

            def body(t, acc, i=i, s=s):
                at = pl.ds(pl.multiple_of((s * (tiles // SEGS) + t) * LANES, LANES), LANES)
                out = []
                for h in range(batch // LANES):
                    ls = slice(h * LANES, (h + 1) * LANES)
                    code = qall[i, ls, at].astype(jnp.int32).astype(F32)
                    y = code.T + float(HALF)
                    y = y * y
                    qt = y * y * q_scale[i:i + 1, ls]
                    ex = jnp.maximum(z[i, at, ls] * fac[i:i + 1, ls] - qt, 0.0)
                    z[i, at, ls] = ex
                    out.append(acc[h] + jnp.sum(ex.reshape(LANES // 8, 8, LANES), axis=0))
                return tuple(out)

            acc = lax.fori_loop(0, tiles // SEGS, body, tuple(acc))
        for h in range(batch // LANES):
            mass[i, k, :, h * LANES:(h + 1) * LANES] = acc[h]
        for p in range(1, n):
            xmsg(p, i, k).start()
    small_ref[...] = jnp.zeros(small_ref.shape, F32)
    small_ref[2:4, :] = p_pick
    small_ref[4:6, :] = q_pick
    for i in range(drafts):
        for p in range(1, n):
            xmsg(p, i, (k + p) % n).wait_recv()
        total = jnp.sum(jnp.sum(mass[i], axis=0), axis=0, keepdims=True)
        small_ref[i:i + 1, :] = 1.0 / total

    for cp in own_sends + [rel_r, rel_l] + fwd:
        cp.wait_send()
    for p in range(1, n):
        msg(p, k).wait_send()
        for i in range(drafts):
            xmsg(p, i, k).wait_send()

    def drain(u, _):
        direct(u // 8, (u % 8) // SEGS, u % SEGS, mate).wait_send()
        return 0

    lax.fori_loop(0, 7 * 8, drain, 0)

    def drain_relay(v, _):
        relay(0, v).wait_send()
        relay(1, v).wait_send()
        return 0

    lax.fori_loop(0, 8, drain_relay, 0)


def finish(n, z, small, res_ref, bonus_ref, acc_ref, exp_ref, buf, sem):
    drafts, vocab, _ = res_ref.shape
    off = pl.multiple_of((lax.axis_index("tp") * vocab) % LANES, 8)
    last = pltpu.make_async_copy(z.at[drafts, pl.ds(off, vocab), :], bonus_ref, sem.at[0])
    last.start()
    copies = [last]
    part = vocab // PARTS
    for i in range(drafts):
        scale = small[i:i + 1, :]
        for t in range(PARTS):
            to = pl.ds(t * part, part)
            buf[i, to, :] = z[i, pl.ds(pl.multiple_of(off + t * part, 8), part), :] * scale
            cp = pltpu.make_async_copy(buf.at[i, to], res_ref.at[i, to], sem.at[len(copies)])
            cp.start()
            copies.append(cp)
    accept = jnp.minimum(small[2:4, :] / small[4:6, :], 1.0)
    acc_ref[...] = accept
    exp_ref[...] = accept[0:1] + accept[0:1] * accept[1:2]
    for cp in copies:
        cp.wait()


def solution(mesh):
    n = mesh.shape["tp"]

    def local(hid, w, q, tok):
        rows, positions, dim = hid.shape
        vocab = w.shape[1]
        drafts = positions - 1
        batch = rows * n
        q_tiles = q.shape[2] // LANES
        width = -(-vocab // LANES) * LANES
        q_view = q.reshape(rows, drafts, q_tiles, LANES).transpose(0, 2, 1, 3)
        q_view = with_layout_constraint(q_view, Layout((0, 1, 2, 3))).reshape(-1, LANES)
        dma = pltpu.SemaphoreType.DMA
        vmem, anywhere = pl.BlockSpec(memory_space=pltpu.VMEM), pl.BlockSpec(memory_space=pltpu.HBM)
        z, small = pl.pallas_call(
            functools.partial(kernel, n),
            out_shape=(
                jax.ShapeDtypeStruct((positions, width, batch), F32),
                jax.ShapeDtypeStruct((8, batch), F32),
            ),
            in_specs=[anywhere] * 4,
            out_specs=(vmem, vmem),
            scratch_shapes=[
                pltpu.VMEM((drafts, batch), jnp.int32),
                pltpu.VMEM((positions, batch, dim), jnp.bfloat16),
                pltpu.VMEM((rows * q_tiles * drafts, LANES), F32),
                pltpu.VMEM((n - 1, drafts, rows, width), jnp.int16),
                pltpu.VMEM((drafts, batch, width), jnp.int16),
                pltpu.VMEM((2, 8, rows, width // SEGS), jnp.int16),
                pltpu.VMEM((2, vocab // STEPS, dim), jnp.bfloat16),
                pltpu.VMEM((n, 16, batch), F32),
                pltpu.VMEM((drafts, n, 8, batch), F32),
                pltpu.VMEM((drafts * (rows // 8), 8, LANES), F32),
                dma((8,)), dma((8,)), dma((2 * n,)),
                dma((7 * 8,)), dma((8 * 8,)), dma((16,)), dma((16,)),
                dma((n,)), dma((n,)), dma((2 * n,)), dma((2 * n,)),
                dma((8,)), dma((2,)),
            ],
            compiler_params=pltpu.CompilerParams(
                collective_id=0, has_side_effects=True, vmem_limit_bytes=40 * 2**20
            ),
        )(*[pltpu.with_memory_space_constraint(a, pltpu.HBM) for a in (tok.T, hid.transpose(1, 0, 2), w.T, q_view)])
        residual, bonus, accept, expected = pl.pallas_call(
            functools.partial(finish, n),
            out_shape=(
                jax.ShapeDtypeStruct((drafts, vocab, batch), F32),
                jax.ShapeDtypeStruct((vocab, batch), F32),
                jax.ShapeDtypeStruct((drafts, batch), F32),
                jax.ShapeDtypeStruct((1, batch), F32),
            ),
            in_specs=[vmem, vmem],
            out_specs=(anywhere, anywhere, vmem, vmem),
            scratch_shapes=[pltpu.VMEM((drafts, vocab, batch), F32), dma((drafts * PARTS + 1,))],
            compiler_params=pltpu.CompilerParams(vmem_limit_bytes=24 * 2**20),
        )(z, small)
        return accept.T, expected[0], residual.transpose(2, 0, 1), bonus.T

    return jax.shard_map(
        local,
        mesh=mesh,
        in_specs=(P(("dp", "tp"), None, None), P(None, "tp"), P(("dp", "tp"), None, None), P("dp", None)),
        out_specs=(P("dp", None), P("dp"), P("dp", None, "tp"), P("dp", "tp")),
        check_vma=False,
    )
```

```python
import functools

import jax
import jax.numpy as jnp
from jax import lax
from jax.experimental import pallas as pl
from jax.experimental.pallas import tpu as pltpu
from jax.experimental.layout import Layout, with_layout_constraint
from jax.sharding import PartitionSpec as P

INV_TEMP = 1.25
TOP = 65535.0
HALF = 32768
LANES = 128
SEGS = 4
STEPS = 10
PARTS = 5
F32 = jnp.float32
MESH = pl.DeviceIdType.MESH


def kernel(
    n, tok_in, hid_ref, w_ref, q_ref,
    z, small_ref,
    tok_ref, hall, stage, scode, qall, rbuf, wbuf, msgs, mass, rowc,
    h_send, h_fwd, h_recv, q_send, q_recv, r_send, r_recv,
    m_send, m_recv, x_send, x_recv, loc, wsem,
):
    k = lax.axis_index("tp")
    x, c = k // 2, k % 2
    chips = n // 2
    right, left = (x + 1) % chips, (x + chips - 1) % chips
    far = (x + 2) % chips
    mate = 2 * x + 1 - c
    positions, batch, dim = hall.shape
    drafts = positions - 1
    rows = batch // n
    vocab = w_ref.shape[0]
    width = qall.shape[2]
    seg = width // SEGS
    tiles = width // LANES
    pitch = q_ref.shape[0] // rows
    all_tiles = pitch // drafts
    off = (k * vocab) % LANES
    hcol = dim // 2
    wrows = vocab // STEPS

    def remote(src, dst, ssem, rsem, who):
        return pltpu.make_async_remote_copy(
            src_ref=src, dst_ref=dst, send_sem=ssem, recv_sem=rsem,
            device_id={"tp": who}, device_id_type=MESH,
        )

    hid_cp = pltpu.make_async_copy(hid_ref, hall.at[:, pl.ds(k * rows, rows), :], loc.at[0])
    hid_cp.start()
    tok_cp = pltpu.make_async_copy(tok_in, tok_ref, loc.at[6])
    tok_cp.start()

    def stage_cp(g):
        part = pl.ds(g * 8 * pitch, 8 * pitch)
        return pltpu.make_async_copy(q_ref.at[part], stage.at[part], loc.at[1 + g])

    for g in range(rows // 8):
        stage_cp(g).start()

    def w_cp(t, slot):
        return pltpu.make_async_copy(
            w_ref.at[pl.ds(pl.multiple_of(t * wrows, 8), wrows)], wbuf.at[slot], wsem.at[slot]
        )

    barrier = pltpu.get_barrier_semaphore()
    for p in range(1, n):
        pl.semaphore_signal(barrier, inc=1, device_id={"tp": (k + p) % n}, device_id_type=MESH)
    pl.semaphore_wait(barrier, n - 1)

    def hpiece(src, half):
        return hall.at[:, pl.ds(pl.multiple_of(src * rows, rows), rows), pl.ds(half * hcol, hcol)]

    def hcopy(src, half, ssem, who):
        return remote(hpiece(src, half), hpiece(src, half), ssem, h_recv.at[src * 2 + half], who)

    def hwait(src, half):
        hcopy(src, half, h_send.at[0], mate).wait_recv()

    hid_cp.wait()
    own_sends = []
    for idx, (who, half) in enumerate(
        [(2 * right + c, 0), (2 * left + c, 1), (2 * right + c, 1), (2 * left + c, 0), (mate, 0), (mate, 1)]
    ):
        cp = hcopy(k, half, h_send.at[idx], who)
        cp.start()
        own_sends.append(cp)
    w_cp(0, 0).start()
    w_cp(1, 1).start()

    z[:, 0:96, :] = jnp.zeros((positions, 96, batch), F32)
    z[:, width - 96:width, :] = jnp.zeros((positions, 96, batch), F32)

    tok_cp.wait()
    for g in range(rows // 8):
        stage_cp(g).wait()

    def qrows(g, i, j):
        return stage[pl.ds(g * 8 * pitch + drafts * j + i, 8, stride=pitch), :]

    groups = [(i, g) for i in range(drafts) for g in range(rows // 8)]
    lane_b = lax.broadcasted_iota(jnp.int32, (8, batch), 1)
    sub_b = lax.broadcasted_iota(jnp.int32, (8, batch), 0)
    lane_t = lax.broadcasted_iota(jnp.int32, (8, LANES), 1)
    mine = [lane_b == k * rows + 8 * g + sub_b for g in range(rows // 8)]
    tok_col = []
    for i, g in groups:
        t = jnp.where(mine[g], jnp.broadcast_to(tok_ref[i:i + 1, :].astype(F32), (8, batch)), 0.0)
        tok_col.append(jnp.broadcast_to(jnp.sum(t, axis=1, keepdims=True), (8, LANES)).astype(jnp.int32))

    def scan(j, carry):
        top, got = carry
        new_top, new_got = [], []
        col = lane_t + j * LANES
        for a, (i, g) in enumerate(groups):
            v = qrows(g, i, j)
            new_top.append(jnp.maximum(top[a], v))
            new_got.append(jnp.where(col == tok_col[a], v, got[a]))
        return tuple(new_top), tuple(new_got)

    zero8 = tuple(jnp.zeros((8, LANES), F32) for _ in groups)
    top, got = lax.fori_loop(0, all_tiles, scan, (zero8, zero8))
    qtop_row, qgot_row = [], []
    for i in range(drafts):
        acc_t = jnp.zeros((8, batch), F32)
        acc_g = jnp.zeros((8, batch), F32)
        for a, (ii, g) in enumerate(groups):
            if ii != i:
                continue
            tcol = jnp.max(top[a], axis=1, keepdims=True)
            gcol = jnp.sum(got[a], axis=1, keepdims=True)
            rowc[a] = jnp.broadcast_to(jnp.log(TOP) - 0.25 * jnp.log(tcol), (8, LANES))
            acc_t = acc_t + jnp.where(mine[g], jnp.broadcast_to(tcol, (8, batch)), 0.0)
            acc_g = acc_g + jnp.where(mine[g], jnp.broadcast_to(gcol, (8, batch)), 0.0)
        qtop_row.append(jnp.sum(acc_t, axis=0, keepdims=True))
        qgot_row.append(jnp.sum(acc_g, axis=0, keepdims=True))
    msgs[k] = jnp.zeros(msgs.shape[1:], F32)
    for i in range(drafts):
        msgs[k, 8 + i:9 + i, :] = qgot_row[i]
        msgs[k, 10 + i:11 + i, :] = qtop_row[i]

    def encode(dest, put):
        first = (dest * vocab) // LANES

        def body(j, _):
            for i in range(drafts):
                for gg in range(rows // 16):
                    parts = []
                    for g in (2 * gg, 2 * gg + 1):
                        v = qrows(g, i, first + j)
                        y = jnp.exp(0.25 * jnp.log(v) + rowc[i * (rows // 8) + g])
                        parts.append((y + 0.5).astype(jnp.int32) - HALF)
                    code = jnp.concatenate(parts, axis=0).astype(jnp.int16)
                    put(i, gg, pl.ds(pl.multiple_of(j * LANES, LANES), LANES), code)
            return 0

        lax.fori_loop(0, tiles, body, 0)

    def to_slot(r):
        def put(i, gg, cols, code):
            scode[r, i, 16 * gg:16 * gg + 16, cols] = code

        return put

    def to_self(i, gg, cols, code):
        qall[i, pl.ds(pl.multiple_of(k * rows + 16 * gg, 16), 16), cols] = code

    encode(2 * far, to_slot(0))
    encode(2 * far + 1, to_slot(1))

    fwd = []

    def forward(src, half):
        cp = hcopy(src, half, h_fwd.at[len(fwd)], mate)
        cp.start()
        fwd.append(cp)

    hwait(2 * left + c, 0)
    rel_r = hcopy(2 * left + c, 0, h_send.at[6], 2 * right + c)
    rel_r.start()
    forward(2 * left + c, 0)
    hwait(2 * right + c, 1)
    rel_l = hcopy(2 * right + c, 1, h_send.at[7], 2 * left + c)
    rel_l.start()
    forward(2 * right + c, 1)

    def unit(buf_i, i, s):
        return buf_i.at[i, :, pl.ds(pl.multiple_of(s * seg, LANES), seg)]

    def landing(src, i, s):
        return qall.at[
            i, pl.ds(pl.multiple_of(src * rows, rows), rows), pl.ds(pl.multiple_of(s * seg, LANES), seg)
        ]

    def direct(slot, i, s, who):
        return remote(
            unit(scode.at[slot], i, s), landing(k, i, s),
            q_send.at[slot * 8 + i * SEGS + s], q_recv.at[k * 8 + i * SEGS + s], who,
        )

    def out_far(way, v):
        i, s, cc = v // 4, 2 * ((v // 2) % 2) + way, v % 2
        who = 2 * (right if way == 0 else left) + c
        return remote(
            unit(scode.at[cc], i, s), rbuf.at[way, v],
            q_send.at[cc * 8 + i * SEGS + s], r_recv.at[way * 8 + v], who,
        )

    def relay(way, v):
        i, s, cc = v // 4, 2 * ((v // 2) % 2) + way, v % 2
        src = 2 * (left if way == 0 else right) + c
        who = 2 * (right if way == 0 else left) + cc
        return remote(
            rbuf.at[way, v], landing(src, i, s),
            r_send.at[way * 8 + v], q_recv.at[src * 8 + i * SEGS + s], who,
        )

    def near(way, u):
        i, s, cc = u // 8, (u // 2) % SEGS, u % 2
        who = 2 * (right if way == 0 else left) + cc
        return direct(2 + 2 * way + cc, i, s, who)

    def send_far(v):
        out_far(0, v).start()
        out_far(1, v).start()

    def send_near(u):
        near(0, u).start()
        near(1, u).start()

    def pass_on(v):
        for way in range(2):
            out_far(way, v).wait_recv()
            relay(way, v).start()

    encode(2 * right, to_slot(2))
    encode(2 * right + 1, to_slot(3))
    encode(2 * left, to_slot(4))
    encode(2 * left + 1, to_slot(5))

    hwait(2 * left + c, 1)
    forward(2 * left + c, 1)
    hwait(2 * right + c, 0)
    forward(2 * right + c, 0)

    def first_far(v, _):
        send_far(v)
        return 0

    def first_near(u, _):
        send_near(u)
        return 0

    lax.fori_loop(0, 4, first_far, 0)
    lax.fori_loop(0, 8, first_near, 0)
    encode(mate, to_slot(6))
    encode(k, to_self)

    def to_mate(u, _):
        direct(6, u // SEGS, u % SEGS, mate).start()
        return 0

    lax.fori_loop(0, drafts * SEGS, to_mate, 0)

    hwait(2 * far + c, 0)
    forward(2 * far + c, 0)
    hwait(2 * far + c, 1)
    forward(2 * far + c, 1)
    for chip in (x, left, right, far):
        for half in range(2):
            hwait(2 * chip + 1 - c, half)

    def step(t, top):
        slot = t % 2

        @pl.when((t >= 2) & (t < 4))
        def _():
            pass_on(2 * (t - 2))
            pass_on(2 * (t - 2) + 1)

        @pl.when((t >= 4) & (t < 6))
        def _():
            send_far(4 + 2 * (t - 4))
            send_far(4 + 2 * (t - 4) + 1)

        @pl.when(t >= 6)
        def _():
            send_near(8 + 2 * (t - 6))
            send_near(8 + 2 * (t - 6) + 1)

        w_cp(t, slot).wait()
        prod = INV_TEMP * lax.dot_general(
            wbuf[slot], hall[...].reshape(positions * batch, dim), (((1,), (1,)), ((), ())), preferred_element_type=F32
        )
        base = pl.multiple_of(off + t * wrows, 8)
        for i in range(positions):
            z[i, pl.ds(base, wrows), :] = prod[:, i * batch:(i + 1) * batch]

        @pl.when(t + 2 < STEPS)
        def _():
            w_cp(t + 2, slot).start()

        return jnp.maximum(top, jnp.max(prod.reshape(wrows // 8, 8, positions * batch), axis=0))

    top = lax.fori_loop(0, STEPS, step, jnp.full((8, positions * batch), -jnp.inf, F32))
    own_max = jnp.max(top, axis=0, keepdims=True)

    chunk = 160
    row_i = lax.broadcasted_iota(jnp.int32, (chunk, batch), 0)
    for i in range(positions):
        m_i = own_max[:, i * batch:(i + 1) * batch]
        want = tok_ref[i:i + 1, :] - k * vocab if i < drafts else None

        def expo(t, carry, i=i, m_i=m_i, want=want):
            total, got = carry
            at = pl.ds(pl.multiple_of(off + t * chunk, 8), chunk)
            e = jnp.exp(z[i, at, :] - m_i)
            z[i, at, :] = e
            total = total + jnp.sum(e.reshape(chunk // 8, 8, batch), axis=0)
            if want is not None:
                pick = jnp.where(row_i + t * chunk == want, e, 0.0)
                got = got + jnp.sum(pick.reshape(chunk // 8, 8, batch), axis=0)
            return total, got

        zero = jnp.zeros((8, batch), F32)
        total, got = lax.fori_loop(0, vocab // chunk, expo, (zero, zero))
        msgs[k, i:i + 1, :] = m_i
        msgs[k, 3 + i:4 + i, :] = jnp.sum(total, axis=0, keepdims=True)
        if i < drafts:
            msgs[k, 6 + i:7 + i, :] = jnp.sum(got, axis=0, keepdims=True)

    def msg(p, src):
        return remote(msgs.at[src], msgs.at[src], m_send.at[p], m_recv.at[src], (k + p) % n)

    for p in range(1, n):
        msg(p, k).start()

    for v in range(4, 8):
        pass_on(v)
    for p in range(1, n):
        msg(p, (k + p) % n).wait_recv()

    allm = msgs[...]
    peak = jnp.max(allm[:, 0:3, :], axis=0)
    part = jnp.exp(allm[:, 0:3, :] - peak[None])
    inv = 1.0 / jnp.sum(part * allm[:, 3:6, :], axis=0)
    p_pick = jnp.sum(part[:, 0:drafts, :] * allm[:, 6:8, :], axis=0) * inv[0:drafts]
    q_pick = jnp.sum(allm[:, 8:10, :], axis=0)
    q_scale = jnp.sum(allm[:, 10:12, :], axis=0) * (1.0 / (TOP * TOP * TOP * TOP))
    fac = jnp.exp(msgs[k, 0:3, :] - peak) * inv

    def scale(t, _):
        at = pl.ds(pl.multiple_of(off + t * chunk, 8), chunk)
        z[drafts, at, :] = z[drafts, at, :] * fac[drafts:drafts + 1, :]
        return 0

    lax.fori_loop(0, vocab // chunk, scale, 0)

    def xmsg(p, i, src):
        return remote(mass.at[i, src], mass.at[i, src], x_send.at[i * n + p], x_recv.at[i * n + src], (k + p) % n)

    for i in range(drafts):
        acc = [jnp.zeros((8, LANES), F32) for _ in range(batch // LANES)]
        for s in range(SEGS):
            for p in range(1, n):
                src = (k + p) % n
                remote(
                    landing(src, i, s), landing(src, i, s), q_send.at[0],
                    q_recv.at[src * 8 + i * SEGS + s], mate,
                ).wait_recv()

            def body(t, acc, i=i, s=s):
                at = pl.ds(pl.multiple_of((s * (tiles // SEGS) + t) * LANES, LANES), LANES)
                out = []
                for h in range(batch // LANES):
                    ls = slice(h * LANES, (h + 1) * LANES)
                    code = qall[i, ls, at].astype(jnp.int32).astype(F32)
                    y = code.T + float(HALF)
                    y = y * y
                    qt = y * y * q_scale[i:i + 1, ls]
                    ex = jnp.maximum(z[i, at, ls] * fac[i:i + 1, ls] - qt, 0.0)
                    z[i, at, ls] = ex
                    out.append(acc[h] + jnp.sum(ex.reshape(LANES // 8, 8, LANES), axis=0))
                return tuple(out)

            acc = lax.fori_loop(0, tiles // SEGS, body, tuple(acc))
        for h in range(batch // LANES):
            mass[i, k, :, h * LANES:(h + 1) * LANES] = acc[h]
        for p in range(1, n):
            xmsg(p, i, k).start()
    small_ref[...] = jnp.zeros(small_ref.shape, F32)
    small_ref[2:4, :] = p_pick
    small_ref[4:6, :] = q_pick
    for i in range(drafts):
        for p in range(1, n):
            xmsg(p, i, (k + p) % n).wait_recv()
        total = jnp.sum(jnp.sum(mass[i], axis=0), axis=0, keepdims=True)
        small_ref[i:i + 1, :] = 1.0 / total

    for cp in own_sends + [rel_r, rel_l] + fwd:
        cp.wait_send()
    for p in range(1, n):
        msg(p, k).wait_send()
        for i in range(drafts):
            xmsg(p, i, k).wait_send()

    def drain(u, _):
        direct(u // 8, (u % 8) // SEGS, u % SEGS, mate).wait_send()
        return 0

    lax.fori_loop(0, 7 * 8, drain, 0)

    def drain_relay(v, _):
        relay(0, v).wait_send()
        relay(1, v).wait_send()
        return 0

    lax.fori_loop(0, 8, drain_relay, 0)


def finish(n, z, small, res_ref, bonus_ref, acc_ref, exp_ref, buf, sem):
    drafts, vocab, _ = res_ref.shape
    off = pl.multiple_of((lax.axis_index("tp") * vocab) % LANES, 8)
    last = pltpu.make_async_copy(z.at[drafts, pl.ds(off, vocab), :], bonus_ref, sem.at[0])
    last.start()
    copies = [last]
    part = vocab // PARTS
    for i in range(drafts):
        scale = small[i:i + 1, :]
        for t in range(PARTS):
            to = pl.ds(t * part, part)
            buf[i, to, :] = z[i, pl.ds(pl.multiple_of(off + t * part, 8), part), :] * scale
            cp = pltpu.make_async_copy(buf.at[i, to], res_ref.at[i, to], sem.at[len(copies)])
            cp.start()
            copies.append(cp)
    accept = jnp.minimum(small[2:4, :] / small[4:6, :], 1.0)
    acc_ref[...] = accept
    exp_ref[...] = accept[0:1] + accept[0:1] * accept[1:2]
    for cp in copies:
        cp.wait()


def solution(mesh):
    n = mesh.shape["tp"]

    def local(hid, w, q, tok):
        rows, positions, dim = hid.shape
        vocab = w.shape[1]
        drafts = positions - 1
        batch = rows * n
        q_tiles = q.shape[2] // LANES
        width = -(-vocab // LANES) * LANES
        q_view = q.reshape(rows, drafts, q_tiles, LANES).transpose(0, 2, 1, 3)
        q_view = with_layout_constraint(q_view, Layout((0, 1, 2, 3))).reshape(-1, LANES)
        dma = pltpu.SemaphoreType.DMA
        vmem, anywhere = pl.BlockSpec(memory_space=pltpu.VMEM), pl.BlockSpec(memory_space=pltpu.HBM)
        z, small = pl.pallas_call(
            functools.partial(kernel, n),
            out_shape=(
                jax.ShapeDtypeStruct((positions, width, batch), F32),
                jax.ShapeDtypeStruct((8, batch), F32),
            ),
            in_specs=[anywhere] * 4,
            out_specs=(vmem, vmem),
            scratch_shapes=[
                pltpu.VMEM((drafts, batch), jnp.int32),
                pltpu.VMEM((positions, batch, dim), jnp.bfloat16),
                pltpu.VMEM((rows * q_tiles * drafts, LANES), F32),
                pltpu.VMEM((n - 1, drafts, rows, width), jnp.int16),
                pltpu.VMEM((drafts, batch, width), jnp.int16),
                pltpu.VMEM((2, 8, rows, width // SEGS), jnp.int16),
                pltpu.VMEM((2, vocab // STEPS, dim), jnp.bfloat16),
                pltpu.VMEM((n, 16, batch), F32),
                pltpu.VMEM((drafts, n, 8, batch), F32),
                pltpu.VMEM((drafts * (rows // 8), 8, LANES), F32),
                dma((8,)), dma((8,)), dma((2 * n,)),
                dma((7 * 8,)), dma((8 * 8,)), dma((16,)), dma((16,)),
                dma((n,)), dma((n,)), dma((2 * n,)), dma((2 * n,)),
                dma((8,)), dma((2,)),
            ],
            compiler_params=pltpu.CompilerParams(
                collective_id=0, has_side_effects=True, vmem_limit_bytes=40 * 2**20
            ),
        )(*[pltpu.with_memory_space_constraint(a, pltpu.HBM) for a in (tok.T, hid.transpose(1, 0, 2), w.T, q_view)])
        residual, bonus, accept, expected = pl.pallas_call(
            functools.partial(finish, n),
            out_shape=(
                jax.ShapeDtypeStruct((drafts, vocab, batch), F32),
                jax.ShapeDtypeStruct((vocab, batch), F32),
                jax.ShapeDtypeStruct((drafts, batch), F32),
                jax.ShapeDtypeStruct((1, batch), F32),
            ),
            in_specs=[vmem, vmem],
            out_specs=(anywhere, anywhere, vmem, vmem),
            scratch_shapes=[pltpu.VMEM((drafts, vocab, batch), F32), dma((drafts * PARTS + 1,))],
            compiler_params=pltpu.CompilerParams(vmem_limit_bytes=24 * 2**20),
        )(z, small)
        return accept.T, expected[0], residual.transpose(2, 0, 1), bonus.T

    return jax.shard_map(
        local,
        mesh=mesh,
        in_specs=(P(("dp", "tp"), None, None), P(None, "tp"), P(("dp", "tp"), None, None), P("dp", None)),
        out_specs=(P("dp", None), P("dp"), P("dp", None, "tp"), P("dp", "tp")),
        check_vma=False,
    )
```

```python
import functools

import jax
import jax.numpy as jnp
from jax import lax
from jax.experimental import pallas as pl
from jax.experimental.pallas import tpu as pltpu
from jax.experimental.layout import Layout, with_layout_constraint
from jax.sharding import PartitionSpec as P

INV_TEMP = 1.25
TOP = 65535.0
HALF = 32768
LANES = 128
SEGS = 4
STEPS = 10
PARTS = 5
F32 = jnp.float32
MESH = pl.DeviceIdType.MESH


def kernel(
    n, tok_in, hid_ref, w_ref, q_ref,
    z, small_ref,
    tok_ref, hall, stage, scode, qall, rbuf, wbuf, msgs, mass, rowc,
    h_send, h_fwd, h_recv, q_send, q_recv, r_send, r_recv,
    m_send, m_recv, x_send, x_recv, loc, wsem,
):
    k = lax.axis_index("tp")
    x, c = k // 2, k % 2
    chips = n // 2
    right, left = (x + 1) % chips, (x + chips - 1) % chips
    far = (x + 2) % chips
    mate = 2 * x + 1 - c
    positions, batch, dim = hall.shape
    drafts = positions - 1
    rows = batch // n
    vocab = w_ref.shape[0]
    width = qall.shape[2]
    seg = width // SEGS
    tiles = width // LANES
    pitch = q_ref.shape[0] // rows
    all_tiles = pitch // drafts
    off = (k * vocab) % LANES
    hcol = dim // 2
    wrows = vocab // STEPS

    def remote(src, dst, ssem, rsem, who):
        return pltpu.make_async_remote_copy(
            src_ref=src, dst_ref=dst, send_sem=ssem, recv_sem=rsem,
            device_id={"tp": who}, device_id_type=MESH,
        )

    hid_cp = pltpu.make_async_copy(hid_ref, hall.at[:, pl.ds(k * rows, rows), :], loc.at[0])
    hid_cp.start()
    tok_cp = pltpu.make_async_copy(tok_in, tok_ref, loc.at[6])
    tok_cp.start()

    def stage_cp(g):
        part = pl.ds(g * 8 * pitch, 8 * pitch)
        return pltpu.make_async_copy(q_ref.at[part], stage.at[part], loc.at[1 + g])

    for g in range(rows // 8):
        stage_cp(g).start()

    def w_cp(t, slot):
        return pltpu.make_async_copy(
            w_ref.at[pl.ds(pl.multiple_of(t * wrows, 8), wrows)], wbuf.at[slot], wsem.at[slot]
        )

    barrier = pltpu.get_barrier_semaphore()
    for p in range(1, n):
        pl.semaphore_signal(barrier, inc=1, device_id={"tp": (k + p) % n}, device_id_type=MESH)
    pl.semaphore_wait(barrier, n - 1)

    def hpiece(src, half):
        return hall.at[:, pl.ds(pl.multiple_of(src * rows, rows), rows), pl.ds(half * hcol, hcol)]

    def hcopy(src, half, ssem, who):
        return remote(hpiece(src, half), hpiece(src, half), ssem, h_recv.at[src * 2 + half], who)

    def hwait(src, half):
        hcopy(src, half, h_send.at[0], mate).wait_recv()

    hid_cp.wait()
    own_sends = []
    for idx, (who, half) in enumerate(
        [(2 * right + c, 0), (2 * left + c, 1), (2 * right + c, 1), (2 * left + c, 0), (mate, 0), (mate, 1)]
    ):
        cp = hcopy(k, half, h_send.at[idx], who)
        cp.start()
        own_sends.append(cp)
    w_cp(0, 0).start()
    w_cp(1, 1).start()

    z[:, 0:96, :] = jnp.zeros((positions, 96, batch), F32)
    z[:, width - 96:width, :] = jnp.zeros((positions, 96, batch), F32)

    tok_cp.wait()
    for g in range(rows // 8):
        stage_cp(g).wait()

    def qrows(g, i, j):
        return stage[pl.ds(g * 8 * pitch + drafts * j + i, 8, stride=pitch), :]

    groups = [(i, g) for i in range(drafts) for g in range(rows // 8)]
    lane_b = lax.broadcasted_iota(jnp.int32, (8, batch), 1)
    sub_b = lax.broadcasted_iota(jnp.int32, (8, batch), 0)
    lane_t = lax.broadcasted_iota(jnp.int32, (8, LANES), 1)
    mine = [lane_b == k * rows + 8 * g + sub_b for g in range(rows // 8)]
    tok_col = []
    for i, g in groups:
        t = jnp.where(mine[g], jnp.broadcast_to(tok_ref[i:i + 1, :].astype(F32), (8, batch)), 0.0)
        tok_col.append(jnp.broadcast_to(jnp.sum(t, axis=1, keepdims=True), (8, LANES)).astype(jnp.int32))

    def scan(j, carry):
        top, got = carry
        new_top, new_got = [], []
        col = lane_t + j * LANES
        for a, (i, g) in enumerate(groups):
            v = qrows(g, i, j)
            new_top.append(jnp.maximum(top[a], v))
            new_got.append(jnp.where(col == tok_col[a], v, got[a]))
        return tuple(new_top), tuple(new_got)

    zero8 = tuple(jnp.zeros((8, LANES), F32) for _ in groups)
    top, got = lax.fori_loop(0, all_tiles, scan, (zero8, zero8))
    qtop_row, qgot_row = [], []
    for i in range(drafts):
        acc_t = jnp.zeros((8, batch), F32)
        acc_g = jnp.zeros((8, batch), F32)
        for a, (ii, g) in enumerate(groups):
            if ii != i:
                continue
            tcol = jnp.max(top[a], axis=1, keepdims=True)
            gcol = jnp.sum(got[a], axis=1, keepdims=True)
            rowc[a] = jnp.broadcast_to(jnp.log(TOP) - 0.25 * jnp.log(tcol), (8, LANES))
            acc_t = acc_t + jnp.where(mine[g], jnp.broadcast_to(tcol, (8, batch)), 0.0)
            acc_g = acc_g + jnp.where(mine[g], jnp.broadcast_to(gcol, (8, batch)), 0.0)
        qtop_row.append(jnp.sum(acc_t, axis=0, keepdims=True))
        qgot_row.append(jnp.sum(acc_g, axis=0, keepdims=True))
    msgs[k] = jnp.zeros(msgs.shape[1:], F32)
    for i in range(drafts):
        msgs[k, 8 + i:9 + i, :] = qgot_row[i]
        msgs[k, 10 + i:11 + i, :] = qtop_row[i]

    def encode(dest, put):
        first = (dest * vocab) // LANES

        def body(j, _):
            for i in range(drafts):
                for gg in range(rows // 16):
                    parts = []
                    for g in (2 * gg, 2 * gg + 1):
                        v = qrows(g, i, first + j)
                        y = jnp.exp(0.25 * jnp.log(v) + rowc[i * (rows // 8) + g])
                        parts.append((y + 0.5).astype(jnp.int32) - HALF)
                    code = jnp.concatenate(parts, axis=0).astype(jnp.int16)
                    put(i, gg, pl.ds(pl.multiple_of(j * LANES, LANES), LANES), code)
            return 0

        lax.fori_loop(0, tiles, body, 0)

    def to_slot(r):
        def put(i, gg, cols, code):
            scode[r, i, 16 * gg:16 * gg + 16, cols] = code

        return put

    def to_self(i, gg, cols, code):
        qall[i, pl.ds(pl.multiple_of(k * rows + 16 * gg, 16), 16), cols] = code

    encode(2 * far, to_slot(0))
    encode(2 * far + 1, to_slot(1))

    fwd = []

    def forward(src, half):
        cp = hcopy(src, half, h_fwd.at[len(fwd)], mate)
        cp.start()
        fwd.append(cp)

    hwait(2 * left + c, 0)
    rel_r = hcopy(2 * left + c, 0, h_send.at[6], 2 * right + c)
    rel_r.start()
    forward(2 * left + c, 0)
    hwait(2 * right + c, 1)
    rel_l = hcopy(2 * right + c, 1, h_send.at[7], 2 * left + c)
    rel_l.start()
    forward(2 * right + c, 1)

    def unit(buf_i, i, s):
        return buf_i.at[i, :, pl.ds(pl.multiple_of(s * seg, LANES), seg)]

    def landing(src, i, s):
        return qall.at[
            i, pl.ds(pl.multiple_of(src * rows, rows), rows), pl.ds(pl.multiple_of(s * seg, LANES), seg)
        ]

    def direct(slot, i, s, who):
        return remote(
            unit(scode.at[slot], i, s), landing(k, i, s),
            q_send.at[slot * 8 + i * SEGS + s], q_recv.at[k * 8 + i * SEGS + s], who,
        )

    def out_far(way, v):
        i, s, cc = v // 4, 2 * ((v // 2) % 2) + way, v % 2
        who = 2 * (right if way == 0 else left) + c
        return remote(
            unit(scode.at[cc], i, s), rbuf.at[way, v],
            q_send.at[cc * 8 + i * SEGS + s], r_recv.at[way * 8 + v], who,
        )

    def relay(way, v):
        i, s, cc = v // 4, 2 * ((v // 2) % 2) + way, v % 2
        src = 2 * (left if way == 0 else right) + c
        who = 2 * (right if way == 0 else left) + cc
        return remote(
            rbuf.at[way, v], landing(src, i, s),
            r_send.at[way * 8 + v], q_recv.at[src * 8 + i * SEGS + s], who,
        )

    def near(way, u):
        i, s, cc = u // 8, (u // 2) % SEGS, u % 2
        who = 2 * (right if way == 0 else left) + cc
        return direct(2 + 2 * way + cc, i, s, who)

    def send_far(v):
        out_far(0, v).start()
        out_far(1, v).start()

    def send_near(u):
        near(0, u).start()
        near(1, u).start()

    def pass_on(v):
        for way in range(2):
            out_far(way, v).wait_recv()
            relay(way, v).start()

    encode(2 * right, to_slot(2))
    encode(2 * right + 1, to_slot(3))
    encode(2 * left, to_slot(4))
    encode(2 * left + 1, to_slot(5))

    hwait(2 * left + c, 1)
    forward(2 * left + c, 1)
    hwait(2 * right + c, 0)
    forward(2 * right + c, 0)

    def first_far(v, _):
        send_far(v)
        return 0

    def first_near(u, _):
        send_near(u)
        return 0

    lax.fori_loop(0, 4, first_far, 0)
    lax.fori_loop(0, 8, first_near, 0)
    encode(mate, to_slot(6))
    encode(k, to_self)

    def to_mate(u, _):
        direct(6, u // SEGS, u % SEGS, mate).start()
        return 0

    lax.fori_loop(0, drafts * SEGS, to_mate, 0)

    hwait(2 * far + c, 0)
    forward(2 * far + c, 0)
    hwait(2 * far + c, 1)
    forward(2 * far + c, 1)
    for chip in (x, left, right, far):
        for half in range(2):
            hwait(2 * chip + 1 - c, half)

    def step(t, top):
        slot = t % 2

        @pl.when((t >= 2) & (t < 4))
        def _():
            pass_on(2 * (t - 2))
            pass_on(2 * (t - 2) + 1)

        @pl.when((t >= 4) & (t < 6))
        def _():
            send_far(4 + 2 * (t - 4))
            send_far(4 + 2 * (t - 4) + 1)

        @pl.when(t >= 6)
        def _():
            send_near(8 + 2 * (t - 6))
            send_near(8 + 2 * (t - 6) + 1)

        @pl.when(t >= STEPS - 2)
        def _():
            pass_on(4 + 2 * (t - (STEPS - 2)))
            pass_on(4 + 2 * (t - (STEPS - 2)) + 1)

        w_cp(t, slot).wait()
        prod = INV_TEMP * lax.dot_general(
            wbuf[slot], hall[...].reshape(positions * batch, dim), (((1,), (1,)), ((), ())), preferred_element_type=F32
        )
        base = pl.multiple_of(off + t * wrows, 8)
        for i in range(positions):
            z[i, pl.ds(base, wrows), :] = prod[:, i * batch:(i + 1) * batch]

        @pl.when(t + 2 < STEPS)
        def _():
            w_cp(t + 2, slot).start()

        return jnp.maximum(top, jnp.max(prod.reshape(wrows // 8, 8, positions * batch), axis=0))

    top = lax.fori_loop(0, STEPS, step, jnp.full((8, positions * batch), -jnp.inf, F32))
    own_max = jnp.max(top, axis=0, keepdims=True)

    chunk = 160
    row_i = lax.broadcasted_iota(jnp.int32, (chunk, batch), 0)
    for i in range(positions):
        m_i = own_max[:, i * batch:(i + 1) * batch]
        want = tok_ref[i:i + 1, :] - k * vocab if i < drafts else None

        def expo(t, carry, i=i, m_i=m_i, want=want):
            total, got = carry
            at = pl.ds(pl.multiple_of(off + t * chunk, 8), chunk)
            e = jnp.exp(z[i, at, :] - m_i)
            z[i, at, :] = e
            total = total + jnp.sum(e.reshape(chunk // 8, 8, batch), axis=0)
            if want is not None:
                pick = jnp.where(row_i + t * chunk == want, e, 0.0)
                got = got + jnp.sum(pick.reshape(chunk // 8, 8, batch), axis=0)
            return total, got

        zero = jnp.zeros((8, batch), F32)
        total, got = lax.fori_loop(0, vocab // chunk, expo, (zero, zero))
        msgs[k, i:i + 1, :] = m_i
        msgs[k, 3 + i:4 + i, :] = jnp.sum(total, axis=0, keepdims=True)
        if i < drafts:
            msgs[k, 6 + i:7 + i, :] = jnp.sum(got, axis=0, keepdims=True)

    def msg(p, src):
        return remote(msgs.at[src], msgs.at[src], m_send.at[p], m_recv.at[src], (k + p) % n)

    for p in range(1, n):
        msg(p, k).start()

    for p in range(1, n):
        msg(p, (k + p) % n).wait_recv()

    allm = msgs[...]
    peak = jnp.max(allm[:, 0:3, :], axis=0)
    part = jnp.exp(allm[:, 0:3, :] - peak[None])
    inv = 1.0 / jnp.sum(part * allm[:, 3:6, :], axis=0)
    p_pick = jnp.sum(part[:, 0:drafts, :] * allm[:, 6:8, :], axis=0) * inv[0:drafts]
    q_pick = jnp.sum(allm[:, 8:10, :], axis=0)
    q_scale = jnp.sum(allm[:, 10:12, :], axis=0) * (1.0 / (TOP * TOP * TOP * TOP))
    fac = jnp.exp(msgs[k, 0:3, :] - peak) * inv

    def scale(t, _):
        at = pl.ds(pl.multiple_of(off + t * chunk, 8), chunk)
        z[drafts, at, :] = z[drafts, at, :] * fac[drafts:drafts + 1, :]
        return 0

    lax.fori_loop(0, vocab // chunk, scale, 0)

    def xmsg(p, i, src):
        return remote(mass.at[i, src], mass.at[i, src], x_send.at[i * n + p], x_recv.at[i * n + src], (k + p) % n)

    for i in range(drafts):
        acc = [jnp.zeros((8, LANES), F32) for _ in range(batch // LANES)]
        for s in range(SEGS):
            for p in range(1, n):
                src = (k + p) % n
                remote(
                    landing(src, i, s), landing(src, i, s), q_send.at[0],
                    q_recv.at[src * 8 + i * SEGS + s], mate,
                ).wait_recv()

            def body(t, acc, i=i, s=s):
                at = pl.ds(pl.multiple_of((s * (tiles // SEGS) + t) * LANES, LANES), LANES)
                out = []
                for h in range(batch // LANES):
                    ls = slice(h * LANES, (h + 1) * LANES)
                    code = qall[i, ls, at].astype(jnp.int32).astype(F32)
                    y = code.T + float(HALF)
                    y = y * y
                    qt = y * y * q_scale[i:i + 1, ls]
                    ex = jnp.maximum(z[i, at, ls] * fac[i:i + 1, ls] - qt, 0.0)
                    z[i, at, ls] = ex
                    out.append(acc[h] + jnp.sum(ex.reshape(LANES // 8, 8, LANES), axis=0))
                return tuple(out)

            acc = lax.fori_loop(0, tiles // SEGS, body, tuple(acc))
        for h in range(batch // LANES):
            mass[i, k, :, h * LANES:(h + 1) * LANES] = acc[h]
        for p in range(1, n):
            xmsg(p, i, k).start()
    small_ref[...] = jnp.zeros(small_ref.shape, F32)
    small_ref[2:4, :] = p_pick
    small_ref[4:6, :] = q_pick
    for i in range(drafts):
        for p in range(1, n):
            xmsg(p, i, (k + p) % n).wait_recv()
        total = jnp.sum(jnp.sum(mass[i], axis=0), axis=0, keepdims=True)
        small_ref[i:i + 1, :] = 1.0 / total

    for cp in own_sends + [rel_r, rel_l] + fwd:
        cp.wait_send()
    for p in range(1, n):
        msg(p, k).wait_send()
        for i in range(drafts):
            xmsg(p, i, k).wait_send()

    def drain(u, _):
        direct(u // 8, (u % 8) // SEGS, u % SEGS, mate).wait_send()
        return 0

    lax.fori_loop(0, 7 * 8, drain, 0)

    def drain_relay(v, _):
        relay(0, v).wait_send()
        relay(1, v).wait_send()
        return 0

    lax.fori_loop(0, 8, drain_relay, 0)


def finish(n, z, small, res_ref, bonus_ref, acc_ref, exp_ref, buf, sem):
    drafts, vocab, _ = res_ref.shape
    off = pl.multiple_of((lax.axis_index("tp") * vocab) % LANES, 8)
    last = pltpu.make_async_copy(z.at[drafts, pl.ds(off, vocab), :], bonus_ref, sem.at[0])
    last.start()
    copies = [last]
    part = vocab // PARTS
    for i in range(drafts):
        scale = small[i:i + 1, :]
        for t in range(PARTS):
            to = pl.ds(t * part, part)
            buf[i, to, :] = z[i, pl.ds(pl.multiple_of(off + t * part, 8), part), :] * scale
            cp = pltpu.make_async_copy(buf.at[i, to], res_ref.at[i, to], sem.at[len(copies)])
            cp.start()
            copies.append(cp)
    accept = jnp.minimum(small[2:4, :] / small[4:6, :], 1.0)
    acc_ref[...] = accept
    exp_ref[...] = accept[0:1] + accept[0:1] * accept[1:2]
    for cp in copies:
        cp.wait()


def solution(mesh):
    n = mesh.shape["tp"]

    def local(hid, w, q, tok):
        rows, positions, dim = hid.shape
        vocab = w.shape[1]
        drafts = positions - 1
        batch = rows * n
        q_tiles = q.shape[2] // LANES
        width = -(-vocab // LANES) * LANES
        q_view = q.reshape(rows, drafts, q_tiles, LANES).transpose(0, 2, 1, 3)
        q_view = with_layout_constraint(q_view, Layout((0, 1, 2, 3))).reshape(-1, LANES)
        dma = pltpu.SemaphoreType.DMA
        vmem, anywhere = pl.BlockSpec(memory_space=pltpu.VMEM), pl.BlockSpec(memory_space=pltpu.HBM)
        z, small = pl.pallas_call(
            functools.partial(kernel, n),
            out_shape=(
                jax.ShapeDtypeStruct((positions, width, batch), F32),
                jax.ShapeDtypeStruct((8, batch), F32),
            ),
            in_specs=[anywhere] * 4,
            out_specs=(vmem, vmem),
            scratch_shapes=[
                pltpu.VMEM((drafts, batch), jnp.int32),
                pltpu.VMEM((positions, batch, dim), jnp.bfloat16),
                pltpu.VMEM((rows * q_tiles * drafts, LANES), F32),
                pltpu.VMEM((n - 1, drafts, rows, width), jnp.int16),
                pltpu.VMEM((drafts, batch, width), jnp.int16),
                pltpu.VMEM((2, 8, rows, width // SEGS), jnp.int16),
                pltpu.VMEM((2, vocab // STEPS, dim), jnp.bfloat16),
                pltpu.VMEM((n, 16, batch), F32),
                pltpu.VMEM((drafts, n, 8, batch), F32),
                pltpu.VMEM((drafts * (rows // 8), 8, LANES), F32),
                dma((8,)), dma((8,)), dma((2 * n,)),
                dma((7 * 8,)), dma((8 * 8,)), dma((16,)), dma((16,)),
                dma((n,)), dma((n,)), dma((2 * n,)), dma((2 * n,)),
                dma((8,)), dma((2,)),
            ],
            compiler_params=pltpu.CompilerParams(
                collective_id=0, has_side_effects=True, vmem_limit_bytes=40 * 2**20
            ),
        )(*[pltpu.with_memory_space_constraint(a, pltpu.HBM) for a in (tok.T, hid.transpose(1, 0, 2), w.T, q_view)])
        residual, bonus, accept, expected = pl.pallas_call(
            functools.partial(finish, n),
            out_shape=(
                jax.ShapeDtypeStruct((drafts, vocab, batch), F32),
                jax.ShapeDtypeStruct((vocab, batch), F32),
                jax.ShapeDtypeStruct((drafts, batch), F32),
                jax.ShapeDtypeStruct((1, batch), F32),
            ),
            in_specs=[vmem, vmem],
            out_specs=(anywhere, anywhere, vmem, vmem),
            scratch_shapes=[pltpu.VMEM((drafts, vocab, batch), F32), dma((drafts * PARTS + 1,))],
            compiler_params=pltpu.CompilerParams(vmem_limit_bytes=24 * 2**20),
        )(z, small)
        return accept.T, expected[0], residual.transpose(2, 0, 1), bonus.T

    return jax.shard_map(
        local,
        mesh=mesh,
        in_specs=(P(("dp", "tp"), None, None), P(None, "tp"), P(("dp", "tp"), None, None), P("dp", None)),
        out_specs=(P("dp", None), P("dp"), P("dp", None, "tp"), P("dp", "tp")),
        check_vma=False,
    )
```

```python
import functools

import jax
import jax.numpy as jnp
from jax import lax
from jax.experimental import pallas as pl
from jax.experimental.pallas import tpu as pltpu
from jax.experimental.layout import Layout, with_layout_constraint
from jax.sharding import PartitionSpec as P

INV_TEMP = 1.25
TOP = 65535.0
HALF = 32768
LANES = 128
SEGS = 4
STEPS = 10
PARTS = 5
F32 = jnp.float32
MESH = pl.DeviceIdType.MESH


def kernel(
    n, tok_in, hid_ref, w_ref, q_ref,
    z, small_ref,
    tok_ref, hall, stage, scode, qall, rbuf, wbuf, msgs, mass, rowc,
    h_send, h_fwd, h_recv, q_send, q_recv, r_send, r_recv,
    m_send, m_recv, x_send, x_recv, loc, wsem,
):
    k = lax.axis_index("tp")
    x, c = k // 2, k % 2
    chips = n // 2
    right, left = (x + 1) % chips, (x + chips - 1) % chips
    far = (x + 2) % chips
    mate = 2 * x + 1 - c
    positions, batch, dim = hall.shape
    drafts = positions - 1
    rows = batch // n
    vocab = w_ref.shape[0]
    seg = qall.shape[3]
    width = seg * SEGS
    tiles = width // LANES
    per = seg // LANES
    pitch = q_ref.shape[0] // rows
    all_tiles = pitch // drafts
    off = (k * vocab) % LANES
    hcol = dim // 2
    wrows = vocab // STEPS

    def remote(src, dst, ssem, rsem, who):
        return pltpu.make_async_remote_copy(
            src_ref=src, dst_ref=dst, send_sem=ssem, recv_sem=rsem,
            device_id={"tp": who}, device_id_type=MESH,
        )

    hid_cp = pltpu.make_async_copy(hid_ref, hall.at[:, pl.ds(k * rows, rows), :], loc.at[0])
    hid_cp.start()
    tok_cp = pltpu.make_async_copy(tok_in, tok_ref, loc.at[6])
    tok_cp.start()

    def stage_cp(g):
        part = pl.ds(g * 8 * pitch, 8 * pitch)
        return pltpu.make_async_copy(q_ref.at[part], stage.at[part], loc.at[1 + g])

    for g in range(rows // 8):
        stage_cp(g).start()

    def w_cp(t, slot):
        return pltpu.make_async_copy(
            w_ref.at[pl.ds(pl.multiple_of(t * wrows, 8), wrows)], wbuf.at[slot], wsem.at[slot]
        )

    barrier = pltpu.get_barrier_semaphore()
    for p in range(1, n):
        pl.semaphore_signal(barrier, inc=1, device_id={"tp": (k + p) % n}, device_id_type=MESH)
    pl.semaphore_wait(barrier, n - 1)

    def hpiece(src, half):
        return hall.at[:, pl.ds(pl.multiple_of(src * rows, rows), rows), pl.ds(half * hcol, hcol)]

    def hcopy(src, half, ssem, who):
        return remote(hpiece(src, half), hpiece(src, half), ssem, h_recv.at[src * 2 + half], who)

    def hwait(src, half):
        hcopy(src, half, h_send.at[0], mate).wait_recv()

    hid_cp.wait()
    own_sends = []
    for idx, (who, half) in enumerate(
        [(2 * right + c, 0), (2 * left + c, 1), (2 * right + c, 1), (2 * left + c, 0), (mate, 0), (mate, 1)]
    ):
        cp = hcopy(k, half, h_send.at[idx], who)
        cp.start()
        own_sends.append(cp)
    w_cp(0, 0).start()
    w_cp(1, 1).start()

    z[:, 0:96, :] = jnp.zeros((positions, 96, batch), F32)
    z[:, width - 96:width, :] = jnp.zeros((positions, 96, batch), F32)

    tok_cp.wait()
    for g in range(rows // 8):
        stage_cp(g).wait()

    def qrows(g, i, j):
        return stage[pl.ds(g * 8 * pitch + drafts * j + i, 8, stride=pitch), :]

    groups = [(i, g) for i in range(drafts) for g in range(rows // 8)]
    lane_b = lax.broadcasted_iota(jnp.int32, (8, batch), 1)
    sub_b = lax.broadcasted_iota(jnp.int32, (8, batch), 0)
    lane_t = lax.broadcasted_iota(jnp.int32, (8, LANES), 1)
    mine = [lane_b == k * rows + 8 * g + sub_b for g in range(rows // 8)]
    tok_col = []
    for i, g in groups:
        t = jnp.where(mine[g], jnp.broadcast_to(tok_ref[i:i + 1, :].astype(F32), (8, batch)), 0.0)
        tok_col.append(jnp.broadcast_to(jnp.sum(t, axis=1, keepdims=True), (8, LANES)).astype(jnp.int32))

    def scan(j, carry):
        top, got = carry
        new_top, new_got = [], []
        col = lane_t + j * LANES
        for a, (i, g) in enumerate(groups):
            v = qrows(g, i, j)
            new_top.append(jnp.maximum(top[a], v))
            new_got.append(jnp.where(col == tok_col[a], v, got[a]))
        return tuple(new_top), tuple(new_got)

    zero8 = tuple(jnp.zeros((8, LANES), F32) for _ in groups)
    top, got = lax.fori_loop(0, all_tiles, scan, (zero8, zero8))
    qtop_row, qgot_row = [], []
    for i in range(drafts):
        acc_t = jnp.zeros((8, batch), F32)
        acc_g = jnp.zeros((8, batch), F32)
        for a, (ii, g) in enumerate(groups):
            if ii != i:
                continue
            tcol = jnp.max(top[a], axis=1, keepdims=True)
            gcol = jnp.sum(got[a], axis=1, keepdims=True)
            rowc[a] = jnp.broadcast_to(jnp.log(TOP) - 0.25 * jnp.log(tcol), (8, LANES))
            acc_t = acc_t + jnp.where(mine[g], jnp.broadcast_to(tcol, (8, batch)), 0.0)
            acc_g = acc_g + jnp.where(mine[g], jnp.broadcast_to(gcol, (8, batch)), 0.0)
        qtop_row.append(jnp.sum(acc_t, axis=0, keepdims=True))
        qgot_row.append(jnp.sum(acc_g, axis=0, keepdims=True))
    msgs[k] = jnp.zeros(msgs.shape[1:], F32)
    for i in range(drafts):
        msgs[k, 8 + i:9 + i, :] = qgot_row[i]
        msgs[k, 10 + i:11 + i, :] = qtop_row[i]

    def encode(dest, put):
        first = (dest * vocab) // LANES

        def body(j, _):
            for i in range(drafts):
                for gg in range(rows // 16):
                    parts = []
                    for g in (2 * gg, 2 * gg + 1):
                        v = qrows(g, i, first + j)
                        y = jnp.exp(0.25 * jnp.log(v) + rowc[i * (rows // 8) + g])
                        parts.append((y + 0.5).astype(jnp.int32) - HALF)
                    code = jnp.concatenate(parts, axis=0).astype(jnp.int16)
                    put(i, gg, j // per, pl.ds(pl.multiple_of((j % per) * LANES, LANES), LANES), code)
            return 0

        lax.fori_loop(0, tiles, body, 0)

    def to_slot(r):
        def put(i, gg, s, cols, code):
            scode[r, i, s, 16 * gg:16 * gg + 16, cols] = code

        return put

    def to_self(i, gg, s, cols, code):
        qall[i, s, pl.ds(pl.multiple_of(k * rows + 16 * gg, 16), 16), cols] = code

    encode(2 * far, to_slot(0))
    encode(2 * far + 1, to_slot(1))

    fwd = []

    def forward(src, half):
        cp = hcopy(src, half, h_fwd.at[len(fwd)], mate)
        cp.start()
        fwd.append(cp)

    hwait(2 * left + c, 0)
    rel_r = hcopy(2 * left + c, 0, h_send.at[6], 2 * right + c)
    rel_r.start()
    forward(2 * left + c, 0)
    hwait(2 * right + c, 1)
    rel_l = hcopy(2 * right + c, 1, h_send.at[7], 2 * left + c)
    rel_l.start()
    forward(2 * right + c, 1)

    def unit(buf_i, i, s):
        return buf_i.at[i, s]

    def landing(src, i, s):
        return qall.at[i, s, pl.ds(pl.multiple_of(src * rows, rows), rows)]

    def direct(slot, i, s, who):
        return remote(
            unit(scode.at[slot], i, s), landing(k, i, s),
            q_send.at[slot * 8 + i * SEGS + s], q_recv.at[k * 8 + i * SEGS + s], who,
        )

    def out_far(way, v):
        i, s, cc = v // 4, 2 * ((v // 2) % 2) + way, v % 2
        who = 2 * (right if way == 0 else left) + c
        return remote(
            unit(scode.at[cc], i, s), rbuf.at[way, v],
            q_send.at[cc * 8 + i * SEGS + s], r_recv.at[way * 8 + v], who,
        )

    def relay(way, v):
        i, s, cc = v // 4, 2 * ((v // 2) % 2) + way, v % 2
        src = 2 * (left if way == 0 else right) + c
        who = 2 * (right if way == 0 else left) + cc
        return remote(
            rbuf.at[way, v], landing(src, i, s),
            r_send.at[way * 8 + v], q_recv.at[src * 8 + i * SEGS + s], who,
        )

    def near(way, u):
        i, s, cc = u // 8, (u // 2) % SEGS, u % 2
        who = 2 * (right if way == 0 else left) + cc
        return direct(2 + 2 * way + cc, i, s, who)

    def send_far(v):
        out_far(0, v).start()
        out_far(1, v).start()

    def send_near(u):
        near(0, u).start()
        near(1, u).start()

    def pass_on(v):
        for way in range(2):
            out_far(way, v).wait_recv()
            relay(way, v).start()

    encode(2 * right, to_slot(2))
    encode(2 * right + 1, to_slot(3))
    encode(2 * left, to_slot(4))
    encode(2 * left + 1, to_slot(5))

    hwait(2 * left + c, 1)
    forward(2 * left + c, 1)
    hwait(2 * right + c, 0)
    forward(2 * right + c, 0)

    def first_far(v, _):
        send_far(v)
        return 0

    def first_near(u, _):
        send_near(u)
        return 0

    lax.fori_loop(0, 4, first_far, 0)
    lax.fori_loop(0, 8, first_near, 0)
    encode(mate, to_slot(6))
    encode(k, to_self)

    def to_mate(u, _):
        direct(6, u // SEGS, u % SEGS, mate).start()
        return 0

    lax.fori_loop(0, drafts * SEGS, to_mate, 0)

    hwait(2 * far + c, 0)
    forward(2 * far + c, 0)
    hwait(2 * far + c, 1)
    forward(2 * far + c, 1)
    for chip in (x, left, right, far):
        for half in range(2):
            hwait(2 * chip + 1 - c, half)

    def step(t, top):
        slot = t % 2

        @pl.when((t >= 2) & (t < 4))
        def _():
            pass_on(2 * (t - 2))
            pass_on(2 * (t - 2) + 1)

        @pl.when((t >= 4) & (t < 6))
        def _():
            send_far(4 + 2 * (t - 4))
            send_far(4 + 2 * (t - 4) + 1)

        @pl.when(t >= 6)
        def _():
            send_near(8 + 2 * (t - 6))
            send_near(8 + 2 * (t - 6) + 1)

        w_cp(t, slot).wait()
        prod = INV_TEMP * lax.dot_general(
            wbuf[slot], hall[...].reshape(positions * batch, dim), (((1,), (1,)), ((), ())), preferred_element_type=F32
        )
        base = pl.multiple_of(off + t * wrows, 8)
        for i in range(positions):
            z[i, pl.ds(base, wrows), :] = prod[:, i * batch:(i + 1) * batch]

        @pl.when(t + 2 < STEPS)
        def _():
            w_cp(t + 2, slot).start()

        return jnp.maximum(top, jnp.max(prod.reshape(wrows // 8, 8, positions * batch), axis=0))

    top = lax.fori_loop(0, STEPS, step, jnp.full((8, positions * batch), -jnp.inf, F32))
    own_max = jnp.max(top, axis=0, keepdims=True)

    chunk = 160
    row_i = lax.broadcasted_iota(jnp.int32, (chunk, batch), 0)
    for i in range(positions):
        m_i = own_max[:, i * batch:(i + 1) * batch]
        want = tok_ref[i:i + 1, :] - k * vocab if i < drafts else None

        def expo(t, carry, i=i, m_i=m_i, want=want):
            total, got = carry
            at = pl.ds(pl.multiple_of(off + t * chunk, 8), chunk)
            e = jnp.exp(z[i, at, :] - m_i)
            z[i, at, :] = e
            total = total + jnp.sum(e.reshape(chunk // 8, 8, batch), axis=0)
            if want is not None:
                pick = jnp.where(row_i + t * chunk == want, e, 0.0)
                got = got + jnp.sum(pick.reshape(chunk // 8, 8, batch), axis=0)
            return total, got

        zero = jnp.zeros((8, batch), F32)
        total, got = lax.fori_loop(0, vocab // chunk, expo, (zero, zero))
        msgs[k, i:i + 1, :] = m_i
        msgs[k, 3 + i:4 + i, :] = jnp.sum(total, axis=0, keepdims=True)
        if i < drafts:
            msgs[k, 6 + i:7 + i, :] = jnp.sum(got, axis=0, keepdims=True)

    def msg(p, src):
        return remote(msgs.at[src], msgs.at[src], m_send.at[p], m_recv.at[src], (k + p) % n)

    for p in range(1, n):
        msg(p, k).start()

    for v in range(4, 8):
        pass_on(v)
    for p in range(1, n):
        msg(p, (k + p) % n).wait_recv()

    allm = msgs[...]
    peak = jnp.max(allm[:, 0:3, :], axis=0)
    part = jnp.exp(allm[:, 0:3, :] - peak[None])
    inv = 1.0 / jnp.sum(part * allm[:, 3:6, :], axis=0)
    p_pick = jnp.sum(part[:, 0:drafts, :] * allm[:, 6:8, :], axis=0) * inv[0:drafts]
    q_pick = jnp.sum(allm[:, 8:10, :], axis=0)
    q_scale = jnp.sum(allm[:, 10:12, :], axis=0) * (1.0 / (TOP * TOP * TOP * TOP))
    fac = jnp.exp(msgs[k, 0:3, :] - peak) * inv

    def scale(t, _):
        at = pl.ds(pl.multiple_of(off + t * chunk, 8), chunk)
        z[drafts, at, :] = z[drafts, at, :] * fac[drafts:drafts + 1, :]
        return 0

    lax.fori_loop(0, vocab // chunk, scale, 0)

    def xmsg(p, i, src):
        return remote(mass.at[i, src], mass.at[i, src], x_send.at[i * n + p], x_recv.at[i * n + src], (k + p) % n)

    def drain(u, _):
        direct(u // 8, (u % 8) // SEGS, u % SEGS, mate).wait_send()
        return 0

    def drain_relay(v, _):
        relay(0, v).wait_send()
        relay(1, v).wait_send()
        return 0

    for i in range(drafts):
        acc = [jnp.zeros((8, LANES), F32) for _ in range(batch // LANES)]
        for s in range(SEGS):
            if i == drafts - 1 and s == SEGS - 1:
                for cp in own_sends + [rel_r, rel_l] + fwd:
                    cp.wait_send()
                for p in range(1, n):
                    msg(p, k).wait_send()
                lax.fori_loop(0, 7 * 8, drain, 0)
            for p in range(1, n):
                src = (k + p) % n
                remote(
                    landing(src, i, s), landing(src, i, s), q_send.at[0],
                    q_recv.at[src * 8 + i * SEGS + s], mate,
                ).wait_recv()

            def body(t, acc, i=i, s=s):
                at = pl.ds(pl.multiple_of((s * (tiles // SEGS) + t) * LANES, LANES), LANES)
                out = []
                for h in range(batch // LANES):
                    ls = slice(h * LANES, (h + 1) * LANES)
                    code = qall[i, s, ls, pl.ds(pl.multiple_of(t * LANES, LANES), LANES)].astype(jnp.int32).astype(F32)
                    y = code.T + float(HALF)
                    y = y * y
                    qt = y * y * q_scale[i:i + 1, ls]
                    ex = jnp.maximum(z[i, at, ls] * fac[i:i + 1, ls] - qt, 0.0)
                    z[i, at, ls] = ex
                    out.append(acc[h] + jnp.sum(ex.reshape(LANES // 8, 8, LANES), axis=0))
                return tuple(out)

            acc = lax.fori_loop(0, tiles // SEGS, body, tuple(acc))
        for h in range(batch // LANES):
            mass[i, k, :, h * LANES:(h + 1) * LANES] = acc[h]
        for p in range(1, n):
            xmsg(p, i, k).start()
    lax.fori_loop(0, 8, drain_relay, 0)
    small_ref[...] = jnp.zeros(small_ref.shape, F32)
    small_ref[2:4, :] = p_pick
    small_ref[4:6, :] = q_pick
    for i in range(drafts):
        for p in range(1, n):
            xmsg(p, i, (k + p) % n).wait_recv()
        total = jnp.sum(jnp.sum(mass[i], axis=0), axis=0, keepdims=True)
        small_ref[i:i + 1, :] = 1.0 / total

    for p in range(1, n):
        for i in range(drafts):
            xmsg(p, i, k).wait_send()


def finish(n, z, small, res_ref, bonus_ref, acc_ref, exp_ref, buf, sem):
    drafts, vocab, _ = res_ref.shape
    off = pl.multiple_of((lax.axis_index("tp") * vocab) % LANES, 8)
    last = pltpu.make_async_copy(z.at[drafts, pl.ds(off, vocab), :], bonus_ref, sem.at[0])
    last.start()
    copies = [last]
    part = vocab // PARTS
    for i in range(drafts):
        scale = small[i:i + 1, :]
        for t in range(PARTS):
            to = pl.ds(t * part, part)
            buf[i, to, :] = z[i, pl.ds(pl.multiple_of(off + t * part, 8), part), :] * scale
            cp = pltpu.make_async_copy(buf.at[i, to], res_ref.at[i, to], sem.at[len(copies)])
            cp.start()
            copies.append(cp)
    accept = jnp.minimum(small[2:4, :] / small[4:6, :], 1.0)
    acc_ref[...] = accept
    exp_ref[...] = accept[0:1] + accept[0:1] * accept[1:2]
    for cp in copies:
        cp.wait()


def solution(mesh):
    n = mesh.shape["tp"]

    def local(hid, w, q, tok):
        rows, positions, dim = hid.shape
        vocab = w.shape[1]
        drafts = positions - 1
        batch = rows * n
        q_tiles = q.shape[2] // LANES
        width = -(-vocab // LANES) * LANES
        q_view = q.reshape(rows, drafts, q_tiles, LANES).transpose(0, 2, 1, 3)
        q_view = with_layout_constraint(q_view, Layout((0, 1, 2, 3))).reshape(-1, LANES)
        dma = pltpu.SemaphoreType.DMA
        vmem, anywhere = pl.BlockSpec(memory_space=pltpu.VMEM), pl.BlockSpec(memory_space=pltpu.HBM)
        z, small = pl.pallas_call(
            functools.partial(kernel, n),
            out_shape=(
                jax.ShapeDtypeStruct((positions, width, batch), F32),
                jax.ShapeDtypeStruct((8, batch), F32),
            ),
            in_specs=[anywhere] * 4,
            out_specs=(vmem, vmem),
            scratch_shapes=[
                pltpu.VMEM((drafts, batch), jnp.int32),
                pltpu.VMEM((positions, batch, dim), jnp.bfloat16),
                pltpu.VMEM((rows * q_tiles * drafts, LANES), F32),
                pltpu.VMEM((n - 1, drafts, SEGS, rows, width // SEGS), jnp.int16),
                pltpu.VMEM((drafts, SEGS, batch, width // SEGS), jnp.int16),
                pltpu.VMEM((2, 8, rows, width // SEGS), jnp.int16),
                pltpu.VMEM((2, vocab // STEPS, dim), jnp.bfloat16),
                pltpu.VMEM((n, 16, batch), F32),
                pltpu.VMEM((drafts, n, 8, batch), F32),
                pltpu.VMEM((drafts * (rows // 8), 8, LANES), F32),
                dma((8,)), dma((8,)), dma((2 * n,)),
                dma((7 * 8,)), dma((8 * 8,)), dma((16,)), dma((16,)),
                dma((n,)), dma((n,)), dma((2 * n,)), dma((2 * n,)),
                dma((8,)), dma((2,)),
            ],
            compiler_params=pltpu.CompilerParams(
                collective_id=0, has_side_effects=True, vmem_limit_bytes=40 * 2**20
            ),
        )(*[pltpu.with_memory_space_constraint(a, pltpu.HBM) for a in (tok.T, hid.transpose(1, 0, 2), w.T, q_view)])
        residual, bonus, accept, expected = pl.pallas_call(
            functools.partial(finish, n),
            out_shape=(
                jax.ShapeDtypeStruct((drafts, vocab, batch), F32),
                jax.ShapeDtypeStruct((vocab, batch), F32),
                jax.ShapeDtypeStruct((drafts, batch), F32),
                jax.ShapeDtypeStruct((1, batch), F32),
            ),
            in_specs=[vmem, vmem],
            out_specs=(anywhere, anywhere, vmem, vmem),
            scratch_shapes=[pltpu.VMEM((drafts, vocab, batch), F32), dma((drafts * PARTS + 1,))],
            compiler_params=pltpu.CompilerParams(vmem_limit_bytes=24 * 2**20),
        )(z, small)
        return accept.T, expected[0], residual.transpose(2, 0, 1), bonus.T

    return jax.shard_map(
        local,
        mesh=mesh,
        in_specs=(P(("dp", "tp"), None, None), P(None, "tp"), P(("dp", "tp"), None, None), P("dp", None)),
        out_specs=(P("dp", None), P("dp"), P("dp", None, "tp"), P("dp", "tp")),
        check_vma=False,
    )
```

```python
import functools

import jax
import jax.numpy as jnp
from jax import lax
from jax.experimental import pallas as pl
from jax.experimental.pallas import tpu as pltpu
from jax.experimental.layout import Layout, with_layout_constraint
from jax.sharding import PartitionSpec as P

INV_TEMP = 1.25
TOP = 65535.0
HALF = 32768
LANES = 128
SEGS = 4
STEPS = 10
PARTS = 5
F32 = jnp.float32
MESH = pl.DeviceIdType.MESH


def kernel(
    n, tok_in, hid_ref, w_ref, q_ref,
    z, small_ref,
    tok_ref, hall, stage, scode, qall, rbuf, wbuf, msgs, mass, rowc,
    h_send, h_fwd, h_recv, q_send, q_recv, r_send, r_recv,
    m_send, m_recv, x_send, x_recv, loc, wsem,
):
    k = lax.axis_index("tp")
    x, c = k // 2, k % 2
    chips = n // 2
    right, left = (x + 1) % chips, (x + chips - 1) % chips
    far = (x + 2) % chips
    mate = 2 * x + 1 - c
    positions, batch, dim = hall.shape
    drafts = positions - 1
    rows = batch // n
    vocab = w_ref.shape[0]
    seg = qall.shape[3]
    width = seg * SEGS
    tiles = width // LANES
    units = drafts * SEGS
    per = seg // LANES
    pitch = q_ref.shape[0] // rows
    all_tiles = pitch // drafts
    off = (k * vocab) % LANES
    hcol = dim // 2
    wrows = vocab // STEPS

    def remote(src, dst, ssem, rsem, who):
        return pltpu.make_async_remote_copy(
            src_ref=src, dst_ref=dst, send_sem=ssem, recv_sem=rsem,
            device_id={"tp": who}, device_id_type=MESH,
        )

    hid_cp = pltpu.make_async_copy(hid_ref, hall.at[:, pl.ds(k * rows, rows), :], loc.at[0])
    hid_cp.start()
    tok_cp = pltpu.make_async_copy(tok_in, tok_ref, loc.at[6])
    tok_cp.start()

    def stage_cp(g):
        part = pl.ds(g * 8 * pitch, 8 * pitch)
        return pltpu.make_async_copy(q_ref.at[part], stage.at[part], loc.at[1 + g])

    def w_cp(t, slot):
        return pltpu.make_async_copy(
            w_ref.at[pl.ds(pl.multiple_of(t * wrows, 8), wrows)], wbuf.at[slot], wsem.at[slot]
        )

    barrier = pltpu.get_barrier_semaphore()
    for who in (2 * right + c, 2 * left + c, mate):
        pl.semaphore_signal(barrier, inc=1, device_id={"tp": who}, device_id_type=MESH)
    pl.semaphore_wait(barrier, 3)

    def hpiece(src, half):
        return hall.at[:, pl.ds(pl.multiple_of(src * rows, rows), rows), pl.ds(half * hcol, hcol)]

    def hcopy(src, half, ssem, who):
        return remote(hpiece(src, half), hpiece(src, half), ssem, h_recv.at[src * 2 + half], who)

    def hwait(src, half):
        hcopy(src, half, h_send.at[0], mate).wait_recv()

    hid_cp.wait()
    own_sends = []
    for idx, (who, half) in enumerate(
        [(2 * right + c, 0), (2 * left + c, 1), (2 * right + c, 1), (2 * left + c, 0), (mate, 0), (mate, 1)]
    ):
        cp = hcopy(k, half, h_send.at[idx], who)
        cp.start()
        own_sends.append(cp)
    for g in range(rows // 8):
        stage_cp(g).start()
    w_cp(0, 0).start()
    w_cp(1, 1).start()

    z[:, 0:96, :] = jnp.zeros((positions, 96, batch), F32)
    z[:, width - 96:width, :] = jnp.zeros((positions, 96, batch), F32)

    tok_cp.wait()
    for g in range(rows // 8):
        stage_cp(g).wait()

    def qrows(g, i, j):
        return stage[pl.ds(g * 8 * pitch + drafts * j + i, 8, stride=pitch), :]

    groups = [(i, g) for i in range(drafts) for g in range(rows // 8)]
    lane_b = lax.broadcasted_iota(jnp.int32, (8, batch), 1)
    sub_b = lax.broadcasted_iota(jnp.int32, (8, batch), 0)
    lane_t = lax.broadcasted_iota(jnp.int32, (8, LANES), 1)
    mine = [lane_b == k * rows + 8 * g + sub_b for g in range(rows // 8)]
    tok_col = []
    for i, g in groups:
        t = jnp.where(mine[g], jnp.broadcast_to(tok_ref[i:i + 1, :].astype(F32), (8, batch)), 0.0)
        tok_col.append(jnp.broadcast_to(jnp.sum(t, axis=1, keepdims=True), (8, LANES)).astype(jnp.int32))

    def scan(j, carry):
        top, got = carry
        new_top, new_got = [], []
        col = lane_t + j * LANES
        for a, (i, g) in enumerate(groups):
            v = qrows(g, i, j)
            new_top.append(jnp.maximum(top[a], v))
            new_got.append(jnp.where(col == tok_col[a], v, got[a]))
        return tuple(new_top), tuple(new_got)

    zero8 = tuple(jnp.zeros((8, LANES), F32) for _ in groups)
    top, got = lax.fori_loop(0, all_tiles, scan, (zero8, zero8))
    qtop_row, qgot_row = [], []
    for i in range(drafts):
        acc_t = jnp.zeros((8, batch), F32)
        acc_g = jnp.zeros((8, batch), F32)
        for a, (ii, g) in enumerate(groups):
            if ii != i:
                continue
            tcol = jnp.max(top[a], axis=1, keepdims=True)
            gcol = jnp.sum(got[a], axis=1, keepdims=True)
            rowc[a] = jnp.broadcast_to(jnp.log(TOP) - 0.25 * jnp.log(tcol), (8, LANES))
            acc_t = acc_t + jnp.where(mine[g], jnp.broadcast_to(tcol, (8, batch)), 0.0)
            acc_g = acc_g + jnp.where(mine[g], jnp.broadcast_to(gcol, (8, batch)), 0.0)
        qtop_row.append(jnp.sum(acc_t, axis=0, keepdims=True))
        qgot_row.append(jnp.sum(acc_g, axis=0, keepdims=True))
    msgs[k] = jnp.zeros(msgs.shape[1:], F32)
    for i in range(drafts):
        msgs[k, 8 + i:9 + i, :] = qgot_row[i]
        msgs[k, 10 + i:11 + i, :] = qtop_row[i]

    def encode(dest, put):
        first = (dest * vocab) // LANES

        def body(j, _):
            for i in range(drafts):
                for gg in range(rows // 16):
                    parts = []
                    for g in (2 * gg, 2 * gg + 1):
                        v = qrows(g, i, first + j)
                        y = jnp.exp(0.25 * jnp.log(v) + rowc[i * (rows // 8) + g])
                        parts.append((y + 0.5).astype(jnp.int32) - HALF)
                    code = jnp.concatenate(parts, axis=0).astype(jnp.int16)
                    put(i, gg, j // per, pl.ds(pl.multiple_of((j % per) * LANES, LANES), LANES), code)
            return 0

        lax.fori_loop(0, tiles, body, 0)

    def to_slot(r):
        def put(i, gg, s, cols, code):
            scode[r, i, s, 16 * gg:16 * gg + 16, cols] = code

        return put

    def to_self(i, gg, s, cols, code):
        qall[i, s, pl.ds(pl.multiple_of(k * rows + 16 * gg, 16), 16), cols] = code

    encode(2 * far, to_slot(0))
    encode(2 * far + 1, to_slot(1))

    fwd = []

    def forward(src, half):
        cp = hcopy(src, half, h_fwd.at[len(fwd)], mate)
        cp.start()
        fwd.append(cp)

    hwait(2 * left + c, 0)
    rel_r = hcopy(2 * left + c, 0, h_send.at[6], 2 * right + c)
    rel_r.start()
    forward(2 * left + c, 0)
    hwait(2 * right + c, 1)
    rel_l = hcopy(2 * right + c, 1, h_send.at[7], 2 * left + c)
    rel_l.start()
    forward(2 * right + c, 1)

    def unit(buf_i, i, s):
        return buf_i.at[i, s]

    def landing(src, i, s):
        return qall.at[i, s, pl.ds(pl.multiple_of(src * rows, rows), rows)]

    def direct(slot, i, s, who):
        return remote(
            unit(scode.at[slot], i, s), landing(k, i, s),
            q_send.at[slot * units + i * SEGS + s], q_recv.at[k * units + i * SEGS + s], who,
        )

    def out_far(way, v):
        i, s, cc = v // SEGS, 2 * ((v // 2) % (SEGS // 2)) + way, v % 2
        who = 2 * (right if way == 0 else left) + c
        return remote(
            unit(scode.at[cc], i, s), rbuf.at[way, v],
            q_send.at[cc * units + i * SEGS + s], r_recv.at[way * units + v], who,
        )

    def relay(way, v):
        i, s, cc = v // SEGS, 2 * ((v // 2) % (SEGS // 2)) + way, v % 2
        src = 2 * (left if way == 0 else right) + c
        who = 2 * (right if way == 0 else left) + cc
        return remote(
            rbuf.at[way, v], landing(src, i, s),
            r_send.at[way * units + v], q_recv.at[src * units + i * SEGS + s], who,
        )

    def near(way, u):
        i, s, cc = u // (2 * SEGS), (u // 2) % SEGS, u % 2
        who = 2 * (right if way == 0 else left) + cc
        return direct(2 + 2 * way + cc, i, s, who)

    def send_far(v):
        out_far(0, v).start()
        out_far(1, v).start()

    def send_near(u):
        near(0, u).start()
        near(1, u).start()

    def pass_on(v):
        for way in range(2):
            out_far(way, v).wait_recv()
            relay(way, v).start()

    encode(2 * right, to_slot(2))
    encode(2 * right + 1, to_slot(3))
    encode(2 * left, to_slot(4))
    encode(2 * left + 1, to_slot(5))

    hwait(2 * left + c, 1)
    forward(2 * left + c, 1)
    hwait(2 * right + c, 0)
    forward(2 * right + c, 0)

    def first_far(v, _):
        send_far(v)
        return 0

    def first_near(u, _):
        send_near(u)
        return 0

    lax.fori_loop(0, SEGS, first_far, 0)
    lax.fori_loop(0, 2 * SEGS, first_near, 0)
    encode(mate, to_slot(6))
    encode(k, to_self)

    def to_mate(u, _):
        direct(6, u // SEGS, u % SEGS, mate).start()
        return 0

    lax.fori_loop(0, drafts * SEGS, to_mate, 0)

    hwait(2 * far + c, 0)
    forward(2 * far + c, 0)
    hwait(2 * far + c, 1)
    forward(2 * far + c, 1)
    for chip in (x, left, right, far):
        for half in range(2):
            hwait(2 * chip + 1 - c, half)

    def step(t, top):
        slot = t % 2

        @pl.when((t >= 2) & (t < 4))
        def _():
            for e in range(SEGS // 2):
                pass_on((SEGS // 2) * (t - 2) + e)

        @pl.when((t >= 4) & (t < 6))
        def _():
            for e in range(SEGS // 2):
                send_far(SEGS + (SEGS // 2) * (t - 4) + e)

        @pl.when(t >= 6)
        def _():
            for e in range(SEGS // 2):
                send_near(2 * SEGS + (SEGS // 2) * (t - 6) + e)

        w_cp(t, slot).wait()
        prod = INV_TEMP * lax.dot_general(
            wbuf[slot], hall[...].reshape(positions * batch, dim), (((1,), (1,)), ((), ())), preferred_element_type=F32
        )
        base = pl.multiple_of(off + t * wrows, 8)
        for i in range(positions):
            z[i, pl.ds(base, wrows), :] = prod[:, i * batch:(i + 1) * batch]

        @pl.when(t + 2 < STEPS)
        def _():
            w_cp(t + 2, slot).start()

        return jnp.maximum(top, jnp.max(prod.reshape(wrows // 8, 8, positions * batch), axis=0))

    top = lax.fori_loop(0, STEPS, step, jnp.full((8, positions * batch), -jnp.inf, F32))
    own_max = jnp.max(top, axis=0, keepdims=True)

    chunk = 160
    row_i = lax.broadcasted_iota(jnp.int32, (chunk, batch), 0)
    for i in range(positions):
        m_i = own_max[:, i * batch:(i + 1) * batch]
        want = tok_ref[i:i + 1, :] - k * vocab if i < drafts else None

        def expo(t, carry, i=i, m_i=m_i, want=want):
            total, got = carry
            at = pl.ds(pl.multiple_of(off + t * chunk, 8), chunk)
            e = jnp.exp(z[i, at, :] - m_i)
            z[i, at, :] = e
            total = total + jnp.sum(e.reshape(chunk // 8, 8, batch), axis=0)
            if want is not None:
                pick = jnp.where(row_i + t * chunk == want, e, 0.0)
                got = got + jnp.sum(pick.reshape(chunk // 8, 8, batch), axis=0)
            return total, got

        zero = jnp.zeros((8, batch), F32)
        total, got = lax.fori_loop(0, vocab // chunk, expo, (zero, zero))
        msgs[k, i:i + 1, :] = m_i
        msgs[k, 3 + i:4 + i, :] = jnp.sum(total, axis=0, keepdims=True)
        if i < drafts:
            msgs[k, 6 + i:7 + i, :] = jnp.sum(got, axis=0, keepdims=True)

    def msg(p, src):
        return remote(msgs.at[src], msgs.at[src], m_send.at[p], m_recv.at[src], (k + p) % n)

    for p in range(1, n):
        msg(p, k).start()

    for v in range(SEGS, 2 * SEGS):
        pass_on(v)
    for p in range(1, n):
        msg(p, (k + p) % n).wait_recv()

    allm = msgs[...]
    peak = jnp.max(allm[:, 0:3, :], axis=0)
    part = jnp.exp(allm[:, 0:3, :] - peak[None])
    inv = 1.0 / jnp.sum(part * allm[:, 3:6, :], axis=0)
    p_pick = jnp.sum(part[:, 0:drafts, :] * allm[:, 6:8, :], axis=0) * inv[0:drafts]
    q_pick = jnp.sum(allm[:, 8:10, :], axis=0)
    q_scale = jnp.sum(allm[:, 10:12, :], axis=0) * (1.0 / (TOP * TOP * TOP * TOP))
    fac = jnp.exp(msgs[k, 0:3, :] - peak) * inv

    def scale(t, _):
        at = pl.ds(pl.multiple_of(off + t * chunk, 8), chunk)
        z[drafts, at, :] = z[drafts, at, :] * fac[drafts:drafts + 1, :]
        return 0

    lax.fori_loop(0, vocab // chunk, scale, 0)

    def xmsg(p, i, src):
        return remote(mass.at[i, src], mass.at[i, src], x_send.at[i * n + p], x_recv.at[i * n + src], (k + p) % n)

    def drain(u, _):
        direct(u // units, (u % units) // SEGS, u % SEGS, mate).wait_send()
        return 0

    def drain_relay(v, _):
        relay(0, v).wait_send()
        relay(1, v).wait_send()
        return 0

    for i in range(drafts):
        acc = [jnp.zeros((8, LANES), F32) for _ in range(batch // LANES)]
        for s in range(SEGS):
            if i == drafts - 1 and s == SEGS - 1:
                for cp in own_sends + [rel_r, rel_l] + fwd:
                    cp.wait_send()
                for p in range(1, n):
                    msg(p, k).wait_send()
                lax.fori_loop(0, (n - 1) * units, drain, 0)
            for p in range(1, n):
                src = (k + p) % n
                remote(
                    landing(src, i, s), landing(src, i, s), q_send.at[0],
                    q_recv.at[src * units + i * SEGS + s], mate,
                ).wait_recv()

            def body(t, acc, i=i, s=s):
                at = pl.ds(pl.multiple_of((s * (tiles // SEGS) + t) * LANES, LANES), LANES)
                out = []
                for h in range(batch // LANES):
                    ls = slice(h * LANES, (h + 1) * LANES)
                    code = qall[i, s, ls, pl.ds(pl.multiple_of(t * LANES, LANES), LANES)].astype(jnp.int32).astype(F32)
                    y = code.T + float(HALF)
                    y = y * y
                    qt = y * y * q_scale[i:i + 1, ls]
                    ex = jnp.maximum(z[i, at, ls] * fac[i:i + 1, ls] - qt, 0.0)
                    z[i, at, ls] = ex
                    out.append(acc[h] + jnp.sum(ex.reshape(LANES // 8, 8, LANES), axis=0))
                return tuple(out)

            acc = lax.fori_loop(0, tiles // SEGS, body, tuple(acc))
        for h in range(batch // LANES):
            mass[i, k, :, h * LANES:(h + 1) * LANES] = jnp.sum(acc[h], axis=0, keepdims=True)
        for p in range(1, n):
            xmsg(p, i, k).start()
    lax.fori_loop(0, units, drain_relay, 0)
    small_ref[...] = jnp.zeros(small_ref.shape, F32)
    small_ref[2:4, :] = p_pick
    small_ref[4:6, :] = q_pick
    for i in range(drafts):
        for p in range(1, n):
            xmsg(p, i, (k + p) % n).wait_recv()
        total = jnp.sum(mass[i], axis=0)
        small_ref[i:i + 1, :] = 1.0 / total

    for p in range(1, n):
        for i in range(drafts):
            xmsg(p, i, k).wait_send()


def finish(n, z, small, res_ref, bonus_ref, acc_ref, exp_ref, buf, sem):
    drafts, vocab, _ = res_ref.shape
    off = pl.multiple_of((lax.axis_index("tp") * vocab) % LANES, 8)
    last = pltpu.make_async_copy(z.at[drafts, pl.ds(off, vocab), :], bonus_ref, sem.at[0])
    last.start()
    copies = [last]
    part = vocab // PARTS
    for i in range(drafts):
        scale = small[i:i + 1, :]
        for t in range(PARTS):
            to = pl.ds(t * part, part)
            buf[i, to, :] = z[i, pl.ds(pl.multiple_of(off + t * part, 8), part), :] * scale
            cp = pltpu.make_async_copy(buf.at[i, to], res_ref.at[i, to], sem.at[len(copies)])
            cp.start()
            copies.append(cp)
    accept = jnp.minimum(small[2:4, :] / small[4:6, :], 1.0)
    acc_ref[...] = accept
    exp_ref[...] = accept[0:1] + accept[0:1] * accept[1:2]
    for cp in copies:
        cp.wait()


def solution(mesh):
    n = mesh.shape["tp"]

    def local(hid, w, q, tok):
        rows, positions, dim = hid.shape
        vocab = w.shape[1]
        drafts = positions - 1
        batch = rows * n
        q_tiles = q.shape[2] // LANES
        width = -(-vocab // LANES) * LANES
        q_view = q.reshape(rows, drafts, q_tiles, LANES).transpose(0, 2, 1, 3)
        q_view = with_layout_constraint(q_view, Layout((0, 1, 2, 3))).reshape(-1, LANES)
        dma = pltpu.SemaphoreType.DMA
        vmem, anywhere = pl.BlockSpec(memory_space=pltpu.VMEM), pl.BlockSpec(memory_space=pltpu.HBM)
        z, small = pl.pallas_call(
            functools.partial(kernel, n),
            out_shape=(
                jax.ShapeDtypeStruct((positions, width, batch), F32),
                jax.ShapeDtypeStruct((8, batch), F32),
            ),
            in_specs=[anywhere] * 4,
            out_specs=(vmem, vmem),
            scratch_shapes=[
                pltpu.VMEM((drafts, batch), jnp.int32),
                pltpu.VMEM((positions, batch, dim), jnp.bfloat16),
                pltpu.VMEM((rows * q_tiles * drafts, LANES), F32),
                pltpu.VMEM((n - 1, drafts, SEGS, rows, width // SEGS), jnp.int16),
                pltpu.VMEM((drafts, SEGS, batch, width // SEGS), jnp.int16),
                pltpu.VMEM((2, drafts * SEGS, rows, width // SEGS), jnp.int16),
                pltpu.VMEM((2, vocab // STEPS, dim), jnp.bfloat16),
                pltpu.VMEM((n, 16, batch), F32),
                pltpu.VMEM((drafts, n, 1, batch), F32),
                pltpu.VMEM((drafts * (rows // 8), 8, LANES), F32),
                dma((8,)), dma((8,)), dma((2 * n,)),
                dma((n * drafts * SEGS,)), dma((n * drafts * SEGS,)), dma((2 * drafts * SEGS,)), dma((2 * drafts * SEGS,)),
                dma((n,)), dma((n,)), dma((2 * n,)), dma((2 * n,)),
                dma((8,)), dma((2,)),
            ],
            compiler_params=pltpu.CompilerParams(
                collective_id=0, has_side_effects=True, vmem_limit_bytes=40 * 2**20
            ),
        )(*[pltpu.with_memory_space_constraint(a, pltpu.HBM) for a in (tok.T, hid.transpose(1, 0, 2), w.T, q_view)])
        residual, bonus, accept, expected = pl.pallas_call(
            functools.partial(finish, n),
            out_shape=(
                jax.ShapeDtypeStruct((drafts, vocab, batch), F32),
                jax.ShapeDtypeStruct((vocab, batch), F32),
                jax.ShapeDtypeStruct((drafts, batch), F32),
                jax.ShapeDtypeStruct((1, batch), F32),
            ),
            in_specs=[vmem, vmem],
            out_specs=(anywhere, anywhere, vmem, vmem),
            scratch_shapes=[pltpu.VMEM((drafts, vocab, batch), F32), dma((drafts * PARTS + 1,))],
            compiler_params=pltpu.CompilerParams(vmem_limit_bytes=24 * 2**20),
        )(z, small)
        return accept.T, expected[0], residual.transpose(2, 0, 1), bonus.T

    return jax.shard_map(
        local,
        mesh=mesh,
        in_specs=(P(("dp", "tp"), None, None), P(None, "tp"), P(("dp", "tp"), None, None), P("dp", None)),
        out_specs=(P("dp", None), P("dp"), P("dp", None, "tp"), P("dp", "tp")),
        check_vma=False,
    )
```

```python
import functools

import jax
import jax.numpy as jnp
from jax import lax
from jax.experimental import pallas as pl
from jax.experimental.pallas import tpu as pltpu
from jax.experimental.layout import Layout, with_layout_constraint
from jax.sharding import PartitionSpec as P

INV_TEMP = 1.25
TOP = 65535.0
HALF = 32768
LANES = 128
SEGS = 2
STEPS = 10
PARTS = 5
F32 = jnp.float32
MESH = pl.DeviceIdType.MESH


def kernel(
    n, tok_in, hid_ref, w_ref, q_ref,
    z, small_ref,
    tok_ref, hall, stage, scode, qall, rbuf, wbuf, msgs, mass, rowc,
    h_send, h_fwd, h_recv, q_send, q_recv, r_send, r_recv,
    m_send, m_recv, x_send, x_recv, loc, wsem,
):
    k = lax.axis_index("tp")
    x, c = k // 2, k % 2
    chips = n // 2
    right, left = (x + 1) % chips, (x + chips - 1) % chips
    far = (x + 2) % chips
    mate = 2 * x + 1 - c
    positions, batch, dim = hall.shape
    drafts = positions - 1
    rows = batch // n
    vocab = w_ref.shape[0]
    seg = qall.shape[3]
    width = seg * SEGS
    tiles = width // LANES
    units = drafts * SEGS
    per = seg // LANES
    pitch = q_ref.shape[0] // rows
    all_tiles = pitch // drafts
    off = (k * vocab) % LANES
    hcol = dim // 2
    wrows = vocab // STEPS

    def remote(src, dst, ssem, rsem, who):
        return pltpu.make_async_remote_copy(
            src_ref=src, dst_ref=dst, send_sem=ssem, recv_sem=rsem,
            device_id={"tp": who}, device_id_type=MESH,
        )

    hid_cp = pltpu.make_async_copy(hid_ref, hall.at[:, pl.ds(k * rows, rows), :], loc.at[0])
    hid_cp.start()
    tok_cp = pltpu.make_async_copy(tok_in, tok_ref, loc.at[6])
    tok_cp.start()

    def stage_cp(g):
        part = pl.ds(g * 8 * pitch, 8 * pitch)
        return pltpu.make_async_copy(q_ref.at[part], stage.at[part], loc.at[1 + g])

    def w_cp(t, slot):
        return pltpu.make_async_copy(
            w_ref.at[pl.ds(pl.multiple_of(t * wrows, 8), wrows)], wbuf.at[slot], wsem.at[slot]
        )

    barrier = pltpu.get_barrier_semaphore()
    for who in (2 * right + c, 2 * left + c, mate):
        pl.semaphore_signal(barrier, inc=1, device_id={"tp": who}, device_id_type=MESH)
    pl.semaphore_wait(barrier, 3)

    def hpiece(src, half):
        return hall.at[:, pl.ds(pl.multiple_of(src * rows, rows), rows), pl.ds(half * hcol, hcol)]

    def hcopy(src, half, ssem, who):
        return remote(hpiece(src, half), hpiece(src, half), ssem, h_recv.at[src * 2 + half], who)

    def hwait(src, half):
        hcopy(src, half, h_send.at[0], mate).wait_recv()

    hid_cp.wait()
    own_sends = []
    for idx, (who, half) in enumerate(
        [(2 * right + c, 0), (2 * left + c, 1), (2 * right + c, 1), (2 * left + c, 0), (mate, 0), (mate, 1)]
    ):
        cp = hcopy(k, half, h_send.at[idx], who)
        cp.start()
        own_sends.append(cp)
    for g in range(rows // 8):
        stage_cp(g).start()
    w_cp(0, 0).start()
    w_cp(1, 1).start()

    z[:, 0:96, :] = jnp.zeros((positions, 96, batch), F32)
    z[:, width - 96:width, :] = jnp.zeros((positions, 96, batch), F32)

    tok_cp.wait()
    for g in range(rows // 8):
        stage_cp(g).wait()

    def qrows(g, i, j):
        return stage[pl.ds(g * 8 * pitch + drafts * j + i, 8, stride=pitch), :]

    groups = [(i, g) for i in range(drafts) for g in range(rows // 8)]
    lane_b = lax.broadcasted_iota(jnp.int32, (8, batch), 1)
    sub_b = lax.broadcasted_iota(jnp.int32, (8, batch), 0)
    lane_t = lax.broadcasted_iota(jnp.int32, (8, LANES), 1)
    mine = [lane_b == k * rows + 8 * g + sub_b for g in range(rows // 8)]
    tok_col = []
    for i, g in groups:
        t = jnp.where(mine[g], jnp.broadcast_to(tok_ref[i:i + 1, :].astype(F32), (8, batch)), 0.0)
        tok_col.append(jnp.broadcast_to(jnp.sum(t, axis=1, keepdims=True), (8, LANES)).astype(jnp.int32))

    def scan(j, carry):
        top, got = carry
        new_top, new_got = [], []
        col = lane_t + j * LANES
        for a, (i, g) in enumerate(groups):
            v = qrows(g, i, j)
            new_top.append(jnp.maximum(top[a], v))
            new_got.append(jnp.where(col == tok_col[a], v, got[a]))
        return tuple(new_top), tuple(new_got)

    zero8 = tuple(jnp.zeros((8, LANES), F32) for _ in groups)
    top, got = lax.fori_loop(0, all_tiles, scan, (zero8, zero8))
    qtop_row, qgot_row = [], []
    for i in range(drafts):
        acc_t = jnp.zeros((8, batch), F32)
        acc_g = jnp.zeros((8, batch), F32)
        for a, (ii, g) in enumerate(groups):
            if ii != i:
                continue
            tcol = jnp.max(top[a], axis=1, keepdims=True)
            gcol = jnp.sum(got[a], axis=1, keepdims=True)
            rowc[a] = jnp.broadcast_to(jnp.log(TOP) - 0.25 * jnp.log(tcol), (8, LANES))
            acc_t = acc_t + jnp.where(mine[g], jnp.broadcast_to(tcol, (8, batch)), 0.0)
            acc_g = acc_g + jnp.where(mine[g], jnp.broadcast_to(gcol, (8, batch)), 0.0)
        qtop_row.append(jnp.sum(acc_t, axis=0, keepdims=True))
        qgot_row.append(jnp.sum(acc_g, axis=0, keepdims=True))
    msgs[k] = jnp.zeros(msgs.shape[1:], F32)
    for i in range(drafts):
        msgs[k, 8 + i:9 + i, :] = qgot_row[i]
        msgs[k, 10 + i:11 + i, :] = qtop_row[i]

    def encode(dest, put):
        first = (dest * vocab) // LANES

        def body(j, _):
            for i in range(drafts):
                for gg in range(rows // 16):
                    parts = []
                    for g in (2 * gg, 2 * gg + 1):
                        v = qrows(g, i, first + j)
                        y = jnp.exp(0.25 * jnp.log(v) + rowc[i * (rows // 8) + g])
                        parts.append((y + 0.5).astype(jnp.int32) - HALF)
                    code = jnp.concatenate(parts, axis=0).astype(jnp.int16)
                    put(i, gg, j // per, pl.ds(pl.multiple_of((j % per) * LANES, LANES), LANES), code)
            return 0

        lax.fori_loop(0, tiles, body, 0)

    def to_slot(r):
        def put(i, gg, s, cols, code):
            scode[r, i, s, 16 * gg:16 * gg + 16, cols] = code

        return put

    def to_self(i, gg, s, cols, code):
        qall[i, s, pl.ds(pl.multiple_of(k * rows + 16 * gg, 16), 16), cols] = code

    encode(2 * far, to_slot(0))
    encode(2 * far + 1, to_slot(1))

    fwd = []

    def forward(src, half):
        cp = hcopy(src, half, h_fwd.at[len(fwd)], mate)
        cp.start()
        fwd.append(cp)

    hwait(2 * left + c, 0)
    rel_r = hcopy(2 * left + c, 0, h_send.at[6], 2 * right + c)
    rel_r.start()
    forward(2 * left + c, 0)
    hwait(2 * right + c, 1)
    rel_l = hcopy(2 * right + c, 1, h_send.at[7], 2 * left + c)
    rel_l.start()
    forward(2 * right + c, 1)

    def unit(buf_i, i, s):
        return buf_i.at[i, s]

    def landing(src, i, s):
        return qall.at[i, s, pl.ds(pl.multiple_of(src * rows, rows), rows)]

    def direct(slot, i, s, who):
        return remote(
            unit(scode.at[slot], i, s), landing(k, i, s),
            q_send.at[slot * units + i * SEGS + s], q_recv.at[k * units + i * SEGS + s], who,
        )

    def out_far(way, v):
        i, s, cc = v // SEGS, 2 * ((v // 2) % (SEGS // 2)) + way, v % 2
        who = 2 * (right if way == 0 else left) + c
        return remote(
            unit(scode.at[cc], i, s), rbuf.at[way, v],
            q_send.at[cc * units + i * SEGS + s], r_recv.at[way * units + v], who,
        )

    def relay(way, v):
        i, s, cc = v // SEGS, 2 * ((v // 2) % (SEGS // 2)) + way, v % 2
        src = 2 * (left if way == 0 else right) + c
        who = 2 * (right if way == 0 else left) + cc
        return remote(
            rbuf.at[way, v], landing(src, i, s),
            r_send.at[way * units + v], q_recv.at[src * units + i * SEGS + s], who,
        )

    def near(way, u):
        i, s, cc = u // (2 * SEGS), (u // 2) % SEGS, u % 2
        who = 2 * (right if way == 0 else left) + cc
        return direct(2 + 2 * way + cc, i, s, who)

    def send_far(v):
        out_far(0, v).start()
        out_far(1, v).start()

    def send_near(u):
        near(0, u).start()
        near(1, u).start()

    def pass_on(v):
        for way in range(2):
            out_far(way, v).wait_recv()
            relay(way, v).start()

    encode(2 * right, to_slot(2))
    encode(2 * right + 1, to_slot(3))
    encode(2 * left, to_slot(4))
    encode(2 * left + 1, to_slot(5))

    hwait(2 * left + c, 1)
    forward(2 * left + c, 1)
    hwait(2 * right + c, 0)
    forward(2 * right + c, 0)

    def first_far(v, _):
        send_far(v)
        return 0

    def first_near(u, _):
        send_near(u)
        return 0

    lax.fori_loop(0, SEGS, first_far, 0)
    lax.fori_loop(0, 2 * SEGS, first_near, 0)
    encode(mate, to_slot(6))
    encode(k, to_self)

    def to_mate(u, _):
        direct(6, u // SEGS, u % SEGS, mate).start()
        return 0

    lax.fori_loop(0, drafts * SEGS, to_mate, 0)

    hwait(2 * far + c, 0)
    forward(2 * far + c, 0)
    hwait(2 * far + c, 1)
    forward(2 * far + c, 1)
    for chip in (x, left, right, far):
        for half in range(2):
            hwait(2 * chip + 1 - c, half)

    def step(t, top):
        slot = t % 2

        @pl.when((t >= 2) & (t < 4))
        def _():
            for e in range(SEGS // 2):
                pass_on((SEGS // 2) * (t - 2) + e)

        @pl.when((t >= 4) & (t < 6))
        def _():
            for e in range(SEGS // 2):
                send_far(SEGS + (SEGS // 2) * (t - 4) + e)

        @pl.when(t >= 6)
        def _():
            for e in range(SEGS // 2):
                send_near(2 * SEGS + (SEGS // 2) * (t - 6) + e)

        w_cp(t, slot).wait()
        prod = INV_TEMP * lax.dot_general(
            wbuf[slot], hall[...].reshape(positions * batch, dim), (((1,), (1,)), ((), ())), preferred_element_type=F32
        )
        base = pl.multiple_of(off + t * wrows, 8)
        for i in range(positions):
            z[i, pl.ds(base, wrows), :] = prod[:, i * batch:(i + 1) * batch]

        @pl.when(t + 2 < STEPS)
        def _():
            w_cp(t + 2, slot).start()

        return jnp.maximum(top, jnp.max(prod.reshape(wrows // 8, 8, positions * batch), axis=0))

    top = lax.fori_loop(0, STEPS, step, jnp.full((8, positions * batch), -jnp.inf, F32))
    own_max = jnp.max(top, axis=0, keepdims=True)

    chunk = 160
    row_i = lax.broadcasted_iota(jnp.int32, (chunk, batch), 0)
    for i in range(positions):
        m_i = own_max[:, i * batch:(i + 1) * batch]
        want = tok_ref[i:i + 1, :] - k * vocab if i < drafts else None

        def expo(t, carry, i=i, m_i=m_i, want=want):
            total, got = carry
            at = pl.ds(pl.multiple_of(off + t * chunk, 8), chunk)
            e = jnp.exp(z[i, at, :] - m_i)
            z[i, at, :] = e
            total = total + jnp.sum(e.reshape(chunk // 8, 8, batch), axis=0)
            if want is not None:
                pick = jnp.where(row_i + t * chunk == want, e, 0.0)
                got = got + jnp.sum(pick.reshape(chunk // 8, 8, batch), axis=0)
            return total, got

        zero = jnp.zeros((8, batch), F32)
        total, got = lax.fori_loop(0, vocab // chunk, expo, (zero, zero))
        msgs[k, i:i + 1, :] = m_i
        msgs[k, 3 + i:4 + i, :] = jnp.sum(total, axis=0, keepdims=True)
        if i < drafts:
            msgs[k, 6 + i:7 + i, :] = jnp.sum(got, axis=0, keepdims=True)

    def msg(p, src):
        return remote(msgs.at[src], msgs.at[src], m_send.at[p], m_recv.at[src], (k + p) % n)

    for p in range(1, n):
        msg(p, k).start()

    for v in range(SEGS, 2 * SEGS):
        pass_on(v)
    for p in range(1, n):
        msg(p, (k + p) % n).wait_recv()

    allm = msgs[...]
    peak = jnp.max(allm[:, 0:3, :], axis=0)
    part = jnp.exp(allm[:, 0:3, :] - peak[None])
    inv = 1.0 / jnp.sum(part * allm[:, 3:6, :], axis=0)
    p_pick = jnp.sum(part[:, 0:drafts, :] * allm[:, 6:8, :], axis=0) * inv[0:drafts]
    q_pick = jnp.sum(allm[:, 8:10, :], axis=0)
    q_scale = jnp.sum(allm[:, 10:12, :], axis=0) * (1.0 / (TOP * TOP * TOP * TOP))
    fac = jnp.exp(msgs[k, 0:3, :] - peak) * inv

    def scale(t, _):
        at = pl.ds(pl.multiple_of(off + t * chunk, 8), chunk)
        z[drafts, at, :] = z[drafts, at, :] * fac[drafts:drafts + 1, :]
        return 0

    lax.fori_loop(0, vocab // chunk, scale, 0)

    def xmsg(p, i, src):
        return remote(mass.at[i, src], mass.at[i, src], x_send.at[i * n + p], x_recv.at[i * n + src], (k + p) % n)

    def drain(u, _):
        direct(u // units, (u % units) // SEGS, u % SEGS, mate).wait_send()
        return 0

    def drain_relay(v, _):
        relay(0, v).wait_send()
        relay(1, v).wait_send()
        return 0

    for i in range(drafts):
        acc = [jnp.zeros((8, LANES), F32) for _ in range(batch // LANES)]
        for s in range(SEGS):
            if i == drafts - 1 and s == SEGS - 1:
                for cp in own_sends + [rel_r, rel_l] + fwd:
                    cp.wait_send()
                for p in range(1, n):
                    msg(p, k).wait_send()
                lax.fori_loop(0, (n - 1) * units, drain, 0)
            for p in range(1, n):
                src = (k + p) % n
                remote(
                    landing(src, i, s), landing(src, i, s), q_send.at[0],
                    q_recv.at[src * units + i * SEGS + s], mate,
                ).wait_recv()

            def body(t, acc, i=i, s=s):
                at = pl.ds(pl.multiple_of((s * (tiles // SEGS) + t) * LANES, LANES), LANES)
                out = []
                for h in range(batch // LANES):
                    ls = slice(h * LANES, (h + 1) * LANES)
                    code = qall[i, s, ls, pl.ds(pl.multiple_of(t * LANES, LANES), LANES)].astype(jnp.int32).astype(F32)
                    y = code.T + float(HALF)
                    y = y * y
                    qt = y * y * q_scale[i:i + 1, ls]
                    ex = jnp.maximum(z[i, at, ls] * fac[i:i + 1, ls] - qt, 0.0)
                    z[i, at, ls] = ex
                    out.append(acc[h] + jnp.sum(ex.reshape(LANES // 8, 8, LANES), axis=0))
                return tuple(out)

            acc = lax.fori_loop(0, tiles // SEGS, body, tuple(acc))
        for h in range(batch // LANES):
            mass[i, k, :, h * LANES:(h + 1) * LANES] = jnp.sum(acc[h], axis=0, keepdims=True)
        for p in range(1, n):
            xmsg(p, i, k).start()
    lax.fori_loop(0, units, drain_relay, 0)
    small_ref[...] = jnp.zeros(small_ref.shape, F32)
    small_ref[2:4, :] = p_pick
    small_ref[4:6, :] = q_pick
    for i in range(drafts):
        for p in range(1, n):
            xmsg(p, i, (k + p) % n).wait_recv()
        total = jnp.sum(mass[i], axis=0)
        small_ref[i:i + 1, :] = 1.0 / total

    for p in range(1, n):
        for i in range(drafts):
            xmsg(p, i, k).wait_send()


def finish(n, z, small, res_ref, bonus_ref, acc_ref, exp_ref, buf, sem):
    drafts, vocab, _ = res_ref.shape
    off = pl.multiple_of((lax.axis_index("tp") * vocab) % LANES, 8)
    last = pltpu.make_async_copy(z.at[drafts, pl.ds(off, vocab), :], bonus_ref, sem.at[0])
    last.start()
    copies = [last]
    part = vocab // PARTS
    for i in range(drafts):
        scale = small[i:i + 1, :]
        for t in range(PARTS):
            to = pl.ds(t * part, part)
            buf[i, to, :] = z[i, pl.ds(pl.multiple_of(off + t * part, 8), part), :] * scale
            cp = pltpu.make_async_copy(buf.at[i, to], res_ref.at[i, to], sem.at[len(copies)])
            cp.start()
            copies.append(cp)
    accept = jnp.minimum(small[2:4, :] / small[4:6, :], 1.0)
    acc_ref[...] = accept
    exp_ref[...] = accept[0:1] + accept[0:1] * accept[1:2]
    for cp in copies:
        cp.wait()


def solution(mesh):
    n = mesh.shape["tp"]

    def local(hid, w, q, tok):
        rows, positions, dim = hid.shape
        vocab = w.shape[1]
        drafts = positions - 1
        batch = rows * n
        q_tiles = q.shape[2] // LANES
        width = -(-vocab // LANES) * LANES
        q_view = q.reshape(rows, drafts, q_tiles, LANES).transpose(0, 2, 1, 3)
        q_view = with_layout_constraint(q_view, Layout((0, 1, 2, 3))).reshape(-1, LANES)
        dma = pltpu.SemaphoreType.DMA
        vmem, anywhere = pl.BlockSpec(memory_space=pltpu.VMEM), pl.BlockSpec(memory_space=pltpu.HBM)
        z, small = pl.pallas_call(
            functools.partial(kernel, n),
            out_shape=(
                jax.ShapeDtypeStruct((positions, width, batch), F32),
                jax.ShapeDtypeStruct((8, batch), F32),
            ),
            in_specs=[anywhere] * 4,
            out_specs=(vmem, vmem),
            scratch_shapes=[
                pltpu.VMEM((drafts, batch), jnp.int32),
                pltpu.VMEM((positions, batch, dim), jnp.bfloat16),
                pltpu.VMEM((rows * q_tiles * drafts, LANES), F32),
                pltpu.VMEM((n - 1, drafts, SEGS, rows, width // SEGS), jnp.int16),
                pltpu.VMEM((drafts, SEGS, batch, width // SEGS), jnp.int16),
                pltpu.VMEM((2, drafts * SEGS, rows, width // SEGS), jnp.int16),
                pltpu.VMEM((2, vocab // STEPS, dim), jnp.bfloat16),
                pltpu.VMEM((n, 16, batch), F32),
                pltpu.VMEM((drafts, n, 1, batch), F32),
                pltpu.VMEM((drafts * (rows // 8), 8, LANES), F32),
                dma((8,)), dma((8,)), dma((2 * n,)),
                dma((n * drafts * SEGS,)), dma((n * drafts * SEGS,)), dma((2 * drafts * SEGS,)), dma((2 * drafts * SEGS,)),
                dma((n,)), dma((n,)), dma((2 * n,)), dma((2 * n,)),
                dma((8,)), dma((2,)),
            ],
            compiler_params=pltpu.CompilerParams(
                collective_id=0, has_side_effects=True, vmem_limit_bytes=40 * 2**20
            ),
        )(*[pltpu.with_memory_space_constraint(a, pltpu.HBM) for a in (tok.T, hid.transpose(1, 0, 2), w.T, q_view)])
        residual, bonus, accept, expected = pl.pallas_call(
            functools.partial(finish, n),
            out_shape=(
                jax.ShapeDtypeStruct((drafts, vocab, batch), F32),
                jax.ShapeDtypeStruct((vocab, batch), F32),
                jax.ShapeDtypeStruct((drafts, batch), F32),
                jax.ShapeDtypeStruct((1, batch), F32),
            ),
            in_specs=[vmem, vmem],
            out_specs=(anywhere, anywhere, vmem, vmem),
            scratch_shapes=[pltpu.VMEM((drafts, vocab, batch), F32), dma((drafts * PARTS + 1,))],
            compiler_params=pltpu.CompilerParams(vmem_limit_bytes=24 * 2**20),
        )(z, small)
        return accept.T, expected[0], residual.transpose(2, 0, 1), bonus.T

    return jax.shard_map(
        local,
        mesh=mesh,
        in_specs=(P(("dp", "tp"), None, None), P(None, "tp"), P(("dp", "tp"), None, None), P("dp", None)),
        out_specs=(P("dp", None), P("dp"), P("dp", None, "tp"), P("dp", "tp")),
        check_vma=False,
    )
```

```python
import functools

import jax
import jax.numpy as jnp
from jax import lax
from jax.experimental import pallas as pl
from jax.experimental.pallas import tpu as pltpu
from jax.experimental.layout import Layout, with_layout_constraint
from jax.sharding import PartitionSpec as P

INV_TEMP = 1.25
TOP = 65535.0
HALF = 32768
LANES = 128
SEGS = 4
PIECES = (((0, 4),), ((0, 2), (2, 1), (3, 1)))
STEPS = 10
PARTS = 5
F32 = jnp.float32
MESH = pl.DeviceIdType.MESH


def kernel(
    n, tok_in, hid_ref, w_ref, q_ref,
    z, small_ref,
    tok_ref, hall, stage, scode, qall, rbuf, wbuf, msgs, mass, rowc,
    h_send, h_fwd, h_recv, q_send, q_recv, r_send, r_recv,
    m_send, m_recv, x_send, x_recv, loc, wsem,
):
    k = lax.axis_index("tp")
    x, c = k // 2, k % 2
    chips = n // 2
    right, left = (x + 1) % chips, (x + chips - 1) % chips
    far = (x + 2) % chips
    mate = 2 * x + 1 - c
    positions, batch, dim = hall.shape
    drafts = positions - 1
    rows = batch // n
    vocab = w_ref.shape[0]
    seg = qall.shape[3]
    width = seg * SEGS
    tiles = width // LANES
    units = drafts * SEGS
    per = seg // LANES
    pitch = q_ref.shape[0] // rows
    all_tiles = pitch // drafts
    off = (k * vocab) % LANES
    hcol = dim // 2
    wrows = vocab // STEPS

    def remote(src, dst, ssem, rsem, who):
        return pltpu.make_async_remote_copy(
            src_ref=src, dst_ref=dst, send_sem=ssem, recv_sem=rsem,
            device_id={"tp": who}, device_id_type=MESH,
        )

    hid_cp = pltpu.make_async_copy(hid_ref, hall.at[:, pl.ds(k * rows, rows), :], loc.at[0])
    hid_cp.start()
    tok_cp = pltpu.make_async_copy(tok_in, tok_ref, loc.at[6])
    tok_cp.start()

    def stage_cp(g):
        part = pl.ds(g * 8 * pitch, 8 * pitch)
        return pltpu.make_async_copy(q_ref.at[part], stage.at[part], loc.at[1 + g])

    def w_cp(t, slot):
        return pltpu.make_async_copy(
            w_ref.at[pl.ds(pl.multiple_of(t * wrows, 8), wrows)], wbuf.at[slot], wsem.at[slot]
        )

    barrier = pltpu.get_barrier_semaphore()
    for who in (2 * right + c, 2 * left + c, mate):
        pl.semaphore_signal(barrier, inc=1, device_id={"tp": who}, device_id_type=MESH)
    pl.semaphore_wait(barrier, 3)

    def hpiece(src, half):
        return hall.at[:, pl.ds(pl.multiple_of(src * rows, rows), rows), pl.ds(half * hcol, hcol)]

    def hcopy(src, half, ssem, who):
        return remote(hpiece(src, half), hpiece(src, half), ssem, h_recv.at[src * 2 + half], who)

    def hwait(src, half):
        hcopy(src, half, h_send.at[0], mate).wait_recv()

    hid_cp.wait()
    own_sends = []
    for idx, (who, half) in enumerate(
        [(2 * right + c, 0), (2 * left + c, 1), (2 * right + c, 1), (2 * left + c, 0), (mate, 0), (mate, 1)]
    ):
        cp = hcopy(k, half, h_send.at[idx], who)
        cp.start()
        own_sends.append(cp)
    for g in range(rows // 8):
        stage_cp(g).start()
    w_cp(0, 0).start()
    w_cp(1, 1).start()

    z[:, 0:96, :] = jnp.zeros((positions, 96, batch), F32)
    z[:, width - 96:width, :] = jnp.zeros((positions, 96, batch), F32)

    tok_cp.wait()
    for g in range(rows // 8):
        stage_cp(g).wait()

    def qrows(g, i, j):
        return stage[pl.ds(g * 8 * pitch + drafts * j + i, 8, stride=pitch), :]

    groups = [(i, g) for i in range(drafts) for g in range(rows // 8)]
    lane_b = lax.broadcasted_iota(jnp.int32, (8, batch), 1)
    sub_b = lax.broadcasted_iota(jnp.int32, (8, batch), 0)
    lane_t = lax.broadcasted_iota(jnp.int32, (8, LANES), 1)
    mine = [lane_b == k * rows + 8 * g + sub_b for g in range(rows // 8)]
    tok_col = []
    for i, g in groups:
        t = jnp.where(mine[g], jnp.broadcast_to(tok_ref[i:i + 1, :].astype(F32), (8, batch)), 0.0)
        tok_col.append(jnp.broadcast_to(jnp.sum(t, axis=1, keepdims=True), (8, LANES)).astype(jnp.int32))

    def scan(j, carry):
        top, got = carry
        new_top, new_got = [], []
        col = lane_t + j * LANES
        for a, (i, g) in enumerate(groups):
            v = qrows(g, i, j)
            new_top.append(jnp.maximum(top[a], v))
            new_got.append(jnp.where(col == tok_col[a], v, got[a]))
        return tuple(new_top), tuple(new_got)

    zero8 = tuple(jnp.zeros((8, LANES), F32) for _ in groups)
    top, got = lax.fori_loop(0, all_tiles, scan, (zero8, zero8))
    qtop_row, qgot_row = [], []
    for i in range(drafts):
        acc_t = jnp.zeros((8, batch), F32)
        acc_g = jnp.zeros((8, batch), F32)
        for a, (ii, g) in enumerate(groups):
            if ii != i:
                continue
            tcol = jnp.max(top[a], axis=1, keepdims=True)
            gcol = jnp.sum(got[a], axis=1, keepdims=True)
            rowc[a] = jnp.broadcast_to(jnp.log(TOP) - 0.25 * jnp.log(tcol), (8, LANES))
            acc_t = acc_t + jnp.where(mine[g], jnp.broadcast_to(tcol, (8, batch)), 0.0)
            acc_g = acc_g + jnp.where(mine[g], jnp.broadcast_to(gcol, (8, batch)), 0.0)
        qtop_row.append(jnp.sum(acc_t, axis=0, keepdims=True))
        qgot_row.append(jnp.sum(acc_g, axis=0, keepdims=True))
    msgs[k] = jnp.zeros(msgs.shape[1:], F32)
    for i in range(drafts):
        msgs[k, 8 + i:9 + i, :] = qgot_row[i]
        msgs[k, 10 + i:11 + i, :] = qtop_row[i]

    def encode(dest, put):
        first = (dest * vocab) // LANES

        def body(j, _):
            for i in range(drafts):
                for gg in range(rows // 16):
                    parts = []
                    for g in (2 * gg, 2 * gg + 1):
                        v = qrows(g, i, first + j)
                        y = jnp.exp(0.25 * jnp.log(v) + rowc[i * (rows // 8) + g])
                        parts.append((y + 0.5).astype(jnp.int32) - HALF)
                    code = jnp.concatenate(parts, axis=0).astype(jnp.int16)
                    put(i, gg, j // per, pl.ds(pl.multiple_of((j % per) * LANES, LANES), LANES), code)
            return 0

        lax.fori_loop(0, tiles, body, 0)

    def to_slot(r):
        def put(i, gg, s, cols, code):
            scode[r, i, s, 16 * gg:16 * gg + 16, cols] = code

        return put

    def to_self(i, gg, s, cols, code):
        qall[i, s, pl.ds(pl.multiple_of(k * rows + 16 * gg, 16), 16), cols] = code

    encode(2 * far, to_slot(0))
    encode(2 * far + 1, to_slot(1))

    fwd = []

    def forward(src, half):
        cp = hcopy(src, half, h_fwd.at[len(fwd)], mate)
        cp.start()
        fwd.append(cp)

    hwait(2 * left + c, 0)
    rel_r = hcopy(2 * left + c, 0, h_send.at[6], 2 * right + c)
    rel_r.start()
    forward(2 * left + c, 0)
    hwait(2 * right + c, 1)
    rel_l = hcopy(2 * right + c, 1, h_send.at[7], 2 * left + c)
    rel_l.start()
    forward(2 * right + c, 1)

    def landing(src, i, s, count):
        return qall.at[i, pl.ds(s, count), pl.ds(pl.multiple_of(src * rows, rows), rows)]

    def direct(slot, i, who):
        return remote(
            scode.at[slot, i], landing(k, i, 0, SEGS),
            q_send.at[slot * drafts + i], q_recv.at[k * units + i * SEGS], who,
        )

    def out_far(way, i):
        who = 2 * (right if way == 0 else left) + c
        return remote(
            scode.at[way, i], rbuf.at[way, i],
            q_send.at[way * drafts + i], r_recv.at[way * drafts + i], who,
        )

    def relay(way, i, s, count):
        src = 2 * (left if way == 0 else right) + c
        who = 2 * (right if way == 0 else left) + way
        return remote(
            rbuf.at[way, i, pl.ds(s, count)], landing(src, i, s, count),
            r_send.at[way * units + i * SEGS + s], q_recv.at[src * units + i * SEGS + s], who,
        )

    def send_far(i):
        out_far(0, i).start()
        out_far(1, i).start()

    def send_near(i, cc):
        direct(2 + cc, i, 2 * right + cc).start()
        direct(4 + cc, i, 2 * left + cc).start()

    def pass_on(i):
        for way in range(2):
            out_far(way, i).wait_recv()
        for s, count in PIECES[i]:
            for way in range(2):
                relay(way, i, s, count).start()

    def landed(src, i, s, count):
        remote(
            landing(src, i, s, count), landing(src, i, s, count), q_send.at[0],
            q_recv.at[src * units + i * SEGS + s], mate,
        ).wait_recv()

    encode(2 * right, to_slot(2))
    encode(2 * right + 1, to_slot(3))
    encode(2 * left, to_slot(4))
    encode(2 * left + 1, to_slot(5))

    hwait(2 * left + c, 1)
    forward(2 * left + c, 1)
    hwait(2 * right + c, 0)
    forward(2 * right + c, 0)

    send_far(0)
    send_near(0, 0)
    send_near(0, 1)
    encode(mate, to_slot(6))
    encode(k, to_self)

    for i in range(drafts):
        direct(6, i, mate).start()

    hwait(2 * far + c, 0)
    forward(2 * far + c, 0)
    hwait(2 * far + c, 1)
    forward(2 * far + c, 1)
    for chip in (x, left, right, far):
        for half in range(2):
            hwait(2 * chip + 1 - c, half)

    def step(t, top):
        slot = t % 2

        @pl.when(t == 2)
        def _():
            pass_on(0)

        @pl.when(t == 4)
        def _():
            send_far(1)

        @pl.when(t == 6)
        def _():
            send_near(1, 0)

        @pl.when(t == 7)
        def _():
            send_near(1, 1)

        w_cp(t, slot).wait()
        prod = INV_TEMP * lax.dot_general(
            wbuf[slot], hall[...].reshape(positions * batch, dim), (((1,), (1,)), ((), ())), preferred_element_type=F32
        )
        base = pl.multiple_of(off + t * wrows, 8)
        for i in range(positions):
            z[i, pl.ds(base, wrows), :] = prod[:, i * batch:(i + 1) * batch]

        @pl.when(t + 2 < STEPS)
        def _():
            w_cp(t + 2, slot).start()

        return jnp.maximum(top, jnp.max(prod.reshape(wrows // 8, 8, positions * batch), axis=0))

    top = lax.fori_loop(0, STEPS, step, jnp.full((8, positions * batch), -jnp.inf, F32))
    own_max = jnp.max(top, axis=0, keepdims=True)

    chunk = 160
    row_i = lax.broadcasted_iota(jnp.int32, (chunk, batch), 0)
    for i in range(positions):
        m_i = own_max[:, i * batch:(i + 1) * batch]
        want = tok_ref[i:i + 1, :] - k * vocab if i < drafts else None

        def expo(t, carry, i=i, m_i=m_i, want=want):
            total, got = carry
            at = pl.ds(pl.multiple_of(off + t * chunk, 8), chunk)
            e = jnp.exp(z[i, at, :] - m_i)
            z[i, at, :] = e
            total = total + jnp.sum(e.reshape(chunk // 8, 8, batch), axis=0)
            if want is not None:
                pick = jnp.where(row_i + t * chunk == want, e, 0.0)
                got = got + jnp.sum(pick.reshape(chunk // 8, 8, batch), axis=0)
            return total, got

        zero = jnp.zeros((8, batch), F32)
        total, got = lax.fori_loop(0, vocab // chunk, expo, (zero, zero))
        msgs[k, i:i + 1, :] = m_i
        msgs[k, 3 + i:4 + i, :] = jnp.sum(total, axis=0, keepdims=True)
        if i < drafts:
            msgs[k, 6 + i:7 + i, :] = jnp.sum(got, axis=0, keepdims=True)

    def msg(p, src):
        return remote(msgs.at[src], msgs.at[src], m_send.at[p], m_recv.at[src], (k + p) % n)

    for p in range(1, n):
        msg(p, k).start()

    pass_on(1)
    for p in range(1, n):
        msg(p, (k + p) % n).wait_recv()

    allm = msgs[...]
    peak = jnp.max(allm[:, 0:3, :], axis=0)
    part = jnp.exp(allm[:, 0:3, :] - peak[None])
    inv = 1.0 / jnp.sum(part * allm[:, 3:6, :], axis=0)
    p_pick = jnp.sum(part[:, 0:drafts, :] * allm[:, 6:8, :], axis=0) * inv[0:drafts]
    q_pick = jnp.sum(allm[:, 8:10, :], axis=0)
    q_scale = jnp.sum(allm[:, 10:12, :], axis=0) * (1.0 / (TOP * TOP * TOP * TOP))
    fac = jnp.exp(msgs[k, 0:3, :] - peak) * inv

    def scale(t, _):
        at = pl.ds(pl.multiple_of(off + t * chunk, 8), chunk)
        z[drafts, at, :] = z[drafts, at, :] * fac[drafts:drafts + 1, :]
        return 0

    lax.fori_loop(0, vocab // chunk, scale, 0)

    def xmsg(p, i, src):
        return remote(mass.at[i, src], mass.at[i, src], x_send.at[i * n + p], x_recv.at[i * n + src], (k + p) % n)

    near_srcs = [2 * right, 2 * right + 1, 2 * left, 2 * left + 1, mate]
    for i in range(drafts):
        acc = tuple(jnp.zeros((8, LANES), F32) for _ in range(batch // LANES))
        for src in near_srcs:
            landed(src, i, 0, SEGS)
        for s, count in PIECES[i]:
            if i == drafts - 1 and s > 0 and s + count == SEGS:
                for cp in own_sends + [rel_r, rel_l] + fwd:
                    cp.wait_send()
                for p in range(1, n):
                    msg(p, k).wait_send()
                for u in range((n - 1) * drafts):
                    direct(u // drafts, u % drafts, mate).wait_send()
            for cc in range(2):
                landed(2 * far + cc, i, s, count)

            def body(t, acc, i=i, s=s):
                at = pl.ds(pl.multiple_of((s * per + t) * LANES, LANES), LANES)
                sub = pl.ds(pl.multiple_of((t % per) * LANES, LANES), LANES)
                out = []
                for h in range(batch // LANES):
                    ls = slice(h * LANES, (h + 1) * LANES)
                    code = qall[i, s + t // per, ls, sub].astype(jnp.int32).astype(F32)
                    y = code.T + float(HALF)
                    y = y * y
                    qt = y * y * q_scale[i:i + 1, ls]
                    ex = jnp.maximum(z[i, at, ls] * fac[i:i + 1, ls] - qt, 0.0)
                    z[i, at, ls] = ex
                    out.append(acc[h] + jnp.sum(ex.reshape(LANES // 8, 8, LANES), axis=0))
                return tuple(out)

            acc = lax.fori_loop(0, count * per, body, acc)
        for h in range(batch // LANES):
            mass[i, k, :, h * LANES:(h + 1) * LANES] = jnp.sum(acc[h], axis=0, keepdims=True)
        for p in range(1, n):
            xmsg(p, i, k).start()
    for i in range(drafts):
        for s, count in PIECES[i]:
            for way in range(2):
                relay(way, i, s, count).wait_send()
    small_ref[...] = jnp.zeros(small_ref.shape, F32)
    small_ref[2:4, :] = p_pick
    small_ref[4:6, :] = q_pick
    for i in range(drafts):
        for p in range(1, n):
            xmsg(p, i, (k + p) % n).wait_recv()
        total = jnp.sum(mass[i], axis=0)
        small_ref[i:i + 1, :] = 1.0 / total

    for p in range(1, n):
        for i in range(drafts):
            xmsg(p, i, k).wait_send()


def finish(n, z, small, res_ref, bonus_ref, acc_ref, exp_ref, buf, sem):
    drafts, vocab, _ = res_ref.shape
    off = pl.multiple_of((lax.axis_index("tp") * vocab) % LANES, 8)
    last = pltpu.make_async_copy(z.at[drafts, pl.ds(off, vocab), :], bonus_ref, sem.at[0])
    last.start()
    copies = [last]
    part = vocab // PARTS
    for i in range(drafts):
        scale = small[i:i + 1, :]
        for t in range(PARTS):
            to = pl.ds(t * part, part)
            buf[i, to, :] = z[i, pl.ds(pl.multiple_of(off + t * part, 8), part), :] * scale
            cp = pltpu.make_async_copy(buf.at[i, to], res_ref.at[i, to], sem.at[len(copies)])
            cp.start()
            copies.append(cp)
    accept = jnp.minimum(small[2:4, :] / small[4:6, :], 1.0)
    acc_ref[...] = accept
    exp_ref[...] = accept[0:1] + accept[0:1] * accept[1:2]
    for cp in copies:
        cp.wait()


def solution(mesh):
    n = mesh.shape["tp"]

    def local(hid, w, q, tok):
        rows, positions, dim = hid.shape
        vocab = w.shape[1]
        drafts = positions - 1
        batch = rows * n
        q_tiles = q.shape[2] // LANES
        width = -(-vocab // LANES) * LANES
        q_view = q.reshape(rows, drafts, q_tiles, LANES).transpose(0, 2, 1, 3)
        q_view = with_layout_constraint(q_view, Layout((0, 1, 2, 3))).reshape(-1, LANES)
        dma = pltpu.SemaphoreType.DMA
        vmem, anywhere = pl.BlockSpec(memory_space=pltpu.VMEM), pl.BlockSpec(memory_space=pltpu.HBM)
        z, small = pl.pallas_call(
            functools.partial(kernel, n),
            out_shape=(
                jax.ShapeDtypeStruct((positions, width, batch), F32),
                jax.ShapeDtypeStruct((8, batch), F32),
            ),
            in_specs=[anywhere] * 4,
            out_specs=(vmem, vmem),
            scratch_shapes=[
                pltpu.VMEM((drafts, batch), jnp.int32),
                pltpu.VMEM((positions, batch, dim), jnp.bfloat16),
                pltpu.VMEM((rows * q_tiles * drafts, LANES), F32),
                pltpu.VMEM((n - 1, drafts, SEGS, rows, width // SEGS), jnp.int16),
                pltpu.VMEM((drafts, SEGS, batch, width // SEGS), jnp.int16),
                pltpu.VMEM((2, drafts, SEGS, rows, width // SEGS), jnp.int16),
                pltpu.VMEM((2, vocab // STEPS, dim), jnp.bfloat16),
                pltpu.VMEM((n, 16, batch), F32),
                pltpu.VMEM((drafts, n, 1, batch), F32),
                pltpu.VMEM((drafts * (rows // 8), 8, LANES), F32),
                dma((8,)), dma((8,)), dma((2 * n,)),
                dma((n * drafts * SEGS,)), dma((n * drafts * SEGS,)), dma((2 * drafts * SEGS,)), dma((2 * drafts * SEGS,)),
                dma((n,)), dma((n,)), dma((2 * n,)), dma((2 * n,)),
                dma((8,)), dma((2,)),
            ],
            compiler_params=pltpu.CompilerParams(
                collective_id=0, has_side_effects=True, vmem_limit_bytes=40 * 2**20
            ),
        )(*[pltpu.with_memory_space_constraint(a, pltpu.HBM) for a in (tok.T, hid.transpose(1, 0, 2), w.T, q_view)])
        residual, bonus, accept, expected = pl.pallas_call(
            functools.partial(finish, n),
            out_shape=(
                jax.ShapeDtypeStruct((drafts, vocab, batch), F32),
                jax.ShapeDtypeStruct((vocab, batch), F32),
                jax.ShapeDtypeStruct((drafts, batch), F32),
                jax.ShapeDtypeStruct((1, batch), F32),
            ),
            in_specs=[vmem, vmem],
            out_specs=(anywhere, anywhere, vmem, vmem),
            scratch_shapes=[pltpu.VMEM((drafts, vocab, batch), F32), dma((drafts * PARTS + 1,))],
            compiler_params=pltpu.CompilerParams(vmem_limit_bytes=24 * 2**20),
        )(z, small)
        return accept.T, expected[0], residual.transpose(2, 0, 1), bonus.T

    return jax.shard_map(
        local,
        mesh=mesh,
        in_specs=(P(("dp", "tp"), None, None), P(None, "tp"), P(("dp", "tp"), None, None), P("dp", None)),
        out_specs=(P("dp", None), P("dp"), P("dp", None, "tp"), P("dp", "tp")),
        check_vma=False,
    )
```

```python
import functools

import jax
import jax.numpy as jnp
from jax import lax
from jax.experimental import pallas as pl
from jax.experimental.pallas import tpu as pltpu
from jax.experimental.layout import Layout, with_layout_constraint
from jax.sharding import PartitionSpec as P

INV_TEMP = 1.25
TOP = 65535.0
HALF = 32768
LANES = 128
SEGS = 4
PIECES = (((0, 4),), ((0, 2), (2, 1), (3, 1)))
STEPS = 10
PARTS = 5
F32 = jnp.float32
MESH = pl.DeviceIdType.MESH


def kernel(
    n, tok_in, hid_ref, w_ref, q_ref,
    z, small_ref,
    tok_ref, hall, stage, scode, qall, rbuf, wbuf, msgs, mass, rowc,
    h_send, h_fwd, h_recv, q_send, q_recv, r_send, r_recv,
    m_send, m_recv, x_send, x_recv, loc, wsem,
):
    k = lax.axis_index("tp")
    x, c = k // 2, k % 2
    chips = n // 2
    right, left = (x + 1) % chips, (x + chips - 1) % chips
    far = (x + 2) % chips
    mate = 2 * x + 1 - c
    positions, batch, dim = hall.shape
    drafts = positions - 1
    rows = batch // n
    vocab = w_ref.shape[0]
    seg = qall.shape[3]
    width = seg * SEGS
    tiles = width // LANES
    units = drafts * SEGS
    per = seg // LANES
    pitch = q_ref.shape[0] // rows
    all_tiles = pitch // drafts
    off = (k * vocab) % LANES
    hcol = dim // 2
    wrows = vocab // STEPS

    def remote(src, dst, ssem, rsem, who):
        return pltpu.make_async_remote_copy(
            src_ref=src, dst_ref=dst, send_sem=ssem, recv_sem=rsem,
            device_id={"tp": who}, device_id_type=MESH,
        )

    hid_cp = pltpu.make_async_copy(hid_ref, hall.at[:, pl.ds(k * rows, rows), :], loc.at[0])
    hid_cp.start()
    tok_cp = pltpu.make_async_copy(tok_in, tok_ref, loc.at[6])
    tok_cp.start()

    def stage_cp(g):
        part = pl.ds(g * 8 * pitch, 8 * pitch)
        return pltpu.make_async_copy(q_ref.at[part], stage.at[part], loc.at[1 + g])

    def w_cp(t, slot):
        return pltpu.make_async_copy(
            w_ref.at[pl.ds(pl.multiple_of(t * wrows, 8), wrows)], wbuf.at[slot], wsem.at[slot]
        )

    barrier = pltpu.get_barrier_semaphore()
    for who in (2 * right + c, 2 * left + c, mate):
        pl.semaphore_signal(barrier, inc=1, device_id={"tp": who}, device_id_type=MESH)
    pl.semaphore_wait(barrier, 3)

    def hpiece(src, half):
        return hall.at[:, pl.ds(pl.multiple_of(src * rows, rows), rows), pl.ds(half * hcol, hcol)]

    def hcopy(src, half, ssem, who):
        return remote(hpiece(src, half), hpiece(src, half), ssem, h_recv.at[src * 2 + half], who)

    def hwait(src, half):
        hcopy(src, half, h_send.at[0], mate).wait_recv()

    hid_cp.wait()
    own_sends = []
    for idx, (who, half) in enumerate(
        [(2 * right + c, 0), (2 * left + c, 1), (2 * right + c, 1), (2 * left + c, 0), (mate, 0), (mate, 1)]
    ):
        cp = hcopy(k, half, h_send.at[idx], who)
        cp.start()
        own_sends.append(cp)
    for g in range(rows // 8):
        stage_cp(g).start()
    w_cp(0, 0).start()
    w_cp(1, 1).start()

    z[:, 0:96, :] = jnp.zeros((positions, 96, batch), F32)
    z[:, width - 96:width, :] = jnp.zeros((positions, 96, batch), F32)

    tok_cp.wait()
    for g in range(rows // 8):
        stage_cp(g).wait()

    def qrows(g, i, j):
        return stage[pl.ds(g * 8 * pitch + drafts * j + i, 8, stride=pitch), :]

    groups = [(i, g) for i in range(drafts) for g in range(rows // 8)]
    lane_b = lax.broadcasted_iota(jnp.int32, (8, batch), 1)
    sub_b = lax.broadcasted_iota(jnp.int32, (8, batch), 0)
    lane_t = lax.broadcasted_iota(jnp.int32, (8, LANES), 1)
    mine = [lane_b == k * rows + 8 * g + sub_b for g in range(rows // 8)]
    tok_col = []
    for i, g in groups:
        t = jnp.where(mine[g], jnp.broadcast_to(tok_ref[i:i + 1, :].astype(F32), (8, batch)), 0.0)
        tok_col.append(jnp.broadcast_to(jnp.sum(t, axis=1, keepdims=True), (8, LANES)).astype(jnp.int32))

    def scan(j, carry):
        top, got = carry
        new_top, new_got = [], []
        col = lane_t + j * LANES
        for a, (i, g) in enumerate(groups):
            v = qrows(g, i, j)
            new_top.append(jnp.maximum(top[a], v))
            new_got.append(jnp.where(col == tok_col[a], v, got[a]))
        return tuple(new_top), tuple(new_got)

    zero8 = tuple(jnp.zeros((8, LANES), F32) for _ in groups)
    top, got = lax.fori_loop(0, all_tiles, scan, (zero8, zero8))
    qtop_row, qgot_row = [], []
    for i in range(drafts):
        acc_t = jnp.zeros((8, batch), F32)
        acc_g = jnp.zeros((8, batch), F32)
        for a, (ii, g) in enumerate(groups):
            if ii != i:
                continue
            tcol = jnp.max(top[a], axis=1, keepdims=True)
            gcol = jnp.sum(got[a], axis=1, keepdims=True)
            rowc[a] = jnp.broadcast_to(jnp.log(TOP) - 0.25 * jnp.log(tcol), (8, LANES))
            acc_t = acc_t + jnp.where(mine[g], jnp.broadcast_to(tcol, (8, batch)), 0.0)
            acc_g = acc_g + jnp.where(mine[g], jnp.broadcast_to(gcol, (8, batch)), 0.0)
        qtop_row.append(jnp.sum(acc_t, axis=0, keepdims=True))
        qgot_row.append(jnp.sum(acc_g, axis=0, keepdims=True))
    msgs[k] = jnp.zeros(msgs.shape[1:], F32)
    for i in range(drafts):
        msgs[k, 8 + i:9 + i, :] = qgot_row[i]
        msgs[k, 10 + i:11 + i, :] = qtop_row[i]

    def encode(dest, put):
        first = (dest * vocab) // LANES

        def body(j, _):
            for i in range(drafts):
                for gg in range(rows // 16):
                    parts = []
                    for g in (2 * gg, 2 * gg + 1):
                        v = qrows(g, i, first + j)
                        y = jnp.exp(0.25 * jnp.log(v) + rowc[i * (rows // 8) + g])
                        parts.append((y + 0.5).astype(jnp.int32) - HALF)
                    code = jnp.concatenate(parts, axis=0).astype(jnp.int16)
                    put(i, gg, j // per, pl.ds(pl.multiple_of((j % per) * LANES, LANES), LANES), code)
            return 0

        lax.fori_loop(0, tiles, body, 0)

    def to_slot(r):
        def put(i, gg, s, cols, code):
            scode[r, i, s, 16 * gg:16 * gg + 16, cols] = code

        return put

    def to_self(i, gg, s, cols, code):
        qall[i, s, pl.ds(pl.multiple_of(k * rows + 16 * gg, 16), 16), cols] = code

    encode(2 * far, to_slot(0))
    encode(2 * far + 1, to_slot(1))

    fwd = []

    def forward(src, half):
        cp = hcopy(src, half, h_fwd.at[len(fwd)], mate)
        cp.start()
        fwd.append(cp)

    hwait(2 * left + c, 0)
    rel_r = hcopy(2 * left + c, 0, h_send.at[6], 2 * right + c)
    rel_r.start()
    forward(2 * left + c, 0)
    hwait(2 * right + c, 1)
    rel_l = hcopy(2 * right + c, 1, h_send.at[7], 2 * left + c)
    rel_l.start()
    forward(2 * right + c, 1)

    def landing(src, i, s, count):
        return qall.at[i, pl.ds(s, count), pl.ds(pl.multiple_of(src * rows, rows), rows)]

    def direct(slot, i, who):
        return remote(
            scode.at[slot, i], landing(k, i, 0, SEGS),
            q_send.at[slot * drafts + i], q_recv.at[k * units + i * SEGS], who,
        )

    def core_of(way):
        return c if way == 0 else 1 - c

    def out_far(way, i):
        who = 2 * (right if way == 0 else left) + c
        return remote(
            scode.at[core_of(way), i], rbuf.at[way, i],
            q_send.at[core_of(way) * drafts + i], r_recv.at[way * drafts + i], who,
        )

    def relay(way, i, s, count):
        src = 2 * (left if way == 0 else right) + c
        who = 2 * (right if way == 0 else left) + core_of(way)
        return remote(
            rbuf.at[way, i, pl.ds(s, count)], landing(src, i, s, count),
            r_send.at[way * units + i * SEGS + s], q_recv.at[src * units + i * SEGS + s], who,
        )

    def send_far(i):
        out_far(0, i).start()
        out_far(1, i).start()

    def send_near(i, cc):
        direct(2 + cc, i, 2 * right + cc).start()
        direct(4 + cc, i, 2 * left + cc).start()

    def pass_on(i):
        for way in range(2):
            out_far(way, i).wait_recv()
        for s, count in PIECES[i]:
            for way in range(2):
                relay(way, i, s, count).start()

    def landed(src, i, s, count):
        remote(
            landing(src, i, s, count), landing(src, i, s, count), q_send.at[0],
            q_recv.at[src * units + i * SEGS + s], mate,
        ).wait_recv()

    encode(2 * right, to_slot(2))
    encode(2 * right + 1, to_slot(3))
    encode(2 * left, to_slot(4))
    encode(2 * left + 1, to_slot(5))

    hwait(2 * left + c, 1)
    forward(2 * left + c, 1)
    hwait(2 * right + c, 0)
    forward(2 * right + c, 0)

    send_far(0)
    send_near(0, c)
    send_near(0, 1 - c)
    encode(mate, to_slot(6))
    encode(k, to_self)

    for i in range(drafts):
        direct(6, i, mate).start()

    hwait(2 * far + c, 0)
    forward(2 * far + c, 0)
    hwait(2 * far + c, 1)
    forward(2 * far + c, 1)
    for chip in (x, left, right, far):
        for half in range(2):
            hwait(2 * chip + 1 - c, half)

    def step(t, top):
        slot = t % 2

        @pl.when(t == 2)
        def _():
            pass_on(0)

        @pl.when(t == 4)
        def _():
            send_far(1)

        @pl.when(t == 6)
        def _():
            send_near(1, c)

        @pl.when(t == 7)
        def _():
            send_near(1, 1 - c)

        w_cp(t, slot).wait()
        prod = INV_TEMP * lax.dot_general(
            wbuf[slot], hall[...].reshape(positions * batch, dim), (((1,), (1,)), ((), ())), preferred_element_type=F32
        )
        base = pl.multiple_of(off + t * wrows, 8)
        for i in range(positions):
            z[i, pl.ds(base, wrows), :] = prod[:, i * batch:(i + 1) * batch]

        @pl.when(t + 2 < STEPS)
        def _():
            w_cp(t + 2, slot).start()

        return jnp.maximum(top, jnp.max(prod.reshape(wrows // 8, 8, positions * batch), axis=0))

    top = lax.fori_loop(0, STEPS, step, jnp.full((8, positions * batch), -jnp.inf, F32))
    own_max = jnp.max(top, axis=0, keepdims=True)

    chunk = 160
    row_i = lax.broadcasted_iota(jnp.int32, (chunk, batch), 0)
    for i in range(positions):
        m_i = own_max[:, i * batch:(i + 1) * batch]
        want = tok_ref[i:i + 1, :] - k * vocab if i < drafts else None

        def expo(t, carry, i=i, m_i=m_i, want=want):
            total, got = carry
            at = pl.ds(pl.multiple_of(off + t * chunk, 8), chunk)
            e = jnp.exp(z[i, at, :] - m_i)
            z[i, at, :] = e
            total = total + jnp.sum(e.reshape(chunk // 8, 8, batch), axis=0)
            if want is not None:
                pick = jnp.where(row_i + t * chunk == want, e, 0.0)
                got = got + jnp.sum(pick.reshape(chunk // 8, 8, batch), axis=0)
            return total, got

        zero = jnp.zeros((8, batch), F32)
        total, got = lax.fori_loop(0, vocab // chunk, expo, (zero, zero))
        msgs[k, i:i + 1, :] = m_i
        msgs[k, 3 + i:4 + i, :] = jnp.sum(total, axis=0, keepdims=True)
        if i < drafts:
            msgs[k, 6 + i:7 + i, :] = jnp.sum(got, axis=0, keepdims=True)

    def msg(p, src):
        return remote(msgs.at[src], msgs.at[src], m_send.at[p], m_recv.at[src], (k + p) % n)

    for p in range(1, n):
        msg(p, k).start()

    pass_on(1)
    for p in range(1, n):
        msg(p, (k + p) % n).wait_recv()

    allm = msgs[...]
    peak = jnp.max(allm[:, 0:3, :], axis=0)
    part = jnp.exp(allm[:, 0:3, :] - peak[None])
    inv = 1.0 / jnp.sum(part * allm[:, 3:6, :], axis=0)
    p_pick = jnp.sum(part[:, 0:drafts, :] * allm[:, 6:8, :], axis=0) * inv[0:drafts]
    q_pick = jnp.sum(allm[:, 8:10, :], axis=0)
    q_scale = jnp.sum(allm[:, 10:12, :], axis=0) * (1.0 / (TOP * TOP * TOP * TOP))
    fac = jnp.exp(msgs[k, 0:3, :] - peak) * inv

    def scale(t, _):
        at = pl.ds(pl.multiple_of(off + t * chunk, 8), chunk)
        z[drafts, at, :] = z[drafts, at, :] * fac[drafts:drafts + 1, :]
        return 0

    lax.fori_loop(0, vocab // chunk, scale, 0)

    def xmsg(p, i, src):
        return remote(mass.at[i, src], mass.at[i, src], x_send.at[i * n + p], x_recv.at[i * n + src], (k + p) % n)

    near_srcs = [2 * right, 2 * right + 1, 2 * left, 2 * left + 1, mate]
    for i in range(drafts):
        acc = tuple(jnp.zeros((8, LANES), F32) for _ in range(batch // LANES))
        for src in near_srcs:
            landed(src, i, 0, SEGS)
        for s, count in PIECES[i]:
            if i == drafts - 1 and s > 0 and s + count == SEGS:
                for cp in own_sends + [rel_r, rel_l] + fwd:
                    cp.wait_send()
                for p in range(1, n):
                    msg(p, k).wait_send()
                for u in range((n - 1) * drafts):
                    direct(u // drafts, u % drafts, mate).wait_send()
            for cc in range(2):
                landed(2 * far + cc, i, s, count)

            def body(t, acc, i=i, s=s):
                at = pl.ds(pl.multiple_of((s * per + t) * LANES, LANES), LANES)
                sub = pl.ds(pl.multiple_of((t % per) * LANES, LANES), LANES)
                out = []
                for h in range(batch // LANES):
                    ls = slice(h * LANES, (h + 1) * LANES)
                    code = qall[i, s + t // per, ls, sub].astype(jnp.int32).astype(F32)
                    y = code.T + float(HALF)
                    y = y * y
                    qt = y * y * q_scale[i:i + 1, ls]
                    ex = jnp.maximum(z[i, at, ls] * fac[i:i + 1, ls] - qt, 0.0)
                    z[i, at, ls] = ex
                    out.append(acc[h] + jnp.sum(ex.reshape(LANES // 8, 8, LANES), axis=0))
                return tuple(out)

            acc = lax.fori_loop(0, count * per, body, acc)
        for h in range(batch // LANES):
            mass[i, k, :, h * LANES:(h + 1) * LANES] = jnp.sum(acc[h], axis=0, keepdims=True)
        for p in range(1, n):
            xmsg(p, i, k).start()
    for i in range(drafts):
        for s, count in PIECES[i]:
            for way in range(2):
                relay(way, i, s, count).wait_send()
    small_ref[...] = jnp.zeros(small_ref.shape, F32)
    small_ref[2:4, :] = p_pick
    small_ref[4:6, :] = q_pick
    for i in range(drafts):
        for p in range(1, n):
            xmsg(p, i, (k + p) % n).wait_recv()
        total = jnp.sum(mass[i], axis=0)
        small_ref[i:i + 1, :] = 1.0 / total

    for p in range(1, n):
        for i in range(drafts):
            xmsg(p, i, k).wait_send()


def finish(n, z, small, res_ref, bonus_ref, acc_ref, exp_ref, buf, sem):
    drafts, vocab, _ = res_ref.shape
    off = pl.multiple_of((lax.axis_index("tp") * vocab) % LANES, 8)
    last = pltpu.make_async_copy(z.at[drafts, pl.ds(off, vocab), :], bonus_ref, sem.at[0])
    last.start()
    copies = [last]
    part = vocab // PARTS
    for i in range(drafts):
        scale = small[i:i + 1, :]
        for t in range(PARTS):
            to = pl.ds(t * part, part)
            buf[i, to, :] = z[i, pl.ds(pl.multiple_of(off + t * part, 8), part), :] * scale
            cp = pltpu.make_async_copy(buf.at[i, to], res_ref.at[i, to], sem.at[len(copies)])
            cp.start()
            copies.append(cp)
    accept = jnp.minimum(small[2:4, :] / small[4:6, :], 1.0)
    acc_ref[...] = accept
    exp_ref[...] = accept[0:1] + accept[0:1] * accept[1:2]
    for cp in copies:
        cp.wait()


def solution(mesh):
    n = mesh.shape["tp"]

    def local(hid, w, q, tok):
        rows, positions, dim = hid.shape
        vocab = w.shape[1]
        drafts = positions - 1
        batch = rows * n
        q_tiles = q.shape[2] // LANES
        width = -(-vocab // LANES) * LANES
        q_view = q.reshape(rows, drafts, q_tiles, LANES).transpose(0, 2, 1, 3)
        q_view = with_layout_constraint(q_view, Layout((0, 1, 2, 3))).reshape(-1, LANES)
        dma = pltpu.SemaphoreType.DMA
        vmem, anywhere = pl.BlockSpec(memory_space=pltpu.VMEM), pl.BlockSpec(memory_space=pltpu.HBM)
        z, small = pl.pallas_call(
            functools.partial(kernel, n),
            out_shape=(
                jax.ShapeDtypeStruct((positions, width, batch), F32),
                jax.ShapeDtypeStruct((8, batch), F32),
            ),
            in_specs=[anywhere] * 4,
            out_specs=(vmem, vmem),
            scratch_shapes=[
                pltpu.VMEM((drafts, batch), jnp.int32),
                pltpu.VMEM((positions, batch, dim), jnp.bfloat16),
                pltpu.VMEM((rows * q_tiles * drafts, LANES), F32),
                pltpu.VMEM((n - 1, drafts, SEGS, rows, width // SEGS), jnp.int16),
                pltpu.VMEM((drafts, SEGS, batch, width // SEGS), jnp.int16),
                pltpu.VMEM((2, drafts, SEGS, rows, width // SEGS), jnp.int16),
                pltpu.VMEM((2, vocab // STEPS, dim), jnp.bfloat16),
                pltpu.VMEM((n, 16, batch), F32),
                pltpu.VMEM((drafts, n, 1, batch), F32),
                pltpu.VMEM((drafts * (rows // 8), 8, LANES), F32),
                dma((8,)), dma((8,)), dma((2 * n,)),
                dma((n * drafts * SEGS,)), dma((n * drafts * SEGS,)), dma((2 * drafts * SEGS,)), dma((2 * drafts * SEGS,)),
                dma((n,)), dma((n,)), dma((2 * n,)), dma((2 * n,)),
                dma((8,)), dma((2,)),
            ],
            compiler_params=pltpu.CompilerParams(
                collective_id=0, has_side_effects=True, vmem_limit_bytes=40 * 2**20
            ),
        )(*[pltpu.with_memory_space_constraint(a, pltpu.HBM) for a in (tok.T, hid.transpose(1, 0, 2), w.T, q_view)])
        residual, bonus, accept, expected = pl.pallas_call(
            functools.partial(finish, n),
            out_shape=(
                jax.ShapeDtypeStruct((drafts, vocab, batch), F32),
                jax.ShapeDtypeStruct((vocab, batch), F32),
                jax.ShapeDtypeStruct((drafts, batch), F32),
                jax.ShapeDtypeStruct((1, batch), F32),
            ),
            in_specs=[vmem, vmem],
            out_specs=(anywhere, anywhere, vmem, vmem),
            scratch_shapes=[pltpu.VMEM((drafts, vocab, batch), F32), dma((drafts * PARTS + 1,))],
            compiler_params=pltpu.CompilerParams(vmem_limit_bytes=24 * 2**20),
        )(z, small)
        return accept.T, expected[0], residual.transpose(2, 0, 1), bonus.T

    return jax.shard_map(
        local,
        mesh=mesh,
        in_specs=(P(("dp", "tp"), None, None), P(None, "tp"), P(("dp", "tp"), None, None), P("dp", None)),
        out_specs=(P("dp", None), P("dp"), P("dp", None, "tp"), P("dp", "tp")),
        check_vma=False,
    )
```

```python
import functools

import jax
import jax.numpy as jnp
from jax import lax
from jax.experimental import pallas as pl
from jax.experimental.pallas import tpu as pltpu
from jax.experimental.layout import Layout, with_layout_constraint
from jax.sharding import PartitionSpec as P

INV_TEMP = 1.25
TOP = 65535.0
HALF = 32768
LANES = 128
SEGS = 4
PIECES = (((0, 4),), ((0, 2), (2, 1), (3, 1)))
STEPS = 10
PARTS = 5
F32 = jnp.float32
MESH = pl.DeviceIdType.MESH


def kernel(
    n, tok_in, hid_ref, w_ref, q_ref,
    z, small_ref,
    tok_ref, hall, stage, scode, qall, rbuf, wbuf, msgs, mass, rowc,
    h_send, h_fwd, h_recv, q_send, q_recv, r_send, r_recv,
    m_send, m_recv, x_send, x_recv, loc, wsem,
):
    k = lax.axis_index("tp")
    x, c = k // 2, k % 2
    chips = n // 2
    right, left = (x + 1) % chips, (x + chips - 1) % chips
    far = (x + 2) % chips
    mate = 2 * x + 1 - c
    positions, batch, dim = hall.shape
    drafts = positions - 1
    rows = batch // n
    vocab = w_ref.shape[0]
    seg = qall.shape[3]
    width = seg * SEGS
    tiles = width // LANES
    units = drafts * SEGS
    per = seg // LANES
    pitch = q_ref.shape[0] // rows
    all_tiles = pitch // drafts
    off = (k * vocab) % LANES
    hcol = dim // 2
    wrows = vocab // STEPS

    def remote(src, dst, ssem, rsem, who):
        return pltpu.make_async_remote_copy(
            src_ref=src, dst_ref=dst, send_sem=ssem, recv_sem=rsem,
            device_id={"tp": who}, device_id_type=MESH,
        )

    hid_cp = pltpu.make_async_copy(hid_ref, hall.at[:, pl.ds(k * rows, rows), :], loc.at[0])
    hid_cp.start()
    tok_cp = pltpu.make_async_copy(tok_in, tok_ref, loc.at[6])
    tok_cp.start()

    def stage_cp(g):
        part = pl.ds(g * 8 * pitch, 8 * pitch)
        return pltpu.make_async_copy(q_ref.at[part], stage.at[part], loc.at[1 + g])

    def w_cp(t, slot):
        return pltpu.make_async_copy(
            w_ref.at[pl.ds(pl.multiple_of(t * wrows, 8), wrows)], wbuf.at[slot], wsem.at[slot]
        )

    barrier = pltpu.get_barrier_semaphore()
    for who in (2 * right + c, 2 * left + c, mate):
        pl.semaphore_signal(barrier, inc=1, device_id={"tp": who}, device_id_type=MESH)
    pl.semaphore_wait(barrier, 3)

    def hpiece(src, half):
        return hall.at[:, pl.ds(pl.multiple_of(src * rows, rows), rows), pl.ds(half * hcol, hcol)]

    def hcopy(src, half, ssem, who):
        return remote(hpiece(src, half), hpiece(src, half), ssem, h_recv.at[src * 2 + half], who)

    def hwait(src, half):
        hcopy(src, half, h_send.at[0], mate).wait_recv()

    hid_cp.wait()
    own_sends = []
    for idx, (who, half) in enumerate(
        [(2 * right + c, 0), (2 * left + c, 1), (mate, 0), (mate, 1), (2 * right + c, 1), (2 * left + c, 0)]
    ):
        cp = hcopy(k, half, h_send.at[idx], who)
        own_sends.append(cp)
    for cp in own_sends[:4]:
        cp.start()
    for g in range(rows // 8):
        stage_cp(g).start()
    w_cp(0, 0).start()
    w_cp(1, 1).start()

    z[:, 0:96, :] = jnp.zeros((positions, 96, batch), F32)
    z[:, width - 96:width, :] = jnp.zeros((positions, 96, batch), F32)

    tok_cp.wait()
    for g in range(rows // 8):
        stage_cp(g).wait()

    def qrows(g, i, j):
        return stage[pl.ds(g * 8 * pitch + drafts * j + i, 8, stride=pitch), :]

    groups = [(i, g) for i in range(drafts) for g in range(rows // 8)]
    lane_b = lax.broadcasted_iota(jnp.int32, (8, batch), 1)
    sub_b = lax.broadcasted_iota(jnp.int32, (8, batch), 0)
    lane_t = lax.broadcasted_iota(jnp.int32, (8, LANES), 1)
    mine = [lane_b == k * rows + 8 * g + sub_b for g in range(rows // 8)]
    tok_col = []
    for i, g in groups:
        t = jnp.where(mine[g], jnp.broadcast_to(tok_ref[i:i + 1, :].astype(F32), (8, batch)), 0.0)
        tok_col.append(jnp.broadcast_to(jnp.sum(t, axis=1, keepdims=True), (8, LANES)).astype(jnp.int32))

    def scan(j, carry):
        top, got = carry
        new_top, new_got = [], []
        col = lane_t + j * LANES
        for a, (i, g) in enumerate(groups):
            v = qrows(g, i, j)
            new_top.append(jnp.maximum(top[a], v))
            new_got.append(jnp.where(col == tok_col[a], v, got[a]))
        return tuple(new_top), tuple(new_got)

    zero8 = tuple(jnp.zeros((8, LANES), F32) for _ in groups)
    top, got = lax.fori_loop(0, all_tiles, scan, (zero8, zero8))
    qtop_row, qgot_row = [], []
    for i in range(drafts):
        acc_t = jnp.zeros((8, batch), F32)
        acc_g = jnp.zeros((8, batch), F32)
        for a, (ii, g) in enumerate(groups):
            if ii != i:
                continue
            tcol = jnp.max(top[a], axis=1, keepdims=True)
            gcol = jnp.sum(got[a], axis=1, keepdims=True)
            rowc[a] = jnp.broadcast_to(jnp.log(TOP) - 0.25 * jnp.log(tcol), (8, LANES))
            acc_t = acc_t + jnp.where(mine[g], jnp.broadcast_to(tcol, (8, batch)), 0.0)
            acc_g = acc_g + jnp.where(mine[g], jnp.broadcast_to(gcol, (8, batch)), 0.0)
        qtop_row.append(jnp.sum(acc_t, axis=0, keepdims=True))
        qgot_row.append(jnp.sum(acc_g, axis=0, keepdims=True))
    msgs[k] = jnp.zeros(msgs.shape[1:], F32)
    for i in range(drafts):
        msgs[k, 8 + i:9 + i, :] = qgot_row[i]
        msgs[k, 10 + i:11 + i, :] = qtop_row[i]

    def encode(dest, put):
        first = (dest * vocab) // LANES

        def body(j, _):
            for i in range(drafts):
                for gg in range(rows // 16):
                    parts = []
                    for g in (2 * gg, 2 * gg + 1):
                        v = qrows(g, i, first + j)
                        y = jnp.exp(0.25 * jnp.log(v) + rowc[i * (rows // 8) + g])
                        parts.append((y + 0.5).astype(jnp.int32) - HALF)
                    code = jnp.concatenate(parts, axis=0).astype(jnp.int16)
                    put(i, gg, j // per, pl.ds(pl.multiple_of((j % per) * LANES, LANES), LANES), code)
            return 0

        lax.fori_loop(0, tiles, body, 0)

    def to_slot(r):
        def put(i, gg, s, cols, code):
            scode[r, i, s, 16 * gg:16 * gg + 16, cols] = code

        return put

    def to_self(i, gg, s, cols, code):
        qall[i, s, pl.ds(pl.multiple_of(k * rows + 16 * gg, 16), 16), cols] = code

    encode(2 * far, to_slot(0))
    encode(2 * far + 1, to_slot(1))

    fwd = []

    def forward(src, half):
        cp = hcopy(src, half, h_fwd.at[len(fwd)], mate)
        cp.start()
        fwd.append(cp)

    own_sends[0].wait_send()
    own_sends[4].start()
    own_sends[1].wait_send()
    own_sends[5].start()
    hwait(2 * left + c, 0)
    rel_r = hcopy(2 * left + c, 0, h_send.at[6], 2 * right + c)
    rel_r.start()
    forward(2 * left + c, 0)
    hwait(2 * right + c, 1)
    rel_l = hcopy(2 * right + c, 1, h_send.at[7], 2 * left + c)
    rel_l.start()
    forward(2 * right + c, 1)

    def landing(src, i, s, count):
        return qall.at[i, pl.ds(s, count), pl.ds(pl.multiple_of(src * rows, rows), rows)]

    def direct(slot, i, who):
        return remote(
            scode.at[slot, i], landing(k, i, 0, SEGS),
            q_send.at[slot * drafts + i], q_recv.at[k * units + i * SEGS], who,
        )

    def core_of(way):
        return c if way == 0 else 1 - c

    def out_far(way, i):
        who = 2 * (right if way == 0 else left) + c
        return remote(
            scode.at[core_of(way), i], rbuf.at[way, i],
            q_send.at[core_of(way) * drafts + i], r_recv.at[way * drafts + i], who,
        )

    def relay(way, i, s, count):
        src = 2 * (left if way == 0 else right) + c
        who = 2 * (right if way == 0 else left) + core_of(way)
        return remote(
            rbuf.at[way, i, pl.ds(s, count)], landing(src, i, s, count),
            r_send.at[way * units + i * SEGS + s], q_recv.at[src * units + i * SEGS + s], who,
        )

    def send_far(i):
        out_far(0, i).start()
        out_far(1, i).start()

    def send_near(i, cc):
        direct(2 + cc, i, 2 * right + cc).start()
        direct(4 + cc, i, 2 * left + cc).start()

    def pass_on(i):
        for way in range(2):
            out_far(way, i).wait_recv()
        for s, count in PIECES[i]:
            for way in range(2):
                relay(way, i, s, count).start()

    def landed(src, i, s, count):
        remote(
            landing(src, i, s, count), landing(src, i, s, count), q_send.at[0],
            q_recv.at[src * units + i * SEGS + s], mate,
        ).wait_recv()

    encode(2 * right, to_slot(2))
    encode(2 * right + 1, to_slot(3))
    encode(2 * left, to_slot(4))
    encode(2 * left + 1, to_slot(5))

    encode(mate, to_slot(6))
    encode(k, to_self)
    for cp in own_sends[4:6]:
        cp.wait_send()
    send_far(0)
    send_far(1)
    for i in range(drafts):
        direct(6, i, mate).start()
    hwait(2 * left + c, 1)
    forward(2 * left + c, 1)
    hwait(2 * right + c, 0)
    forward(2 * right + c, 0)
    hwait(2 * far + c, 0)
    forward(2 * far + c, 0)
    hwait(2 * far + c, 1)
    forward(2 * far + c, 1)
    for chip in (x, left, right, far):
        for half in range(2):
            hwait(2 * chip + 1 - c, half)

    def step(t, top):
        slot = t % 2

        for when, act in (
            (1, lambda: send_near(0, c)),
            (3, lambda: send_near(0, 1 - c)),
            (5, lambda: pass_on(0)),
            (6, lambda: send_near(1, c)),
            (8, lambda: pass_on(1)),
            (9, lambda: send_near(1, 1 - c)),
        ):
            pl.when(t == when)(act)

        w_cp(t, slot).wait()
        prod = INV_TEMP * lax.dot_general(
            wbuf[slot], hall[...].reshape(positions * batch, dim), (((1,), (1,)), ((), ())), preferred_element_type=F32
        )
        base = pl.multiple_of(off + t * wrows, 8)
        for i in range(positions):
            z[i, pl.ds(base, wrows), :] = prod[:, i * batch:(i + 1) * batch]

        @pl.when(t + 2 < STEPS)
        def _():
            w_cp(t + 2, slot).start()

        return jnp.maximum(top, jnp.max(prod.reshape(wrows // 8, 8, positions * batch), axis=0))

    top = lax.fori_loop(0, STEPS, step, jnp.full((8, positions * batch), -jnp.inf, F32))
    own_max = jnp.max(top, axis=0, keepdims=True)

    chunk = 160
    row_i = lax.broadcasted_iota(jnp.int32, (chunk, batch), 0)
    for i in range(positions):
        m_i = own_max[:, i * batch:(i + 1) * batch]
        want = tok_ref[i:i + 1, :] - k * vocab if i < drafts else None

        def expo(t, carry, i=i, m_i=m_i, want=want):
            total, got = carry
            at = pl.ds(pl.multiple_of(off + t * chunk, 8), chunk)
            e = jnp.exp(z[i, at, :] - m_i)
            z[i, at, :] = e
            total = total + jnp.sum(e.reshape(chunk // 8, 8, batch), axis=0)
            if want is not None:
                pick = jnp.where(row_i + t * chunk == want, e, 0.0)
                got = got + jnp.sum(pick.reshape(chunk // 8, 8, batch), axis=0)
            return total, got

        zero = jnp.zeros((8, batch), F32)
        total, got = lax.fori_loop(0, vocab // chunk, expo, (zero, zero))
        msgs[k, i:i + 1, :] = m_i
        msgs[k, 3 + i:4 + i, :] = jnp.sum(total, axis=0, keepdims=True)
        if i < drafts:
            msgs[k, 6 + i:7 + i, :] = jnp.sum(got, axis=0, keepdims=True)

    def msg(p, src):
        return remote(msgs.at[src], msgs.at[src], m_send.at[p], m_recv.at[src], (k + p) % n)

    for p in range(1, n):
        msg(p, k).start()

    for p in range(1, n):
        msg(p, (k + p) % n).wait_recv()

    allm = msgs[...]
    peak = jnp.max(allm[:, 0:3, :], axis=0)
    part = jnp.exp(allm[:, 0:3, :] - peak[None])
    inv = 1.0 / jnp.sum(part * allm[:, 3:6, :], axis=0)
    p_pick = jnp.sum(part[:, 0:drafts, :] * allm[:, 6:8, :], axis=0) * inv[0:drafts]
    q_pick = jnp.sum(allm[:, 8:10, :], axis=0)
    q_scale = jnp.sum(allm[:, 10:12, :], axis=0) * (1.0 / (TOP * TOP * TOP * TOP))
    fac = jnp.exp(msgs[k, 0:3, :] - peak) * inv

    def scale(t, _):
        at = pl.ds(pl.multiple_of(off + t * chunk, 8), chunk)
        z[drafts, at, :] = z[drafts, at, :] * fac[drafts:drafts + 1, :]
        return 0

    lax.fori_loop(0, vocab // chunk, scale, 0)

    def xmsg(p, i, src):
        return remote(mass.at[i, src], mass.at[i, src], x_send.at[i * n + p], x_recv.at[i * n + src], (k + p) % n)

    near_srcs = [2 * right, 2 * right + 1, 2 * left, 2 * left + 1, mate]
    for i in range(drafts):
        acc = tuple(jnp.zeros((8, LANES), F32) for _ in range(batch // LANES))
        for src in near_srcs:
            landed(src, i, 0, SEGS)
        for s, count in PIECES[i]:
            if i == drafts - 1 and s > 0 and s + count == SEGS:
                for cp in own_sends[2:4] + [rel_r, rel_l] + fwd:
                    cp.wait_send()
                for p in range(1, n):
                    msg(p, k).wait_send()
                for u in range((n - 1) * drafts):
                    direct(u // drafts, u % drafts, mate).wait_send()
            for cc in range(2):
                landed(2 * far + cc, i, s, count)

            def body(t, acc, i=i, s=s):
                at = pl.ds(pl.multiple_of((s * per + t) * LANES, LANES), LANES)
                sub = pl.ds(pl.multiple_of((t % per) * LANES, LANES), LANES)
                out = []
                for h in range(batch // LANES):
                    ls = slice(h * LANES, (h + 1) * LANES)
                    code = qall[i, s + t // per, ls, sub].astype(jnp.int32).astype(F32)
                    y = code.T + float(HALF)
                    y = y * y
                    qt = y * y * q_scale[i:i + 1, ls]
                    ex = jnp.maximum(z[i, at, ls] * fac[i:i + 1, ls] - qt, 0.0)
                    z[i, at, ls] = ex
                    out.append(acc[h] + jnp.sum(ex.reshape(LANES // 8, 8, LANES), axis=0))
                return tuple(out)

            acc = lax.fori_loop(0, count * per, body, acc)
        for h in range(batch // LANES):
            mass[i, k, :, h * LANES:(h + 1) * LANES] = jnp.sum(acc[h], axis=0, keepdims=True)
        for p in range(1, n):
            xmsg(p, i, k).start()
    for i in range(drafts):
        for s, count in PIECES[i]:
            for way in range(2):
                relay(way, i, s, count).wait_send()
    small_ref[...] = jnp.zeros(small_ref.shape, F32)
    small_ref[2:4, :] = p_pick
    small_ref[4:6, :] = q_pick
    for i in range(drafts):
        for p in range(1, n):
            xmsg(p, i, (k + p) % n).wait_recv()
        total = jnp.sum(mass[i], axis=0)
        small_ref[i:i + 1, :] = 1.0 / total

    for p in range(1, n):
        for i in range(drafts):
            xmsg(p, i, k).wait_send()


def finish(n, z, small, res_ref, bonus_ref, acc_ref, exp_ref, buf, sem):
    drafts, vocab, _ = res_ref.shape
    off = pl.multiple_of((lax.axis_index("tp") * vocab) % LANES, 8)
    last = pltpu.make_async_copy(z.at[drafts, pl.ds(off, vocab), :], bonus_ref, sem.at[0])
    last.start()
    copies = [last]
    part = vocab // PARTS
    for i in range(drafts):
        scale = small[i:i + 1, :]
        for t in range(PARTS):
            to = pl.ds(t * part, part)
            buf[i, to, :] = z[i, pl.ds(pl.multiple_of(off + t * part, 8), part), :] * scale
            cp = pltpu.make_async_copy(buf.at[i, to], res_ref.at[i, to], sem.at[len(copies)])
            cp.start()
            copies.append(cp)
    accept = jnp.minimum(small[2:4, :] / small[4:6, :], 1.0)
    acc_ref[...] = accept
    exp_ref[...] = accept[0:1] + accept[0:1] * accept[1:2]
    for cp in copies:
        cp.wait()


def solution(mesh):
    n = mesh.shape["tp"]

    def local(hid, w, q, tok):
        rows, positions, dim = hid.shape
        vocab = w.shape[1]
        drafts = positions - 1
        batch = rows * n
        q_tiles = q.shape[2] // LANES
        width = -(-vocab // LANES) * LANES
        q_view = q.reshape(rows, drafts, q_tiles, LANES).transpose(0, 2, 1, 3)
        q_view = with_layout_constraint(q_view, Layout((0, 1, 2, 3))).reshape(-1, LANES)
        dma = pltpu.SemaphoreType.DMA
        vmem, anywhere = pl.BlockSpec(memory_space=pltpu.VMEM), pl.BlockSpec(memory_space=pltpu.HBM)
        z, small = pl.pallas_call(
            functools.partial(kernel, n),
            out_shape=(
                jax.ShapeDtypeStruct((positions, width, batch), F32),
                jax.ShapeDtypeStruct((8, batch), F32),
            ),
            in_specs=[anywhere] * 4,
            out_specs=(vmem, vmem),
            scratch_shapes=[
                pltpu.VMEM((drafts, batch), jnp.int32),
                pltpu.VMEM((positions, batch, dim), jnp.bfloat16),
                pltpu.VMEM((rows * q_tiles * drafts, LANES), F32),
                pltpu.VMEM((n - 1, drafts, SEGS, rows, width // SEGS), jnp.int16),
                pltpu.VMEM((drafts, SEGS, batch, width // SEGS), jnp.int16),
                pltpu.VMEM((2, drafts, SEGS, rows, width // SEGS), jnp.int16),
                pltpu.VMEM((2, vocab // STEPS, dim), jnp.bfloat16),
                pltpu.VMEM((n, 16, batch), F32),
                pltpu.VMEM((drafts, n, 1, batch), F32),
                pltpu.VMEM((drafts * (rows // 8), 8, LANES), F32),
                dma((8,)), dma((8,)), dma((2 * n,)),
                dma((n * drafts * SEGS,)), dma((n * drafts * SEGS,)), dma((2 * drafts * SEGS,)), dma((2 * drafts * SEGS,)),
                dma((n,)), dma((n,)), dma((2 * n,)), dma((2 * n,)),
                dma((8,)), dma((2,)),
            ],
            compiler_params=pltpu.CompilerParams(
                collective_id=0, has_side_effects=True, vmem_limit_bytes=40 * 2**20
            ),
        )(*[pltpu.with_memory_space_constraint(a, pltpu.HBM) for a in (tok.T, hid.transpose(1, 0, 2), w.T, q_view)])
        residual, bonus, accept, expected = pl.pallas_call(
            functools.partial(finish, n),
            out_shape=(
                jax.ShapeDtypeStruct((drafts, vocab, batch), F32),
                jax.ShapeDtypeStruct((vocab, batch), F32),
                jax.ShapeDtypeStruct((drafts, batch), F32),
                jax.ShapeDtypeStruct((1, batch), F32),
            ),
            in_specs=[vmem, vmem],
            out_specs=(anywhere, anywhere, vmem, vmem),
            scratch_shapes=[pltpu.VMEM((drafts, vocab, batch), F32), dma((drafts * PARTS + 1,))],
            compiler_params=pltpu.CompilerParams(vmem_limit_bytes=24 * 2**20),
        )(z, small)
        return accept.T, expected[0], residual.transpose(2, 0, 1), bonus.T

    return jax.shard_map(
        local,
        mesh=mesh,
        in_specs=(P(("dp", "tp"), None, None), P(None, "tp"), P(("dp", "tp"), None, None), P("dp", None)),
        out_specs=(P("dp", None), P("dp"), P("dp", None, "tp"), P("dp", "tp")),
        check_vma=False,
    )
```

```python
import functools

import jax
import jax.numpy as jnp
from jax import lax
from jax.experimental import pallas as pl
from jax.experimental.pallas import tpu as pltpu
from jax.experimental.layout import Layout, with_layout_constraint
from jax.sharding import PartitionSpec as P

INV_TEMP = 1.25
TOP = 65535.0
HALF = 32768
LANES = 128
SEGS = 4
PIECES = (((0, 4),), ((0, 2), (2, 1), (3, 1)))
STEPS = 10
PARTS = 5
F32 = jnp.float32
MESH = pl.DeviceIdType.MESH


def kernel(
    n, tok_in, hid_ref, w_ref, q_ref,
    z, small_ref,
    tok_ref, hall, stage, scode, qall, rbuf, wbuf, msgs, mass, rowc,
    h_send, h_fwd, h_recv, q_send, q_recv, r_send, r_recv,
    m_send, m_recv, x_send, x_recv, loc, wsem, p_send,
):
    k = lax.axis_index("tp")
    x, c = k // 2, k % 2
    chips = n // 2
    right, left = (x + 1) % chips, (x + chips - 1) % chips
    far = (x + 2) % chips
    mate = 2 * x + 1 - c
    positions, batch, dim = hall.shape
    drafts = positions - 1
    rows = batch // n
    vocab = w_ref.shape[0]
    seg = qall.shape[3]
    width = seg * SEGS
    tiles = width // LANES
    units = drafts * SEGS
    per = seg // LANES
    pitch = q_ref.shape[0] // rows
    all_tiles = pitch // drafts
    off = (k * vocab) % LANES
    hcol = dim // 2
    wrows = vocab // STEPS

    def remote(src, dst, ssem, rsem, who):
        return pltpu.make_async_remote_copy(
            src_ref=src, dst_ref=dst, send_sem=ssem, recv_sem=rsem,
            device_id={"tp": who}, device_id_type=MESH,
        )

    hid_cp = pltpu.make_async_copy(hid_ref, hall.at[:, pl.ds(k * rows, rows), :], loc.at[0])
    hid_cp.start()
    tok_cp = pltpu.make_async_copy(tok_in, tok_ref, loc.at[6])
    tok_cp.start()

    def stage_cp(g):
        part = pl.ds(g * 8 * pitch, 8 * pitch)
        return pltpu.make_async_copy(q_ref.at[part], stage.at[part], loc.at[1 + g])

    def w_cp(t, slot):
        return pltpu.make_async_copy(
            w_ref.at[pl.ds(pl.multiple_of(t * wrows, 8), wrows)], wbuf.at[slot], wsem.at[slot]
        )

    barrier = pltpu.get_barrier_semaphore()
    for who in (2 * right + c, 2 * left + c, mate):
        pl.semaphore_signal(barrier, inc=1, device_id={"tp": who}, device_id_type=MESH)
    pl.semaphore_wait(barrier, 3)

    def hpiece(src, half):
        return hall.at[:, pl.ds(pl.multiple_of(src * rows, rows), rows), pl.ds(half * hcol, hcol)]

    def hcopy(src, half, ssem, who):
        return remote(hpiece(src, half), hpiece(src, half), ssem, h_recv.at[src * 2 + half], who)

    def hwait(src, half):
        hcopy(src, half, h_send.at[0], mate).wait_recv()

    hid_cp.wait()
    own_sends = []
    for idx, (who, half) in enumerate(
        [(2 * right + c, 0), (2 * left + c, 1), (mate, 0), (mate, 1), (2 * right + c, 1), (2 * left + c, 0)]
    ):
        cp = hcopy(k, half, h_send.at[idx], who)
        own_sends.append(cp)
    for cp in own_sends[:4]:
        cp.start()
    for g in range(rows // 8):
        stage_cp(g).start()
    w_cp(0, 0).start()
    w_cp(1, 1).start()

    z[:, 0:96, :] = jnp.zeros((positions, 96, batch), F32)
    z[:, width - 96:width, :] = jnp.zeros((positions, 96, batch), F32)

    tok_cp.wait()
    for g in range(rows // 8):
        stage_cp(g).wait()

    def qrows(g, i, j):
        return stage[pl.ds(g * 8 * pitch + drafts * j + i, 8, stride=pitch), :]

    groups = [(i, g) for i in range(drafts) for g in range(rows // 8)]
    lane_b = lax.broadcasted_iota(jnp.int32, (8, batch), 1)
    sub_b = lax.broadcasted_iota(jnp.int32, (8, batch), 0)
    lane_t = lax.broadcasted_iota(jnp.int32, (8, LANES), 1)
    mine = [lane_b == k * rows + 8 * g + sub_b for g in range(rows // 8)]
    tok_col = []
    for i, g in groups:
        t = jnp.where(mine[g], jnp.broadcast_to(tok_ref[i:i + 1, :].astype(F32), (8, batch)), 0.0)
        tok_col.append(jnp.broadcast_to(jnp.sum(t, axis=1, keepdims=True), (8, LANES)).astype(jnp.int32))

    def scan(j, carry):
        top, got = carry
        new_top, new_got = [], []
        col = lane_t + j * LANES
        for a, (i, g) in enumerate(groups):
            v = qrows(g, i, j)
            new_top.append(jnp.maximum(top[a], v))
            new_got.append(jnp.where(col == tok_col[a], v, got[a]))
        return tuple(new_top), tuple(new_got)

    zero8 = tuple(jnp.zeros((8, LANES), F32) for _ in groups)
    top, got = lax.fori_loop(0, all_tiles, scan, (zero8, zero8))
    qtop_row, qgot_row = [], []
    for i in range(drafts):
        acc_t = jnp.zeros((8, batch), F32)
        acc_g = jnp.zeros((8, batch), F32)
        for a, (ii, g) in enumerate(groups):
            if ii != i:
                continue
            tcol = jnp.max(top[a], axis=1, keepdims=True)
            gcol = jnp.sum(got[a], axis=1, keepdims=True)
            rowc[a] = jnp.broadcast_to(jnp.log(TOP) - 0.25 * jnp.log(tcol), (8, LANES))
            acc_t = acc_t + jnp.where(mine[g], jnp.broadcast_to(tcol, (8, batch)), 0.0)
            acc_g = acc_g + jnp.where(mine[g], jnp.broadcast_to(gcol, (8, batch)), 0.0)
        qtop_row.append(jnp.sum(acc_t, axis=0, keepdims=True))
        qgot_row.append(jnp.sum(acc_g, axis=0, keepdims=True))
    msgs[k] = jnp.zeros(msgs.shape[1:], F32)
    for i in range(drafts):
        msgs[k, 8 + i:9 + i, :] = qgot_row[i]
        msgs[k, 10 + i:11 + i, :] = qtop_row[i]

    def encode(dest, put):
        first = (dest * vocab) // LANES

        def body(j, _):
            for i in range(drafts):
                for gg in range(rows // 16):
                    parts = []
                    for g in (2 * gg, 2 * gg + 1):
                        v = qrows(g, i, first + j)
                        y = jnp.exp(0.25 * jnp.log(v) + rowc[i * (rows // 8) + g])
                        parts.append((y + 0.5).astype(jnp.int32) - HALF)
                    code = jnp.concatenate(parts, axis=0).astype(jnp.int16)
                    put(i, gg, j // per, pl.ds(pl.multiple_of((j % per) * LANES, LANES), LANES), code)
            return 0

        lax.fori_loop(0, tiles, body, 0)

    def to_slot(r):
        def put(i, gg, s, cols, code):
            scode[r, i, s, 16 * gg:16 * gg + 16, cols] = code

        return put

    def to_self(i, gg, s, cols, code):
        qall[i, s, pl.ds(pl.multiple_of(k * rows + 16 * gg, 16), 16), cols] = code

    encode(2 * far, to_slot(0))
    encode(2 * far + 1, to_slot(1))

    fwd = []

    def forward(src, half):
        cp = hcopy(src, half, h_fwd.at[len(fwd)], mate)
        cp.start()
        fwd.append(cp)

    own_sends[0].wait_send()
    own_sends[4].start()
    own_sends[1].wait_send()
    own_sends[5].start()
    hwait(2 * left + c, 0)
    rel_r = hcopy(2 * left + c, 0, h_send.at[6], 2 * right + c)
    rel_r.start()
    forward(2 * left + c, 0)
    hwait(2 * right + c, 1)
    rel_l = hcopy(2 * right + c, 1, h_send.at[7], 2 * left + c)
    rel_l.start()
    forward(2 * right + c, 1)

    def landing(src, i, s, count):
        return qall.at[i, pl.ds(s, count), pl.ds(pl.multiple_of(src * rows, rows), rows)]

    def direct(slot, i, who):
        return remote(
            scode.at[slot, i], landing(k, i, 0, SEGS),
            q_send.at[slot * drafts + i], q_recv.at[k * units + i * SEGS], who,
        )

    def core_of(way):
        return c if way == 0 else 1 - c

    def out_far(way, i):
        who = 2 * (right if way == 0 else left) + c
        return remote(
            scode.at[core_of(way), i], rbuf.at[way, i],
            q_send.at[core_of(way) * drafts + i], r_recv.at[way * drafts + i], who,
        )

    def relay(way, i, s, count):
        src = 2 * (left if way == 0 else right) + c
        who = 2 * (right if way == 0 else left) + core_of(way)
        return remote(
            rbuf.at[way, i, pl.ds(s, count)], landing(src, i, s, count),
            r_send.at[way * units + i * SEGS + s], q_recv.at[src * units + i * SEGS + s], who,
        )

    def send_far(i):
        out_far(0, i).start()
        out_far(1, i).start()

    def piece(slot, s, count, who):
        i = drafts - 1
        return remote(
            scode.at[slot, i, pl.ds(s, count)], landing(k, i, s, count),
            p_send.at[slot * SEGS + s], q_recv.at[k * units + i * SEGS + s], who,
        )

    def last_pieces():
        for s, count in PIECES[drafts - 1]:
            yield piece(2 + 1 - c, s, count, 2 * right + 1 - c)
            yield piece(4 + 1 - c, s, count, 2 * left + 1 - c)

    def send_near(i, cc):
        direct(2 + cc, i, 2 * right + cc).start()
        direct(4 + cc, i, 2 * left + cc).start()

    def pass_on(i):
        for way in range(2):
            out_far(way, i).wait_recv()
        for way in range(2):
            relay(way, i, 0, SEGS).start()

    def landed(src, i, s, count):
        remote(
            landing(src, i, s, count), landing(src, i, s, count), q_send.at[0],
            q_recv.at[src * units + i * SEGS + s], mate,
        ).wait_recv()

    encode(2 * right, to_slot(2))
    encode(2 * right + 1, to_slot(3))
    encode(2 * left, to_slot(4))
    encode(2 * left + 1, to_slot(5))

    encode(mate, to_slot(6))
    encode(k, to_self)
    for cp in own_sends[4:6]:
        cp.wait_send()
    send_far(0)
    send_far(1)
    for i in range(drafts):
        direct(6, i, mate).start()
    hwait(2 * left + c, 1)
    forward(2 * left + c, 1)
    hwait(2 * right + c, 0)
    forward(2 * right + c, 0)
    hwait(2 * far + c, 0)
    forward(2 * far + c, 0)
    hwait(2 * far + c, 1)
    forward(2 * far + c, 1)
    for chip in (x, left, right, far):
        for half in range(2):
            hwait(2 * chip + 1 - c, half)

    def step(t, top):
        slot = t % 2

        for when, act in (
            (1, lambda: send_near(0, c)),
            (3, lambda: send_near(0, 1 - c)),
            (5, lambda: pass_on(0)),
            (6, lambda: send_near(1, c)),
            (8, lambda: pass_on(1)),
        ):
            pl.when(t == when)(act)

        w_cp(t, slot).wait()
        prod = INV_TEMP * lax.dot_general(
            wbuf[slot], hall[...].reshape(positions * batch, dim), (((1,), (1,)), ((), ())), preferred_element_type=F32
        )
        base = pl.multiple_of(off + t * wrows, 8)
        for i in range(positions):
            z[i, pl.ds(base, wrows), :] = prod[:, i * batch:(i + 1) * batch]

        @pl.when(t + 2 < STEPS)
        def _():
            w_cp(t + 2, slot).start()

        return jnp.maximum(top, jnp.max(prod.reshape(wrows // 8, 8, positions * batch), axis=0))

    top = lax.fori_loop(0, STEPS, step, jnp.full((8, positions * batch), -jnp.inf, F32))
    own_max = jnp.max(top, axis=0, keepdims=True)

    chunk = 160
    row_i = lax.broadcasted_iota(jnp.int32, (chunk, batch), 0)
    for i in range(positions):
        m_i = own_max[:, i * batch:(i + 1) * batch]
        want = tok_ref[i:i + 1, :] - k * vocab if i < drafts else None

        def expo(t, carry, i=i, m_i=m_i, want=want):
            total, got = carry
            at = pl.ds(pl.multiple_of(off + t * chunk, 8), chunk)
            e = jnp.exp(z[i, at, :] - m_i)
            z[i, at, :] = e
            total = total + jnp.sum(e.reshape(chunk // 8, 8, batch), axis=0)
            if want is not None:
                pick = jnp.where(row_i + t * chunk == want, e, 0.0)
                got = got + jnp.sum(pick.reshape(chunk // 8, 8, batch), axis=0)
            return total, got

        zero = jnp.zeros((8, batch), F32)
        total, got = lax.fori_loop(0, vocab // chunk, expo, (zero, zero))
        msgs[k, i:i + 1, :] = m_i
        msgs[k, 3 + i:4 + i, :] = jnp.sum(total, axis=0, keepdims=True)
        if i < drafts:
            msgs[k, 6 + i:7 + i, :] = jnp.sum(got, axis=0, keepdims=True)

    def msg(p, src):
        return remote(msgs.at[src], msgs.at[src], m_send.at[p], m_recv.at[src], (k + p) % n)

    for p in range(1, n):
        msg(p, k).start()

    for cp in last_pieces():
        cp.start()
    for p in range(1, n):
        msg(p, (k + p) % n).wait_recv()

    allm = msgs[...]
    peak = jnp.max(allm[:, 0:3, :], axis=0)
    part = jnp.exp(allm[:, 0:3, :] - peak[None])
    inv = 1.0 / jnp.sum(part * allm[:, 3:6, :], axis=0)
    p_pick = jnp.sum(part[:, 0:drafts, :] * allm[:, 6:8, :], axis=0) * inv[0:drafts]
    q_pick = jnp.sum(allm[:, 8:10, :], axis=0)
    q_scale = jnp.sum(allm[:, 10:12, :], axis=0) * (1.0 / (TOP * TOP * TOP * TOP))
    fac = jnp.exp(msgs[k, 0:3, :] - peak) * inv

    def scale(t, _):
        at = pl.ds(pl.multiple_of(off + t * chunk, 8), chunk)
        z[drafts, at, :] = z[drafts, at, :] * fac[drafts:drafts + 1, :]
        return 0

    lax.fori_loop(0, vocab // chunk, scale, 0)

    def xmsg(p, i, src):
        return remote(mass.at[i, src], mass.at[i, src], x_send.at[i * n + p], x_recv.at[i * n + src], (k + p) % n)

    whole = [[2 * chip + cc for chip in (left, right, far) for cc in range(2)] + [mate], []]
    whole[1] = [2 * left + c, 2 * right + c, 2 * far, 2 * far + 1, mate]
    for i in range(drafts):
        acc = tuple(jnp.zeros((8, LANES), F32) for _ in range(batch // LANES))
        for src in whole[i]:
            landed(src, i, 0, SEGS)
        for s, count in PIECES[i]:
            if i == drafts - 1 and s > 0 and s + count == SEGS:
                for cp in own_sends[2:4] + [rel_r, rel_l] + fwd:
                    cp.wait_send()
                for p in range(1, n):
                    msg(p, k).wait_send()
                for slot in (0, 1, 2 + c, 4 + c, 6):
                    for ii in range(drafts):
                        direct(slot, ii, mate).wait_send()
                for slot in (2 + 1 - c, 4 + 1 - c):
                    direct(slot, 0, mate).wait_send()
            if i == drafts - 1:
                for chip in (left, right):
                    landed(2 * chip + 1 - c, i, s, count)

            def body(t, acc, i=i, s=s):
                at = pl.ds(pl.multiple_of((s * per + t) * LANES, LANES), LANES)
                sub = pl.ds(pl.multiple_of((t % per) * LANES, LANES), LANES)
                out = []
                for h in range(batch // LANES):
                    ls = slice(h * LANES, (h + 1) * LANES)
                    code = qall[i, s + t // per, ls, sub].astype(jnp.int32).astype(F32)
                    y = code.T + float(HALF)
                    y = y * y
                    qt = y * y * q_scale[i:i + 1, ls]
                    ex = jnp.maximum(z[i, at, ls] * fac[i:i + 1, ls] - qt, 0.0)
                    z[i, at, ls] = ex
                    out.append(acc[h] + jnp.sum(ex.reshape(LANES // 8, 8, LANES), axis=0))
                return tuple(out)

            acc = lax.fori_loop(0, count * per, body, acc)
        for h in range(batch // LANES):
            mass[i, k, :, h * LANES:(h + 1) * LANES] = jnp.sum(acc[h], axis=0, keepdims=True)
        for p in range(1, n):
            xmsg(p, i, k).start()
    for i in range(drafts):
        for way in range(2):
            relay(way, i, 0, SEGS).wait_send()
    for cp in last_pieces():
        cp.wait_send()
    small_ref[...] = jnp.zeros(small_ref.shape, F32)
    small_ref[2:4, :] = p_pick
    small_ref[4:6, :] = q_pick
    for i in range(drafts):
        for p in range(1, n):
            xmsg(p, i, (k + p) % n).wait_recv()
        total = jnp.sum(mass[i], axis=0)
        small_ref[i:i + 1, :] = 1.0 / total

    for p in range(1, n):
        for i in range(drafts):
            xmsg(p, i, k).wait_send()


def finish(n, z, small, res_ref, bonus_ref, acc_ref, exp_ref, buf, sem):
    drafts, vocab, _ = res_ref.shape
    off = pl.multiple_of((lax.axis_index("tp") * vocab) % LANES, 8)
    last = pltpu.make_async_copy(z.at[drafts, pl.ds(off, vocab), :], bonus_ref, sem.at[0])
    last.start()
    copies = [last]
    part = vocab // PARTS
    for i in range(drafts):
        scale = small[i:i + 1, :]
        for t in range(PARTS):
            to = pl.ds(t * part, part)
            buf[i, to, :] = z[i, pl.ds(pl.multiple_of(off + t * part, 8), part), :] * scale
            cp = pltpu.make_async_copy(buf.at[i, to], res_ref.at[i, to], sem.at[len(copies)])
            cp.start()
            copies.append(cp)
    accept = jnp.minimum(small[2:4, :] / small[4:6, :], 1.0)
    acc_ref[...] = accept
    exp_ref[...] = accept[0:1] + accept[0:1] * accept[1:2]
    for cp in copies:
        cp.wait()


def solution(mesh):
    n = mesh.shape["tp"]

    def local(hid, w, q, tok):
        rows, positions, dim = hid.shape
        vocab = w.shape[1]
        drafts = positions - 1
        batch = rows * n
        q_tiles = q.shape[2] // LANES
        width = -(-vocab // LANES) * LANES
        q_view = q.reshape(rows, drafts, q_tiles, LANES).transpose(0, 2, 1, 3)
        q_view = with_layout_constraint(q_view, Layout((0, 1, 2, 3))).reshape(-1, LANES)
        dma = pltpu.SemaphoreType.DMA
        vmem, anywhere = pl.BlockSpec(memory_space=pltpu.VMEM), pl.BlockSpec(memory_space=pltpu.HBM)
        z, small = pl.pallas_call(
            functools.partial(kernel, n),
            out_shape=(
                jax.ShapeDtypeStruct((positions, width, batch), F32),
                jax.ShapeDtypeStruct((8, batch), F32),
            ),
            in_specs=[anywhere] * 4,
            out_specs=(vmem, vmem),
            scratch_shapes=[
                pltpu.VMEM((drafts, batch), jnp.int32),
                pltpu.VMEM((positions, batch, dim), jnp.bfloat16),
                pltpu.VMEM((rows * q_tiles * drafts, LANES), F32),
                pltpu.VMEM((n - 1, drafts, SEGS, rows, width // SEGS), jnp.int16),
                pltpu.VMEM((drafts, SEGS, batch, width // SEGS), jnp.int16),
                pltpu.VMEM((2, drafts, SEGS, rows, width // SEGS), jnp.int16),
                pltpu.VMEM((2, vocab // STEPS, dim), jnp.bfloat16),
                pltpu.VMEM((n, 16, batch), F32),
                pltpu.VMEM((drafts, n, 1, batch), F32),
                pltpu.VMEM((drafts * (rows // 8), 8, LANES), F32),
                dma((8,)), dma((8,)), dma((2 * n,)),
                dma((n * drafts * SEGS,)), dma((n * drafts * SEGS,)), dma((2 * drafts * SEGS,)), dma((2 * drafts * SEGS,)),
                dma((n,)), dma((n,)), dma((2 * n,)), dma((2 * n,)),
                dma((8,)), dma((2,)), dma((n * SEGS,)),
            ],
            compiler_params=pltpu.CompilerParams(
                collective_id=0, has_side_effects=True, vmem_limit_bytes=40 * 2**20
            ),
        )(*[pltpu.with_memory_space_constraint(a, pltpu.HBM) for a in (tok.T, hid.transpose(1, 0, 2), w.T, q_view)])
        residual, bonus, accept, expected = pl.pallas_call(
            functools.partial(finish, n),
            out_shape=(
                jax.ShapeDtypeStruct((drafts, vocab, batch), F32),
                jax.ShapeDtypeStruct((vocab, batch), F32),
                jax.ShapeDtypeStruct((drafts, batch), F32),
                jax.ShapeDtypeStruct((1, batch), F32),
            ),
            in_specs=[vmem, vmem],
            out_specs=(anywhere, anywhere, vmem, vmem),
            scratch_shapes=[pltpu.VMEM((drafts, vocab, batch), F32), dma((drafts * PARTS + 1,))],
            compiler_params=pltpu.CompilerParams(vmem_limit_bytes=24 * 2**20),
        )(z, small)
        return accept.T, expected[0], residual.transpose(2, 0, 1), bonus.T

    return jax.shard_map(
        local,
        mesh=mesh,
        in_specs=(P(("dp", "tp"), None, None), P(None, "tp"), P(("dp", "tp"), None, None), P("dp", None)),
        out_specs=(P("dp", None), P("dp"), P("dp", None, "tp"), P("dp", "tp")),
        check_vma=False,
    )
```

```python
import functools

import jax
import jax.numpy as jnp
from jax import lax
from jax.experimental import pallas as pl
from jax.experimental.pallas import tpu as pltpu
from jax.experimental.layout import Layout, with_layout_constraint
from jax.sharding import PartitionSpec as P

INV_TEMP = 1.25
TOP = 65535.0
HALF = 32768
LANES = 128
SEGS = 2
STEPS = 10
PARTS = 5
F32 = jnp.float32
MESH = pl.DeviceIdType.MESH


def kernel(
    n, tok_in, hid_ref, w_ref, q_ref,
    z, small_ref,
    tok_ref, hall, stage, scode, qall, rbuf, wbuf, msgs, mass, rowc,
    h_send, h_fwd, h_recv, q_send, q_recv, r_send, r_recv,
    m_send, m_recv, x_send, x_recv, loc, wsem,
):
    k = lax.axis_index("tp")
    x, c = k // 2, k % 2
    chips = n // 2
    right, left = (x + 1) % chips, (x + chips - 1) % chips
    far = (x + 2) % chips
    mate = 2 * x + 1 - c
    positions, batch, dim = hall.shape
    drafts = positions - 1
    rows = batch // n
    vocab = w_ref.shape[0]
    seg = qall.shape[3]
    width = seg * SEGS
    tiles = width // LANES
    units = drafts * SEGS
    per = seg // LANES
    pitch = q_ref.shape[0] // rows
    all_tiles = pitch // drafts
    off = (k * vocab) % LANES
    hcol = dim // 2
    wrows = vocab // STEPS

    def remote(src, dst, ssem, rsem, who):
        return pltpu.make_async_remote_copy(
            src_ref=src, dst_ref=dst, send_sem=ssem, recv_sem=rsem,
            device_id={"tp": who}, device_id_type=MESH,
        )

    hid_cp = pltpu.make_async_copy(hid_ref, hall.at[:, pl.ds(k * rows, rows), :], loc.at[0])
    hid_cp.start()
    tok_cp = pltpu.make_async_copy(tok_in, tok_ref, loc.at[6])
    tok_cp.start()

    def stage_cp(g):
        part = pl.ds(g * 8 * pitch, 8 * pitch)
        return pltpu.make_async_copy(q_ref.at[part], stage.at[part], loc.at[1 + g])

    def w_cp(t, slot):
        return pltpu.make_async_copy(
            w_ref.at[pl.ds(pl.multiple_of(t * wrows, 8), wrows)], wbuf.at[slot], wsem.at[slot]
        )

    barrier = pltpu.get_barrier_semaphore()
    for who in (2 * right + c, 2 * left + c, mate):
        pl.semaphore_signal(barrier, inc=1, device_id={"tp": who}, device_id_type=MESH)
    pl.semaphore_wait(barrier, 3)

    def hpiece(src, half):
        return hall.at[:, pl.ds(pl.multiple_of(src * rows, rows), rows), pl.ds(half * hcol, hcol)]

    def hcopy(src, half, ssem, who):
        return remote(hpiece(src, half), hpiece(src, half), ssem, h_recv.at[src * 2 + half], who)

    def hwait(src, half):
        hcopy(src, half, h_send.at[0], mate).wait_recv()

    hid_cp.wait()
    own_sends = []
    for idx, (who, half) in enumerate(
        [(2 * right + c, 0), (2 * left + c, 1), (2 * right + c, 1), (2 * left + c, 0), (mate, 0), (mate, 1)]
    ):
        cp = hcopy(k, half, h_send.at[idx], who)
        cp.start()
        own_sends.append(cp)
    for g in range(rows // 8):
        stage_cp(g).start()
    w_cp(0, 0).start()
    w_cp(1, 1).start()

    z[:, 0:96, :] = jnp.zeros((positions, 96, batch), F32)
    z[:, width - 96:width, :] = jnp.zeros((positions, 96, batch), F32)

    tok_cp.wait()
    for g in range(rows // 8):
        stage_cp(g).wait()

    def qrows(g, i, j):
        return stage[pl.ds(g * 8 * pitch + drafts * j + i, 8, stride=pitch), :]

    groups = [(i, g) for i in range(drafts) for g in range(rows // 8)]
    lane_b = lax.broadcasted_iota(jnp.int32, (8, batch), 1)
    sub_b = lax.broadcasted_iota(jnp.int32, (8, batch), 0)
    lane_t = lax.broadcasted_iota(jnp.int32, (8, LANES), 1)
    mine = [lane_b == k * rows + 8 * g + sub_b for g in range(rows // 8)]
    tok_col = []
    for i, g in groups:
        t = jnp.where(mine[g], jnp.broadcast_to(tok_ref[i:i + 1, :].astype(F32), (8, batch)), 0.0)
        tok_col.append(jnp.broadcast_to(jnp.sum(t, axis=1, keepdims=True), (8, LANES)).astype(jnp.int32))

    def scan(j, carry):
        top, got = carry
        new_top, new_got = [], []
        col = lane_t + j * LANES
        for a, (i, g) in enumerate(groups):
            v = qrows(g, i, j)
            new_top.append(jnp.maximum(top[a], v))
            new_got.append(jnp.where(col == tok_col[a], v, got[a]))
        return tuple(new_top), tuple(new_got)

    zero8 = tuple(jnp.zeros((8, LANES), F32) for _ in groups)
    top, got = lax.fori_loop(0, all_tiles, scan, (zero8, zero8))
    qtop_row, qgot_row = [], []
    for i in range(drafts):
        acc_t = jnp.zeros((8, batch), F32)
        acc_g = jnp.zeros((8, batch), F32)
        for a, (ii, g) in enumerate(groups):
            if ii != i:
                continue
            tcol = jnp.max(top[a], axis=1, keepdims=True)
            gcol = jnp.sum(got[a], axis=1, keepdims=True)
            rowc[a] = jnp.broadcast_to(jnp.log(TOP) - 0.25 * jnp.log(tcol), (8, LANES))
            acc_t = acc_t + jnp.where(mine[g], jnp.broadcast_to(tcol, (8, batch)), 0.0)
            acc_g = acc_g + jnp.where(mine[g], jnp.broadcast_to(gcol, (8, batch)), 0.0)
        qtop_row.append(jnp.sum(acc_t, axis=0, keepdims=True))
        qgot_row.append(jnp.sum(acc_g, axis=0, keepdims=True))
    msgs[k] = jnp.zeros(msgs.shape[1:], F32)
    for i in range(drafts):
        msgs[k, 8 + i:9 + i, :] = qgot_row[i]
        msgs[k, 10 + i:11 + i, :] = qtop_row[i]

    def encode(dest, put):
        first = (dest * vocab) // LANES

        def body(j, _):
            for i in range(drafts):
                for gg in range(rows // 16):
                    parts = []
                    for g in (2 * gg, 2 * gg + 1):
                        v = qrows(g, i, first + j)
                        y = jnp.exp(0.25 * jnp.log(v) + rowc[i * (rows // 8) + g])
                        parts.append((y + 0.5).astype(jnp.int32) - HALF)
                    code = jnp.concatenate(parts, axis=0).astype(jnp.int16)
                    put(i, gg, j // per, pl.ds(pl.multiple_of((j % per) * LANES, LANES), LANES), code)
            return 0

        lax.fori_loop(0, tiles, body, 0)

    def to_slot(r):
        def put(i, gg, s, cols, code):
            scode[r, i, s, 16 * gg:16 * gg + 16, cols] = code

        return put

    def to_self(i, gg, s, cols, code):
        qall[i, s, pl.ds(pl.multiple_of(k * rows + 16 * gg, 16), 16), cols] = code

    encode(2 * far, to_slot(0))
    encode(2 * far + 1, to_slot(1))

    fwd = []

    def forward(src, half):
        cp = hcopy(src, half, h_fwd.at[len(fwd)], mate)
        cp.start()
        fwd.append(cp)

    hwait(2 * left + c, 0)
    rel_r = hcopy(2 * left + c, 0, h_send.at[6], 2 * right + c)
    rel_r.start()
    forward(2 * left + c, 0)
    hwait(2 * right + c, 1)
    rel_l = hcopy(2 * right + c, 1, h_send.at[7], 2 * left + c)
    rel_l.start()
    forward(2 * right + c, 1)

    def unit(buf_i, i, s):
        return buf_i.at[i, s]

    def landing(src, i, s):
        return qall.at[i, s, pl.ds(pl.multiple_of(src * rows, rows), rows)]

    def direct(slot, i, s, who):
        return remote(
            unit(scode.at[slot], i, s), landing(k, i, s),
            q_send.at[slot * units + i * SEGS + s], q_recv.at[k * units + i * SEGS + s], who,
        )

    def core_of(way):
        return c if way == 0 else 1 - c

    def out_far(way, v):
        i, s, cc = v // SEGS, v % SEGS, core_of(way)
        who = 2 * (right if way == 0 else left) + c
        return remote(
            unit(scode.at[cc], i, s), rbuf.at[way, v],
            q_send.at[cc * units + i * SEGS + s], r_recv.at[way * units + v], who,
        )

    def relay(way, v):
        i, s, cc = v // SEGS, v % SEGS, core_of(way)
        src = 2 * (left if way == 0 else right) + c
        who = 2 * (right if way == 0 else left) + cc
        return remote(
            rbuf.at[way, v], landing(src, i, s),
            r_send.at[way * units + v], q_recv.at[src * units + i * SEGS + s], who,
        )

    def near(way, u):
        i, s, cc = u // (2 * SEGS), (u // 2) % SEGS, u % 2
        who = 2 * (right if way == 0 else left) + cc
        return direct(2 + 2 * way + cc, i, s, who)

    def send_far(v):
        out_far(0, v).start()
        out_far(1, v).start()

    def send_near(u):
        near(0, u).start()
        near(1, u).start()

    def pass_on(v):
        for way in range(2):
            out_far(way, v).wait_recv()
            relay(way, v).start()

    encode(2 * right, to_slot(2))
    encode(2 * right + 1, to_slot(3))
    encode(2 * left, to_slot(4))
    encode(2 * left + 1, to_slot(5))

    hwait(2 * left + c, 1)
    forward(2 * left + c, 1)
    hwait(2 * right + c, 0)
    forward(2 * right + c, 0)

    def first_far(v, _):
        send_far(v)
        return 0

    def first_near(u, _):
        send_near(u)
        return 0

    lax.fori_loop(0, SEGS, first_far, 0)
    lax.fori_loop(0, 2 * SEGS, first_near, 0)
    encode(mate, to_slot(6))
    encode(k, to_self)

    def to_mate(u, _):
        direct(6, u // SEGS, u % SEGS, mate).start()
        return 0

    lax.fori_loop(0, drafts * SEGS, to_mate, 0)

    hwait(2 * far + c, 0)
    forward(2 * far + c, 0)
    hwait(2 * far + c, 1)
    forward(2 * far + c, 1)
    for chip in (x, left, right, far):
        for half in range(2):
            hwait(2 * chip + 1 - c, half)

    def step(t, top):
        slot = t % 2

        @pl.when((t >= 2) & (t < 4))
        def _():
            for e in range(SEGS // 2):
                pass_on((SEGS // 2) * (t - 2) + e)

        @pl.when((t >= 4) & (t < 6))
        def _():
            for e in range(SEGS // 2):
                send_far(SEGS + (SEGS // 2) * (t - 4) + e)

        @pl.when(t >= 6)
        def _():
            for e in range(SEGS // 2):
                send_near(2 * SEGS + (SEGS // 2) * (t - 6) + e)

        w_cp(t, slot).wait()
        prod = INV_TEMP * lax.dot_general(
            wbuf[slot], hall[...].reshape(positions * batch, dim), (((1,), (1,)), ((), ())), preferred_element_type=F32
        )
        base = pl.multiple_of(off + t * wrows, 8)
        for i in range(positions):
            z[i, pl.ds(base, wrows), :] = prod[:, i * batch:(i + 1) * batch]

        @pl.when(t + 2 < STEPS)
        def _():
            w_cp(t + 2, slot).start()

        return jnp.maximum(top, jnp.max(prod.reshape(wrows // 8, 8, positions * batch), axis=0))

    top = lax.fori_loop(0, STEPS, step, jnp.full((8, positions * batch), -jnp.inf, F32))
    own_max = jnp.max(top, axis=0, keepdims=True)

    chunk = 160
    row_i = lax.broadcasted_iota(jnp.int32, (chunk, batch), 0)
    for i in range(positions):
        m_i = own_max[:, i * batch:(i + 1) * batch]
        want = tok_ref[i:i + 1, :] - k * vocab if i < drafts else None

        def expo(t, carry, i=i, m_i=m_i, want=want):
            total, got = carry
            at = pl.ds(pl.multiple_of(off + t * chunk, 8), chunk)
            e = jnp.exp(z[i, at, :] - m_i)
            z[i, at, :] = e
            total = total + jnp.sum(e.reshape(chunk // 8, 8, batch), axis=0)
            if want is not None:
                pick = jnp.where(row_i + t * chunk == want, e, 0.0)
                got = got + jnp.sum(pick.reshape(chunk // 8, 8, batch), axis=0)
            return total, got

        zero = jnp.zeros((8, batch), F32)
        total, got = lax.fori_loop(0, vocab // chunk, expo, (zero, zero))
        msgs[k, i:i + 1, :] = m_i
        msgs[k, 3 + i:4 + i, :] = jnp.sum(total, axis=0, keepdims=True)
        if i < drafts:
            msgs[k, 6 + i:7 + i, :] = jnp.sum(got, axis=0, keepdims=True)

    def msg(p, src):
        return remote(msgs.at[src], msgs.at[src], m_send.at[p], m_recv.at[src], (k + p) % n)

    for p in range(1, n):
        msg(p, k).start()

    for v in range(SEGS, 2 * SEGS):
        pass_on(v)
    for p in range(1, n):
        msg(p, (k + p) % n).wait_recv()

    allm = msgs[...]
    peak = jnp.max(allm[:, 0:3, :], axis=0)
    part = jnp.exp(allm[:, 0:3, :] - peak[None])
    inv = 1.0 / jnp.sum(part * allm[:, 3:6, :], axis=0)
    p_pick = jnp.sum(part[:, 0:drafts, :] * allm[:, 6:8, :], axis=0) * inv[0:drafts]
    q_pick = jnp.sum(allm[:, 8:10, :], axis=0)
    q_scale = jnp.sum(allm[:, 10:12, :], axis=0) * (1.0 / (TOP * TOP * TOP * TOP))
    fac = jnp.exp(msgs[k, 0:3, :] - peak) * inv

    def scale(t, _):
        at = pl.ds(pl.multiple_of(off + t * chunk, 8), chunk)
        z[drafts, at, :] = z[drafts, at, :] * fac[drafts:drafts + 1, :]
        return 0

    lax.fori_loop(0, vocab // chunk, scale, 0)

    def xmsg(p, i, src):
        return remote(mass.at[i, src], mass.at[i, src], x_send.at[i * n + p], x_recv.at[i * n + src], (k + p) % n)

    def drain(u, _):
        direct(u // units, (u % units) // SEGS, u % SEGS, mate).wait_send()
        return 0

    def drain_relay(v, _):
        relay(0, v).wait_send()
        relay(1, v).wait_send()
        return 0

    for i in range(drafts):
        acc = [jnp.zeros((8, LANES), F32) for _ in range(batch // LANES)]
        for s in range(SEGS):
            if i == drafts - 1 and s == SEGS - 1:
                for cp in own_sends + [rel_r, rel_l] + fwd:
                    cp.wait_send()
                for p in range(1, n):
                    msg(p, k).wait_send()
                lax.fori_loop(0, (n - 1) * units, drain, 0)
            for p in range(1, n):
                src = (k + p) % n
                remote(
                    landing(src, i, s), landing(src, i, s), q_send.at[0],
                    q_recv.at[src * units + i * SEGS + s], mate,
                ).wait_recv()

            def body(t, acc, i=i, s=s):
                at = pl.ds(pl.multiple_of((s * (tiles // SEGS) + t) * LANES, LANES), LANES)
                out = []
                for h in range(batch // LANES):
                    ls = slice(h * LANES, (h + 1) * LANES)
                    code = qall[i, s, ls, pl.ds(pl.multiple_of(t * LANES, LANES), LANES)].astype(jnp.int32).astype(F32)
                    y = code.T + float(HALF)
                    y = y * y
                    qt = y * y * q_scale[i:i + 1, ls]
                    ex = jnp.maximum(z[i, at, ls] * fac[i:i + 1, ls] - qt, 0.0)
                    z[i, at, ls] = ex
                    out.append(acc[h] + jnp.sum(ex.reshape(LANES // 8, 8, LANES), axis=0))
                return tuple(out)

            acc = lax.fori_loop(0, tiles // SEGS, body, tuple(acc))
        for h in range(batch // LANES):
            mass[i, k, :, h * LANES:(h + 1) * LANES] = jnp.sum(acc[h], axis=0, keepdims=True)
        for p in range(1, n):
            xmsg(p, i, k).start()
    lax.fori_loop(0, units, drain_relay, 0)
    small_ref[...] = jnp.zeros(small_ref.shape, F32)
    small_ref[2:4, :] = p_pick
    small_ref[4:6, :] = q_pick
    for i in range(drafts):
        for p in range(1, n):
            xmsg(p, i, (k + p) % n).wait_recv()
        total = jnp.sum(mass[i], axis=0)
        small_ref[i:i + 1, :] = 1.0 / total

    for p in range(1, n):
        for i in range(drafts):
            xmsg(p, i, k).wait_send()


def finish(n, z, small, res_ref, bonus_ref, acc_ref, exp_ref, buf, sem):
    drafts, vocab, _ = res_ref.shape
    off = pl.multiple_of((lax.axis_index("tp") * vocab) % LANES, 8)
    last = pltpu.make_async_copy(z.at[drafts, pl.ds(off, vocab), :], bonus_ref, sem.at[0])
    last.start()
    copies = [last]
    part = vocab // PARTS
    for i in range(drafts):
        scale = small[i:i + 1, :]
        for t in range(PARTS):
            to = pl.ds(t * part, part)
            buf[i, to, :] = z[i, pl.ds(pl.multiple_of(off + t * part, 8), part), :] * scale
            cp = pltpu.make_async_copy(buf.at[i, to], res_ref.at[i, to], sem.at[len(copies)])
            cp.start()
            copies.append(cp)
    accept = jnp.minimum(small[2:4, :] / small[4:6, :], 1.0)
    acc_ref[...] = accept
    exp_ref[...] = accept[0:1] + accept[0:1] * accept[1:2]
    for cp in copies:
        cp.wait()


def solution(mesh):
    n = mesh.shape["tp"]

    def local(hid, w, q, tok):
        rows, positions, dim = hid.shape
        vocab = w.shape[1]
        drafts = positions - 1
        batch = rows * n
        q_tiles = q.shape[2] // LANES
        width = -(-vocab // LANES) * LANES
        q_view = q.reshape(rows, drafts, q_tiles, LANES).transpose(0, 2, 1, 3)
        q_view = with_layout_constraint(q_view, Layout((0, 1, 2, 3))).reshape(-1, LANES)
        dma = pltpu.SemaphoreType.DMA
        vmem, anywhere = pl.BlockSpec(memory_space=pltpu.VMEM), pl.BlockSpec(memory_space=pltpu.HBM)
        z, small = pl.pallas_call(
            functools.partial(kernel, n),
            out_shape=(
                jax.ShapeDtypeStruct((positions, width, batch), F32),
                jax.ShapeDtypeStruct((8, batch), F32),
            ),
            in_specs=[anywhere] * 4,
            out_specs=(vmem, vmem),
            scratch_shapes=[
                pltpu.VMEM((drafts, batch), jnp.int32),
                pltpu.VMEM((positions, batch, dim), jnp.bfloat16),
                pltpu.VMEM((rows * q_tiles * drafts, LANES), F32),
                pltpu.VMEM((n - 1, drafts, SEGS, rows, width // SEGS), jnp.int16),
                pltpu.VMEM((drafts, SEGS, batch, width // SEGS), jnp.int16),
                pltpu.VMEM((2, drafts * SEGS, rows, width // SEGS), jnp.int16),
                pltpu.VMEM((2, vocab // STEPS, dim), jnp.bfloat16),
                pltpu.VMEM((n, 16, batch), F32),
                pltpu.VMEM((drafts, n, 1, batch), F32),
                pltpu.VMEM((drafts * (rows // 8), 8, LANES), F32),
                dma((8,)), dma((8,)), dma((2 * n,)),
                dma((n * drafts * SEGS,)), dma((n * drafts * SEGS,)), dma((2 * drafts * SEGS,)), dma((2 * drafts * SEGS,)),
                dma((n,)), dma((n,)), dma((2 * n,)), dma((2 * n,)),
                dma((8,)), dma((2,)),
            ],
            compiler_params=pltpu.CompilerParams(
                collective_id=0, has_side_effects=True, vmem_limit_bytes=40 * 2**20
            ),
        )(*[pltpu.with_memory_space_constraint(a, pltpu.HBM) for a in (tok.T, hid.transpose(1, 0, 2), w.T, q_view)])
        residual, bonus, accept, expected = pl.pallas_call(
            functools.partial(finish, n),
            out_shape=(
                jax.ShapeDtypeStruct((drafts, vocab, batch), F32),
                jax.ShapeDtypeStruct((vocab, batch), F32),
                jax.ShapeDtypeStruct((drafts, batch), F32),
                jax.ShapeDtypeStruct((1, batch), F32),
            ),
            in_specs=[vmem, vmem],
            out_specs=(anywhere, anywhere, vmem, vmem),
            scratch_shapes=[pltpu.VMEM((drafts, vocab, batch), F32), dma((drafts * PARTS + 1,))],
            compiler_params=pltpu.CompilerParams(vmem_limit_bytes=24 * 2**20),
        )(z, small)
        return accept.T, expected[0], residual.transpose(2, 0, 1), bonus.T

    return jax.shard_map(
        local,
        mesh=mesh,
        in_specs=(P(("dp", "tp"), None, None), P(None, "tp"), P(("dp", "tp"), None, None), P("dp", None)),
        out_specs=(P("dp", None), P("dp"), P("dp", None, "tp"), P("dp", "tp")),
        check_vma=False,
    )
```

```python
import functools

import jax
import jax.numpy as jnp
from jax import lax
from jax.experimental import pallas as pl
from jax.experimental.pallas import tpu as pltpu
from jax.experimental.layout import Layout, with_layout_constraint
from jax.sharding import PartitionSpec as P

INV_TEMP = 1.25
TOP = 65535.0
HALF = 32768
LANES = 128
SEGS = 2
STEPS = 10
PARTS = 5
F32 = jnp.float32
MESH = pl.DeviceIdType.MESH


def kernel(
    n, tok_in, hid_ref, w_ref, q_ref,
    z, small_ref,
    tok_ref, hall, stage, scode, qall, rbuf, wbuf, msgs, mass, rowc,
    h_send, h_fwd, h_recv, q_send, q_recv, r_send, r_recv,
    m_send, m_recv, x_send, x_recv, loc, wsem,
):
    k = lax.axis_index("tp")
    x, c = k // 2, k % 2
    chips = n // 2
    right, left = (x + 1) % chips, (x + chips - 1) % chips
    far = (x + 2) % chips
    mate = 2 * x + 1 - c
    positions, batch, dim = hall.shape
    drafts = positions - 1
    rows = batch // n
    vocab = w_ref.shape[0]
    seg = qall.shape[3]
    width = seg * SEGS
    tiles = width // LANES
    units = drafts * SEGS
    per = seg // LANES
    pitch = q_ref.shape[0] // rows
    all_tiles = pitch // drafts
    off = (k * vocab) % LANES
    hcol = dim // 2
    wrows = vocab // STEPS

    def remote(src, dst, ssem, rsem, who):
        return pltpu.make_async_remote_copy(
            src_ref=src, dst_ref=dst, send_sem=ssem, recv_sem=rsem,
            device_id={"tp": who}, device_id_type=MESH,
        )

    hid_cp = pltpu.make_async_copy(hid_ref, hall.at[:, pl.ds(k * rows, rows), :], loc.at[0])
    hid_cp.start()
    tok_cp = pltpu.make_async_copy(tok_in, tok_ref, loc.at[6])
    tok_cp.start()

    def stage_cp(g):
        part = pl.ds(g * 8 * pitch, 8 * pitch)
        return pltpu.make_async_copy(q_ref.at[part], stage.at[part], loc.at[1 + g])

    def w_cp(t, slot):
        return pltpu.make_async_copy(
            w_ref.at[pl.ds(pl.multiple_of(t * wrows, 8), wrows)], wbuf.at[slot], wsem.at[slot]
        )

    barrier = pltpu.get_barrier_semaphore()
    for who in (2 * right + c, 2 * left + c, mate):
        pl.semaphore_signal(barrier, inc=1, device_id={"tp": who}, device_id_type=MESH)
    pl.semaphore_wait(barrier, 3)

    def hpiece(src, half):
        return hall.at[:, pl.ds(pl.multiple_of(src * rows, rows), rows), pl.ds(half * hcol, hcol)]

    def hcopy(src, half, ssem, who):
        return remote(hpiece(src, half), hpiece(src, half), ssem, h_recv.at[src * 2 + half], who)

    def hwait(src, half):
        hcopy(src, half, h_send.at[0], mate).wait_recv()

    hid_cp.wait()
    own_sends = []
    for idx, (who, half) in enumerate(
        [(2 * right + c, 0), (2 * left + c, 1), (2 * right + c, 1), (2 * left + c, 0), (mate, 0), (mate, 1)]
    ):
        cp = hcopy(k, half, h_send.at[idx], who)
        cp.start()
        own_sends.append(cp)
    for g in range(rows // 8):
        stage_cp(g).start()
    w_cp(0, 0).start()
    w_cp(1, 1).start()

    z[:, 0:96, :] = jnp.zeros((positions, 96, batch), F32)
    z[:, width - 96:width, :] = jnp.zeros((positions, 96, batch), F32)

    tok_cp.wait()
    for g in range(rows // 8):
        stage_cp(g).wait()

    def qrows(g, i, j):
        return stage[pl.ds(g * 8 * pitch + drafts * j + i, 8, stride=pitch), :]

    groups = [(i, g) for i in range(drafts) for g in range(rows // 8)]
    lane_b = lax.broadcasted_iota(jnp.int32, (8, batch), 1)
    sub_b = lax.broadcasted_iota(jnp.int32, (8, batch), 0)
    lane_t = lax.broadcasted_iota(jnp.int32, (8, LANES), 1)
    mine = [lane_b == k * rows + 8 * g + sub_b for g in range(rows // 8)]
    tok_col = []
    for i, g in groups:
        t = jnp.where(mine[g], jnp.broadcast_to(tok_ref[i:i + 1, :].astype(F32), (8, batch)), 0.0)
        tok_col.append(jnp.broadcast_to(jnp.sum(t, axis=1, keepdims=True), (8, LANES)).astype(jnp.int32))

    def scan(j, carry):
        top, got = carry
        new_top, new_got = [], []
        col = lane_t + j * LANES
        for a, (i, g) in enumerate(groups):
            v = qrows(g, i, j)
            new_top.append(jnp.maximum(top[a], v))
            new_got.append(jnp.where(col == tok_col[a], v, got[a]))
        return tuple(new_top), tuple(new_got)

    zero8 = tuple(jnp.zeros((8, LANES), F32) for _ in groups)
    top, got = lax.fori_loop(0, all_tiles, scan, (zero8, zero8))
    qtop_row, qgot_row = [], []
    for i in range(drafts):
        acc_t = jnp.zeros((8, batch), F32)
        acc_g = jnp.zeros((8, batch), F32)
        for a, (ii, g) in enumerate(groups):
            if ii != i:
                continue
            tcol = jnp.max(top[a], axis=1, keepdims=True)
            gcol = jnp.sum(got[a], axis=1, keepdims=True)
            rowc[a] = jnp.broadcast_to(jnp.log(TOP) - 0.25 * jnp.log(tcol), (8, LANES))
            acc_t = acc_t + jnp.where(mine[g], jnp.broadcast_to(tcol, (8, batch)), 0.0)
            acc_g = acc_g + jnp.where(mine[g], jnp.broadcast_to(gcol, (8, batch)), 0.0)
        qtop_row.append(jnp.sum(acc_t, axis=0, keepdims=True))
        qgot_row.append(jnp.sum(acc_g, axis=0, keepdims=True))
    msgs[k] = jnp.zeros(msgs.shape[1:], F32)
    for i in range(drafts):
        msgs[k, 8 + i:9 + i, :] = qgot_row[i]
        msgs[k, 10 + i:11 + i, :] = qtop_row[i]

    def encode(dest, put):
        first = (dest * vocab) // LANES

        def body(j, _):
            for i in range(drafts):
                for gg in range(rows // 16):
                    parts = []
                    for g in (2 * gg, 2 * gg + 1):
                        v = qrows(g, i, first + j)
                        y = jnp.exp(0.25 * jnp.log(v) + rowc[i * (rows // 8) + g])
                        parts.append((y + 0.5).astype(jnp.int32) - HALF)
                    code = jnp.concatenate(parts, axis=0).astype(jnp.int16)
                    put(i, gg, j // per, pl.ds(pl.multiple_of((j % per) * LANES, LANES), LANES), code)
            return 0

        lax.fori_loop(0, tiles, body, 0)

    def to_slot(r):
        def put(i, gg, s, cols, code):
            scode[r, i, s, 16 * gg:16 * gg + 16, cols] = code

        return put

    def to_self(i, gg, s, cols, code):
        qall[i, s, pl.ds(pl.multiple_of(k * rows + 16 * gg, 16), 16), cols] = code

    encode(2 * far, to_slot(0))
    encode(2 * far + 1, to_slot(1))

    fwd = []

    def forward(src, half):
        cp = hcopy(src, half, h_fwd.at[len(fwd)], mate)
        cp.start()
        fwd.append(cp)

    hwait(2 * left + c, 0)
    rel_r = hcopy(2 * left + c, 0, h_send.at[6], 2 * right + c)
    rel_r.start()
    forward(2 * left + c, 0)
    hwait(2 * right + c, 1)
    rel_l = hcopy(2 * right + c, 1, h_send.at[7], 2 * left + c)
    rel_l.start()
    forward(2 * right + c, 1)

    def unit(buf_i, i, s):
        return buf_i.at[i, s]

    def landing(src, i, s):
        return qall.at[i, s, pl.ds(pl.multiple_of(src * rows, rows), rows)]

    def direct(slot, i, s, who):
        return remote(
            unit(scode.at[slot], i, s), landing(k, i, s),
            q_send.at[slot * units + i * SEGS + s], q_recv.at[k * units + i * SEGS + s], who,
        )

    def core_of(way):
        return c if way == 0 else 1 - c

    def out_far(way, v):
        i, s, cc = v // SEGS, v % SEGS, core_of(way)
        who = 2 * (right if way == 0 else left) + c
        return remote(
            unit(scode.at[cc], i, s), rbuf.at[way, v],
            q_send.at[cc * units + i * SEGS + s], r_recv.at[way * units + v], who,
        )

    def relay(way, v):
        i, s, cc = v // SEGS, v % SEGS, core_of(way)
        src = 2 * (left if way == 0 else right) + c
        who = 2 * (right if way == 0 else left) + cc
        return remote(
            rbuf.at[way, v], landing(src, i, s),
            r_send.at[way * units + v], q_recv.at[src * units + i * SEGS + s], who,
        )

    def near(way, u):
        i, s, cc = u // (2 * SEGS), (u // 2) % SEGS, u % 2
        who = 2 * (right if way == 0 else left) + cc
        return direct(2 + 2 * way + cc, i, s, who)

    def send_far(v):
        out_far(0, v).start()
        out_far(1, v).start()

    def send_near(u):
        near(0, u).start()
        near(1, u).start()

    def pass_on(v):
        for way in range(2):
            out_far(way, v).wait_recv()
            relay(way, v).start()

    encode(2 * right, to_slot(2))
    encode(2 * right + 1, to_slot(3))
    encode(2 * left, to_slot(4))
    encode(2 * left + 1, to_slot(5))

    hwait(2 * left + c, 1)
    forward(2 * left + c, 1)
    hwait(2 * right + c, 0)
    forward(2 * right + c, 0)

    def first_far(v, _):
        send_far(v)
        return 0

    def first_near(u, _):
        send_near(u)
        return 0

    lax.fori_loop(0, SEGS, first_far, 0)
    lax.fori_loop(0, 2 * SEGS, first_near, 0)
    encode(mate, to_slot(6))
    encode(k, to_self)

    def to_mate(u, _):
        direct(6, u // SEGS, u % SEGS, mate).start()
        return 0

    lax.fori_loop(0, drafts * SEGS, to_mate, 0)

    hwait(2 * far + c, 0)
    forward(2 * far + c, 0)
    hwait(2 * far + c, 1)
    forward(2 * far + c, 1)
    for chip in (x, left, right, far):
        for half in range(2):
            hwait(2 * chip + 1 - c, half)

    def step(t, top):
        slot = t % 2

        @pl.when((t >= 2) & (t < 4))
        def _():
            for e in range(SEGS // 2):
                pass_on((SEGS // 2) * (t - 2) + e)

        @pl.when((t >= 4) & (t < 6))
        def _():
            for e in range(SEGS // 2):
                send_far(SEGS + (SEGS // 2) * (t - 4) + e)

        @pl.when((t == 6) | (t == 8))
        def _():
            for e in range(SEGS // 2):
                send_near(2 * SEGS + (SEGS // 2) * ((t - 6) // 2) + e)

        w_cp(t, slot).wait()
        prod = INV_TEMP * lax.dot_general(
            wbuf[slot], hall[...].reshape(positions * batch, dim), (((1,), (1,)), ((), ())), preferred_element_type=F32
        )
        base = pl.multiple_of(off + t * wrows, 8)
        for i in range(positions):
            z[i, pl.ds(base, wrows), :] = prod[:, i * batch:(i + 1) * batch]

        @pl.when(t + 2 < STEPS)
        def _():
            w_cp(t + 2, slot).start()

        return jnp.maximum(top, jnp.max(prod.reshape(wrows // 8, 8, positions * batch), axis=0))

    top = lax.fori_loop(0, STEPS, step, jnp.full((8, positions * batch), -jnp.inf, F32))
    own_max = jnp.max(top, axis=0, keepdims=True)

    chunk = 160
    row_i = lax.broadcasted_iota(jnp.int32, (chunk, batch), 0)
    for i in range(positions):
        m_i = own_max[:, i * batch:(i + 1) * batch]
        want = tok_ref[i:i + 1, :] - k * vocab if i < drafts else None

        def expo(t, carry, i=i, m_i=m_i, want=want):
            total, got = carry
            at = pl.ds(pl.multiple_of(off + t * chunk, 8), chunk)
            e = jnp.exp(z[i, at, :] - m_i)
            z[i, at, :] = e
            total = total + jnp.sum(e.reshape(chunk // 8, 8, batch), axis=0)
            if want is not None:
                pick = jnp.where(row_i + t * chunk == want, e, 0.0)
                got = got + jnp.sum(pick.reshape(chunk // 8, 8, batch), axis=0)
            return total, got

        zero = jnp.zeros((8, batch), F32)
        total, got = lax.fori_loop(0, vocab // chunk, expo, (zero, zero))
        msgs[k, i:i + 1, :] = m_i
        msgs[k, 3 + i:4 + i, :] = jnp.sum(total, axis=0, keepdims=True)
        if i < drafts:
            msgs[k, 6 + i:7 + i, :] = jnp.sum(got, axis=0, keepdims=True)

    def msg(p, src):
        return remote(msgs.at[src], msgs.at[src], m_send.at[p], m_recv.at[src], (k + p) % n)

    for p in range(1, n):
        msg(p, k).start()

    for u in range(3 * SEGS, 4 * SEGS):
        send_near(u)
    for v in range(SEGS, 2 * SEGS):
        pass_on(v)
    for p in range(1, n):
        msg(p, (k + p) % n).wait_recv()

    allm = msgs[...]
    peak = jnp.max(allm[:, 0:3, :], axis=0)
    part = jnp.exp(allm[:, 0:3, :] - peak[None])
    inv = 1.0 / jnp.sum(part * allm[:, 3:6, :], axis=0)
    p_pick = jnp.sum(part[:, 0:drafts, :] * allm[:, 6:8, :], axis=0) * inv[0:drafts]
    q_pick = jnp.sum(allm[:, 8:10, :], axis=0)
    q_scale = jnp.sum(allm[:, 10:12, :], axis=0) * (1.0 / (TOP * TOP * TOP * TOP))
    fac = jnp.exp(msgs[k, 0:3, :] - peak) * inv

    def scale(t, _):
        at = pl.ds(pl.multiple_of(off + t * chunk, 8), chunk)
        z[drafts, at, :] = z[drafts, at, :] * fac[drafts:drafts + 1, :]
        return 0

    lax.fori_loop(0, vocab // chunk, scale, 0)

    def xmsg(p, i, src):
        return remote(mass.at[i, src], mass.at[i, src], x_send.at[i * n + p], x_recv.at[i * n + src], (k + p) % n)

    def drain(u, _):
        direct(u // units, (u % units) // SEGS, u % SEGS, mate).wait_send()
        return 0

    def drain_relay(v, _):
        relay(0, v).wait_send()
        relay(1, v).wait_send()
        return 0

    for i in range(drafts):
        acc = [jnp.zeros((8, LANES), F32) for _ in range(batch // LANES)]
        for s in range(SEGS):
            if i == drafts - 1 and s == SEGS - 1:
                for cp in own_sends + [rel_r, rel_l] + fwd:
                    cp.wait_send()
                for p in range(1, n):
                    msg(p, k).wait_send()
                lax.fori_loop(0, (n - 1) * units, drain, 0)
            for p in range(1, n):
                src = (k + p) % n
                remote(
                    landing(src, i, s), landing(src, i, s), q_send.at[0],
                    q_recv.at[src * units + i * SEGS + s], mate,
                ).wait_recv()

            def body(t, acc, i=i, s=s):
                at = pl.ds(pl.multiple_of((s * (tiles // SEGS) + t) * LANES, LANES), LANES)
                out = []
                for h in range(batch // LANES):
                    ls = slice(h * LANES, (h + 1) * LANES)
                    code = qall[i, s, ls, pl.ds(pl.multiple_of(t * LANES, LANES), LANES)].astype(jnp.int32).astype(F32)
                    y = code.T + float(HALF)
                    y = y * y
                    qt = y * y * q_scale[i:i + 1, ls]
                    ex = jnp.maximum(z[i, at, ls] * fac[i:i + 1, ls] - qt, 0.0)
                    z[i, at, ls] = ex
                    out.append(acc[h] + jnp.sum(ex.reshape(LANES // 8, 8, LANES), axis=0))
                return tuple(out)

            acc = lax.fori_loop(0, tiles // SEGS, body, tuple(acc))
        for h in range(batch // LANES):
            mass[i, k, :, h * LANES:(h + 1) * LANES] = jnp.sum(acc[h], axis=0, keepdims=True)
        for p in range(1, n):
            xmsg(p, i, k).start()
    lax.fori_loop(0, units, drain_relay, 0)
    small_ref[...] = jnp.zeros(small_ref.shape, F32)
    small_ref[2:4, :] = p_pick
    small_ref[4:6, :] = q_pick
    for i in range(drafts):
        for p in range(1, n):
            xmsg(p, i, (k + p) % n).wait_recv()
        total = jnp.sum(mass[i], axis=0)
        small_ref[i:i + 1, :] = 1.0 / total

    for p in range(1, n):
        for i in range(drafts):
            xmsg(p, i, k).wait_send()


def finish(n, z, small, res_ref, bonus_ref, acc_ref, exp_ref, buf, sem):
    drafts, vocab, _ = res_ref.shape
    off = pl.multiple_of((lax.axis_index("tp") * vocab) % LANES, 8)
    last = pltpu.make_async_copy(z.at[drafts, pl.ds(off, vocab), :], bonus_ref, sem.at[0])
    last.start()
    copies = [last]
    part = vocab // PARTS
    for i in range(drafts):
        scale = small[i:i + 1, :]
        for t in range(PARTS):
            to = pl.ds(t * part, part)
            buf[i, to, :] = z[i, pl.ds(pl.multiple_of(off + t * part, 8), part), :] * scale
            cp = pltpu.make_async_copy(buf.at[i, to], res_ref.at[i, to], sem.at[len(copies)])
            cp.start()
            copies.append(cp)
    accept = jnp.minimum(small[2:4, :] / small[4:6, :], 1.0)
    acc_ref[...] = accept
    exp_ref[...] = accept[0:1] + accept[0:1] * accept[1:2]
    for cp in copies:
        cp.wait()


def solution(mesh):
    n = mesh.shape["tp"]

    def local(hid, w, q, tok):
        rows, positions, dim = hid.shape
        vocab = w.shape[1]
        drafts = positions - 1
        batch = rows * n
        q_tiles = q.shape[2] // LANES
        width = -(-vocab // LANES) * LANES
        q_view = q.reshape(rows, drafts, q_tiles, LANES).transpose(0, 2, 1, 3)
        q_view = with_layout_constraint(q_view, Layout((0, 1, 2, 3))).reshape(-1, LANES)
        dma = pltpu.SemaphoreType.DMA
        vmem, anywhere = pl.BlockSpec(memory_space=pltpu.VMEM), pl.BlockSpec(memory_space=pltpu.HBM)
        z, small = pl.pallas_call(
            functools.partial(kernel, n),
            out_shape=(
                jax.ShapeDtypeStruct((positions, width, batch), F32),
                jax.ShapeDtypeStruct((8, batch), F32),
            ),
            in_specs=[anywhere] * 4,
            out_specs=(vmem, vmem),
            scratch_shapes=[
                pltpu.VMEM((drafts, batch), jnp.int32),
                pltpu.VMEM((positions, batch, dim), jnp.bfloat16),
                pltpu.VMEM((rows * q_tiles * drafts, LANES), F32),
                pltpu.VMEM((n - 1, drafts, SEGS, rows, width // SEGS), jnp.int16),
                pltpu.VMEM((drafts, SEGS, batch, width // SEGS), jnp.int16),
                pltpu.VMEM((2, drafts * SEGS, rows, width // SEGS), jnp.int16),
                pltpu.VMEM((2, vocab // STEPS, dim), jnp.bfloat16),
                pltpu.VMEM((n, 16, batch), F32),
                pltpu.VMEM((drafts, n, 1, batch), F32),
                pltpu.VMEM((drafts * (rows // 8), 8, LANES), F32),
                dma((8,)), dma((8,)), dma((2 * n,)),
                dma((n * drafts * SEGS,)), dma((n * drafts * SEGS,)), dma((2 * drafts * SEGS,)), dma((2 * drafts * SEGS,)),
                dma((n,)), dma((n,)), dma((2 * n,)), dma((2 * n,)),
                dma((8,)), dma((2,)),
            ],
            compiler_params=pltpu.CompilerParams(
                collective_id=0, has_side_effects=True, vmem_limit_bytes=40 * 2**20
            ),
        )(*[pltpu.with_memory_space_constraint(a, pltpu.HBM) for a in (tok.T, hid.transpose(1, 0, 2), w.T, q_view)])
        residual, bonus, accept, expected = pl.pallas_call(
            functools.partial(finish, n),
            out_shape=(
                jax.ShapeDtypeStruct((drafts, vocab, batch), F32),
                jax.ShapeDtypeStruct((vocab, batch), F32),
                jax.ShapeDtypeStruct((drafts, batch), F32),
                jax.ShapeDtypeStruct((1, batch), F32),
            ),
            in_specs=[vmem, vmem],
            out_specs=(anywhere, anywhere, vmem, vmem),
            scratch_shapes=[pltpu.VMEM((drafts, vocab, batch), F32), dma((drafts * PARTS + 1,))],
            compiler_params=pltpu.CompilerParams(vmem_limit_bytes=24 * 2**20),
        )(z, small)
        return accept.T, expected[0], residual.transpose(2, 0, 1), bonus.T

    return jax.shard_map(
        local,
        mesh=mesh,
        in_specs=(P(("dp", "tp"), None, None), P(None, "tp"), P(("dp", "tp"), None, None), P("dp", None)),
        out_specs=(P("dp", None), P("dp"), P("dp", None, "tp"), P("dp", "tp")),
        check_vma=False,
    )
```

```python
import functools

import jax
import jax.numpy as jnp
from jax import lax
from jax.experimental import pallas as pl
from jax.experimental.pallas import tpu as pltpu
from jax.experimental.layout import Layout, with_layout_constraint
from jax.sharding import PartitionSpec as P

INV_TEMP = 1.25
TOP = 65535.0
HALF = 32768
LANES = 128
SEGS = 2
STEPS = 10
PARTS = 5
F32 = jnp.float32
MESH = pl.DeviceIdType.MESH


def kernel(
    n, tok_in, hid_ref, w_ref, q_ref,
    z, small_ref,
    tok_ref, hall, stage, scode, qall, rbuf, wbuf, msgs, mass, rowc,
    h_send, h_fwd, h_recv, q_send, q_recv, r_send, r_recv,
    m_send, m_recv, x_send, x_recv, loc, wsem,
):
    k = lax.axis_index("tp")
    x, c = k // 2, k % 2
    chips = n // 2
    right, left = (x + 1) % chips, (x + chips - 1) % chips
    far = (x + 2) % chips
    mate = 2 * x + 1 - c
    positions, batch, dim = hall.shape
    drafts = positions - 1
    rows = batch // n
    vocab = w_ref.shape[0]
    seg = qall.shape[3]
    width = seg * SEGS
    tiles = width // LANES
    units = drafts * SEGS
    per = seg // LANES
    pitch = q_ref.shape[0] // rows
    all_tiles = pitch // drafts
    off = (k * vocab) % LANES
    hcol = dim // 2
    wrows = vocab // STEPS

    def remote(src, dst, ssem, rsem, who):
        return pltpu.make_async_remote_copy(
            src_ref=src, dst_ref=dst, send_sem=ssem, recv_sem=rsem,
            device_id={"tp": who}, device_id_type=MESH,
        )

    hid_cp = pltpu.make_async_copy(hid_ref, hall.at[:, pl.ds(k * rows, rows), :], loc.at[0])
    hid_cp.start()
    tok_cp = pltpu.make_async_copy(tok_in, tok_ref, loc.at[6])
    tok_cp.start()

    def stage_cp(g):
        part = pl.ds(g * 8 * pitch, 8 * pitch)
        return pltpu.make_async_copy(q_ref.at[part], stage.at[part], loc.at[1 + g])

    def w_cp(t, slot):
        return pltpu.make_async_copy(
            w_ref.at[pl.ds(pl.multiple_of(t * wrows, 8), wrows)], wbuf.at[slot], wsem.at[slot]
        )

    barrier = pltpu.get_barrier_semaphore()
    for who in (2 * right + c, 2 * left + c, mate):
        pl.semaphore_signal(barrier, inc=1, device_id={"tp": who}, device_id_type=MESH)
    pl.semaphore_wait(barrier, 3)

    def hpiece(src, half):
        return hall.at[:, pl.ds(pl.multiple_of(src * rows, rows), rows), pl.ds(half * hcol, hcol)]

    def hcopy(src, half, ssem, who):
        return remote(hpiece(src, half), hpiece(src, half), ssem, h_recv.at[src * 2 + half], who)

    def hwait(src, half):
        hcopy(src, half, h_send.at[0], mate).wait_recv()

    hid_cp.wait()
    own_sends = []
    for idx, (who, half) in enumerate(
        [(2 * right + c, 0), (2 * left + c, 1), (2 * right + c, 1), (2 * left + c, 0), (mate, 0), (mate, 1)]
    ):
        cp = hcopy(k, half, h_send.at[idx], who)
        cp.start()
        own_sends.append(cp)
    for g in range(rows // 8):
        stage_cp(g).start()
    w_cp(0, 0).start()
    w_cp(1, 1).start()

    z[:, 0:96, :] = jnp.zeros((positions, 96, batch), F32)
    z[:, width - 96:width, :] = jnp.zeros((positions, 96, batch), F32)

    tok_cp.wait()
    for g in range(rows // 8):
        stage_cp(g).wait()

    def qrows(g, i, j):
        return stage[pl.ds(g * 8 * pitch + drafts * j + i, 8, stride=pitch), :]

    groups = [(i, g) for i in range(drafts) for g in range(rows // 8)]
    lane_b = lax.broadcasted_iota(jnp.int32, (8, batch), 1)
    sub_b = lax.broadcasted_iota(jnp.int32, (8, batch), 0)
    lane_t = lax.broadcasted_iota(jnp.int32, (8, LANES), 1)
    mine = [lane_b == k * rows + 8 * g + sub_b for g in range(rows // 8)]
    tok_col = []
    for i, g in groups:
        t = jnp.where(mine[g], jnp.broadcast_to(tok_ref[i:i + 1, :].astype(F32), (8, batch)), 0.0)
        tok_col.append(jnp.broadcast_to(jnp.sum(t, axis=1, keepdims=True), (8, LANES)).astype(jnp.int32))

    def scan(j, carry):
        top, got = carry
        new_top, new_got = [], []
        col = lane_t + j * LANES
        for a, (i, g) in enumerate(groups):
            v = qrows(g, i, j)
            new_top.append(jnp.maximum(top[a], v))
            new_got.append(jnp.where(col == tok_col[a], v, got[a]))
        return tuple(new_top), tuple(new_got)

    zero8 = tuple(jnp.zeros((8, LANES), F32) for _ in groups)
    top, got = lax.fori_loop(0, all_tiles, scan, (zero8, zero8))
    qtop_row, qgot_row = [], []
    for i in range(drafts):
        acc_t = jnp.zeros((8, batch), F32)
        acc_g = jnp.zeros((8, batch), F32)
        for a, (ii, g) in enumerate(groups):
            if ii != i:
                continue
            tcol = jnp.max(top[a], axis=1, keepdims=True)
            gcol = jnp.sum(got[a], axis=1, keepdims=True)
            rowc[a] = jnp.broadcast_to(jnp.log(TOP) - 0.25 * jnp.log(tcol), (8, LANES))
            acc_t = acc_t + jnp.where(mine[g], jnp.broadcast_to(tcol, (8, batch)), 0.0)
            acc_g = acc_g + jnp.where(mine[g], jnp.broadcast_to(gcol, (8, batch)), 0.0)
        qtop_row.append(jnp.sum(acc_t, axis=0, keepdims=True))
        qgot_row.append(jnp.sum(acc_g, axis=0, keepdims=True))
    msgs[k] = jnp.zeros(msgs.shape[1:], F32)
    for i in range(drafts):
        msgs[k, 8 + i:9 + i, :] = qgot_row[i]
        msgs[k, 10 + i:11 + i, :] = qtop_row[i]

    def encode(dest, put):
        first = (dest * vocab) // LANES

        def body(j, _):
            for i in range(drafts):
                for gg in range(rows // 16):
                    parts = []
                    for g in (2 * gg, 2 * gg + 1):
                        v = qrows(g, i, first + j)
                        y = jnp.exp(0.25 * jnp.log(v) + rowc[i * (rows // 8) + g])
                        parts.append((y + 0.5).astype(jnp.int32) - HALF)
                    code = jnp.concatenate(parts, axis=0).astype(jnp.int16)
                    put(i, gg, j // per, pl.ds(pl.multiple_of((j % per) * LANES, LANES), LANES), code)
            return 0

        lax.fori_loop(0, tiles, body, 0)

    def to_slot(r):
        def put(i, gg, s, cols, code):
            scode[r, i, s, 16 * gg:16 * gg + 16, cols] = code

        return put

    def to_self(i, gg, s, cols, code):
        qall[i, s, pl.ds(pl.multiple_of(k * rows + 16 * gg, 16), 16), cols] = code

    encode(2 * far, to_slot(0))
    encode(2 * far + 1, to_slot(1))

    def unit(buf_i, i, s):
        return buf_i.at[i, s]

    def landing(src, i, s):
        return qall.at[i, s, pl.ds(pl.multiple_of(src * rows, rows), rows)]

    def direct(slot, i, s, who):
        return remote(
            unit(scode.at[slot], i, s), landing(k, i, s),
            q_send.at[slot * units + i * SEGS + s], q_recv.at[k * units + i * SEGS + s], who,
        )

    def core_of(way):
        return c if way == 0 else 1 - c

    def out_far(way, v):
        i, s, cc = v // SEGS, v % SEGS, core_of(way)
        who = 2 * (right if way == 0 else left) + c
        return remote(
            unit(scode.at[cc], i, s), rbuf.at[way, v],
            q_send.at[cc * units + i * SEGS + s], r_recv.at[way * units + v], who,
        )

    def relay(way, v):
        i, s, cc = v // SEGS, v % SEGS, core_of(way)
        src = 2 * (left if way == 0 else right) + c
        who = 2 * (right if way == 0 else left) + cc
        return remote(
            rbuf.at[way, v], landing(src, i, s),
            r_send.at[way * units + v], q_recv.at[src * units + i * SEGS + s], who,
        )

    def near(way, u):
        i, s, cc = u // (2 * SEGS), (u // 2) % SEGS, u % 2
        who = 2 * (right if way == 0 else left) + cc
        return direct(2 + 2 * way + cc, i, s, who)

    def send_far(v):
        out_far(0, v).start()
        out_far(1, v).start()

    def send_near(u):
        near(0, u).start()
        near(1, u).start()

    def pass_on(v):
        for way in range(2):
            out_far(way, v).wait_recv()
            relay(way, v).start()

    def first_far(v, _):
        send_far(v)
        return 0

    lax.fori_loop(0, SEGS, first_far, 0)

    fwd = []

    def forward(src, half):
        cp = hcopy(src, half, h_fwd.at[len(fwd)], mate)
        cp.start()
        fwd.append(cp)

    hwait(2 * left + c, 0)
    rel_r = hcopy(2 * left + c, 0, h_send.at[6], 2 * right + c)
    rel_r.start()
    forward(2 * left + c, 0)
    hwait(2 * right + c, 1)
    rel_l = hcopy(2 * right + c, 1, h_send.at[7], 2 * left + c)
    rel_l.start()
    forward(2 * right + c, 1)

    encode(2 * right, to_slot(2))
    encode(2 * right + 1, to_slot(3))
    encode(2 * left, to_slot(4))
    encode(2 * left + 1, to_slot(5))

    hwait(2 * left + c, 1)
    forward(2 * left + c, 1)
    hwait(2 * right + c, 0)
    forward(2 * right + c, 0)

    def first_near(u, _):
        send_near(u)
        return 0

    lax.fori_loop(0, 2 * SEGS, first_near, 0)
    encode(mate, to_slot(6))
    encode(k, to_self)

    def to_mate(u, _):
        direct(6, u // SEGS, u % SEGS, mate).start()
        return 0

    lax.fori_loop(0, drafts * SEGS, to_mate, 0)

    hwait(2 * far + c, 0)
    forward(2 * far + c, 0)
    hwait(2 * far + c, 1)
    forward(2 * far + c, 1)
    for chip in (x, left, right, far):
        for half in range(2):
            hwait(2 * chip + 1 - c, half)

    def step(t, top):
        slot = t % 2

        @pl.when((t >= 2) & (t < 4))
        def _():
            for e in range(SEGS // 2):
                pass_on((SEGS // 2) * (t - 2) + e)

        @pl.when((t >= 4) & (t < 6))
        def _():
            for e in range(SEGS // 2):
                send_far(SEGS + (SEGS // 2) * (t - 4) + e)

        @pl.when(t >= 6)
        def _():
            for e in range(SEGS // 2):
                send_near(2 * SEGS + (SEGS // 2) * (t - 6) + e)

        w_cp(t, slot).wait()
        prod = INV_TEMP * lax.dot_general(
            wbuf[slot], hall[...].reshape(positions * batch, dim), (((1,), (1,)), ((), ())), preferred_element_type=F32
        )
        base = pl.multiple_of(off + t * wrows, 8)
        for i in range(positions):
            z[i, pl.ds(base, wrows), :] = prod[:, i * batch:(i + 1) * batch]

        @pl.when(t + 2 < STEPS)
        def _():
            w_cp(t + 2, slot).start()

        return jnp.maximum(top, jnp.max(prod.reshape(wrows // 8, 8, positions * batch), axis=0))

    top = lax.fori_loop(0, STEPS, step, jnp.full((8, positions * batch), -jnp.inf, F32))
    own_max = jnp.max(top, axis=0, keepdims=True)

    chunk = 160
    row_i = lax.broadcasted_iota(jnp.int32, (chunk, batch), 0)
    for i in range(positions):
        m_i = own_max[:, i * batch:(i + 1) * batch]
        want = tok_ref[i:i + 1, :] - k * vocab if i < drafts else None

        def expo(t, carry, i=i, m_i=m_i, want=want):
            total, got = carry
            at = pl.ds(pl.multiple_of(off + t * chunk, 8), chunk)
            e = jnp.exp(z[i, at, :] - m_i)
            z[i, at, :] = e
            total = total + jnp.sum(e.reshape(chunk // 8, 8, batch), axis=0)
            if want is not None:
                pick = jnp.where(row_i + t * chunk == want, e, 0.0)
                got = got + jnp.sum(pick.reshape(chunk // 8, 8, batch), axis=0)
            return total, got

        zero = jnp.zeros((8, batch), F32)
        total, got = lax.fori_loop(0, vocab // chunk, expo, (zero, zero))
        msgs[k, i:i + 1, :] = m_i
        msgs[k, 3 + i:4 + i, :] = jnp.sum(total, axis=0, keepdims=True)
        if i < drafts:
            msgs[k, 6 + i:7 + i, :] = jnp.sum(got, axis=0, keepdims=True)

    def msg(p, src):
        return remote(msgs.at[src], msgs.at[src], m_send.at[p], m_recv.at[src], (k + p) % n)

    for p in range(1, n):
        msg(p, k).start()

    for v in range(SEGS, 2 * SEGS):
        pass_on(v)
    for p in range(1, n):
        msg(p, (k + p) % n).wait_recv()

    allm = msgs[...]
    peak = jnp.max(allm[:, 0:3, :], axis=0)
    part = jnp.exp(allm[:, 0:3, :] - peak[None])
    inv = 1.0 / jnp.sum(part * allm[:, 3:6, :], axis=0)
    p_pick = jnp.sum(part[:, 0:drafts, :] * allm[:, 6:8, :], axis=0) * inv[0:drafts]
    q_pick = jnp.sum(allm[:, 8:10, :], axis=0)
    q_scale = jnp.sum(allm[:, 10:12, :], axis=0) * (1.0 / (TOP * TOP * TOP * TOP))
    fac = jnp.exp(msgs[k, 0:3, :] - peak) * inv

    def scale(t, _):
        at = pl.ds(pl.multiple_of(off + t * chunk, 8), chunk)
        z[drafts, at, :] = z[drafts, at, :] * fac[drafts:drafts + 1, :]
        return 0

    lax.fori_loop(0, vocab // chunk, scale, 0)

    def xmsg(p, i, src):
        return remote(mass.at[i, src], mass.at[i, src], x_send.at[i * n + p], x_recv.at[i * n + src], (k + p) % n)

    def drain(u, _):
        direct(u // units, (u % units) // SEGS, u % SEGS, mate).wait_send()
        return 0

    def drain_relay(v, _):
        relay(0, v).wait_send()
        relay(1, v).wait_send()
        return 0

    for i in range(drafts):
        acc = [jnp.zeros((8, LANES), F32) for _ in range(batch // LANES)]
        for s in range(SEGS):
            if i == drafts - 1 and s == SEGS - 1:
                for cp in own_sends + [rel_r, rel_l] + fwd:
                    cp.wait_send()
                for p in range(1, n):
                    msg(p, k).wait_send()
                lax.fori_loop(0, (n - 1) * units, drain, 0)
            for p in range(1, n):
                src = (k + p) % n
                remote(
                    landing(src, i, s), landing(src, i, s), q_send.at[0],
                    q_recv.at[src * units + i * SEGS + s], mate,
                ).wait_recv()

            def body(t, acc, i=i, s=s):
                at = pl.ds(pl.multiple_of((s * (tiles // SEGS) + t) * LANES, LANES), LANES)
                out = []
                for h in range(batch // LANES):
                    ls = slice(h * LANES, (h + 1) * LANES)
                    code = qall[i, s, ls, pl.ds(pl.multiple_of(t * LANES, LANES), LANES)].astype(jnp.int32).astype(F32)
                    y = code.T + float(HALF)
                    y = y * y
                    qt = y * y * q_scale[i:i + 1, ls]
                    ex = jnp.maximum(z[i, at, ls] * fac[i:i + 1, ls] - qt, 0.0)
                    z[i, at, ls] = ex
                    out.append(acc[h] + jnp.sum(ex.reshape(LANES // 8, 8, LANES), axis=0))
                return tuple(out)

            acc = lax.fori_loop(0, tiles // SEGS, body, tuple(acc))
        for h in range(batch // LANES):
            mass[i, k, :, h * LANES:(h + 1) * LANES] = jnp.sum(acc[h], axis=0, keepdims=True)
        for p in range(1, n):
            xmsg(p, i, k).start()
    lax.fori_loop(0, units, drain_relay, 0)
    small_ref[...] = jnp.zeros(small_ref.shape, F32)
    small_ref[2:4, :] = p_pick
    small_ref[4:6, :] = q_pick
    for i in range(drafts):
        for p in range(1, n):
            xmsg(p, i, (k + p) % n).wait_recv()
        total = jnp.sum(mass[i], axis=0)
        small_ref[i:i + 1, :] = 1.0 / total

    for p in range(1, n):
        for i in range(drafts):
            xmsg(p, i, k).wait_send()


def finish(n, z, small, res_ref, bonus_ref, acc_out, exp_out, buf, acc_ref, exp_ref, sem):
    drafts, vocab, _ = res_ref.shape
    off = pl.multiple_of((lax.axis_index("tp") * vocab) % LANES, 8)
    last = pltpu.make_async_copy(z.at[drafts, pl.ds(off, vocab), :], bonus_ref, sem.at[0])
    last.start()
    copies = [last]
    accept = jnp.minimum(small[2:4, :] / small[4:6, :], 1.0)
    acc_ref[...] = accept
    exp_ref[...] = accept[0:1] + accept[0:1] * accept[1:2]
    part = vocab // PARTS
    for i in range(drafts):
        scale = small[i:i + 1, :]
        for t in range(PARTS):
            to = pl.ds(t * part, part)
            buf[i, to, :] = z[i, pl.ds(pl.multiple_of(off + t * part, 8), part), :] * scale
            cp = pltpu.make_async_copy(buf.at[i, to], res_ref.at[i, to], sem.at[len(copies)])
            cp.start()
            copies.append(cp)
        if i == 0:
            for src, dst in ((acc_ref, acc_out), (exp_ref, exp_out)):
                cp = pltpu.make_async_copy(src, dst, sem.at[len(copies)])
                cp.start()
                copies.append(cp)
    for cp in copies:
        cp.wait()


def solution(mesh):
    n = mesh.shape["tp"]

    def local(hid, w, q, tok):
        rows, positions, dim = hid.shape
        vocab = w.shape[1]
        drafts = positions - 1
        batch = rows * n
        q_tiles = q.shape[2] // LANES
        width = -(-vocab // LANES) * LANES
        q_view = q.reshape(rows, drafts, q_tiles, LANES).transpose(0, 2, 1, 3)
        q_view = with_layout_constraint(q_view, Layout((0, 1, 2, 3))).reshape(-1, LANES)
        dma = pltpu.SemaphoreType.DMA
        vmem, anywhere = pl.BlockSpec(memory_space=pltpu.VMEM), pl.BlockSpec(memory_space=pltpu.HBM)
        z, small = pl.pallas_call(
            functools.partial(kernel, n),
            out_shape=(
                jax.ShapeDtypeStruct((positions, width, batch), F32),
                jax.ShapeDtypeStruct((8, batch), F32),
            ),
            in_specs=[anywhere] * 4,
            out_specs=(vmem, vmem),
            scratch_shapes=[
                pltpu.VMEM((drafts, batch), jnp.int32),
                pltpu.VMEM((positions, batch, dim), jnp.bfloat16),
                pltpu.VMEM((rows * q_tiles * drafts, LANES), F32),
                pltpu.VMEM((n - 1, drafts, SEGS, rows, width // SEGS), jnp.int16),
                pltpu.VMEM((drafts, SEGS, batch, width // SEGS), jnp.int16),
                pltpu.VMEM((2, drafts * SEGS, rows, width // SEGS), jnp.int16),
                pltpu.VMEM((2, vocab // STEPS, dim), jnp.bfloat16),
                pltpu.VMEM((n, 16, batch), F32),
                pltpu.VMEM((drafts, n, 1, batch), F32),
                pltpu.VMEM((drafts * (rows // 8), 8, LANES), F32),
                dma((8,)), dma((8,)), dma((2 * n,)),
                dma((n * drafts * SEGS,)), dma((n * drafts * SEGS,)), dma((2 * drafts * SEGS,)), dma((2 * drafts * SEGS,)),
                dma((n,)), dma((n,)), dma((2 * n,)), dma((2 * n,)),
                dma((8,)), dma((2,)),
            ],
            compiler_params=pltpu.CompilerParams(
                collective_id=0, has_side_effects=True, vmem_limit_bytes=40 * 2**20
            ),
        )(*[pltpu.with_memory_space_constraint(a, pltpu.HBM) for a in (tok.T, hid.transpose(1, 0, 2), w.T, q_view)])
        residual, bonus, accept, expected = pl.pallas_call(
            functools.partial(finish, n),
            out_shape=(
                jax.ShapeDtypeStruct((drafts, vocab, batch), F32),
                jax.ShapeDtypeStruct((vocab, batch), F32),
                jax.ShapeDtypeStruct((drafts, batch), F32),
                jax.ShapeDtypeStruct((1, batch), F32),
            ),
            in_specs=[vmem, vmem],
            out_specs=(anywhere,) * 4,
            scratch_shapes=[
                pltpu.VMEM((drafts, vocab, batch), F32),
                pltpu.VMEM((drafts, batch), F32),
                pltpu.VMEM((1, batch), F32),
                dma((drafts * PARTS + 3,)),
            ],
            compiler_params=pltpu.CompilerParams(vmem_limit_bytes=24 * 2**20),
        )(z, small)
        return accept.T, expected[0], residual.transpose(2, 0, 1), bonus.T

    return jax.shard_map(
        local,
        mesh=mesh,
        in_specs=(P(("dp", "tp"), None, None), P(None, "tp"), P(("dp", "tp"), None, None), P("dp", None)),
        out_specs=(P("dp", None), P("dp"), P("dp", None, "tp"), P("dp", "tp")),
        check_vma=False,
    )
```

```python
import functools

import jax
import jax.numpy as jnp
from jax import lax
from jax.experimental import pallas as pl
from jax.experimental.pallas import tpu as pltpu
from jax.experimental.layout import Layout, with_layout_constraint
from jax.sharding import PartitionSpec as P

INV_TEMP = 1.25
TOP = 65535.0
HALF = 32768
LANES = 128
SEGS = 2
STEPS = 10
PARTS = 5
F32 = jnp.float32
MESH = pl.DeviceIdType.MESH


def kernel(
    n, tok_in, hid_ref, w_ref, q_ref,
    z, small_ref,
    tok_ref, hall, stage, scode, qall, rbuf, wbuf, msgs, mass, rowc,
    h_send, h_fwd, h_recv, q_send, q_recv, r_send, r_recv,
    m_send, m_recv, x_send, x_recv, loc, wsem,
):
    k = lax.axis_index("tp")
    x, c = k // 2, k % 2
    chips = n // 2
    right, left = (x + 1) % chips, (x + chips - 1) % chips
    far = (x + 2) % chips
    mate = 2 * x + 1 - c
    positions, batch, dim = hall.shape
    drafts = positions - 1
    rows = batch // n
    vocab = w_ref.shape[0]
    seg = qall.shape[3]
    width = seg * SEGS
    tiles = width // LANES
    units = drafts * SEGS
    per = seg // LANES
    pitch = q_ref.shape[0] // rows
    all_tiles = pitch // drafts
    off = (k * vocab) % LANES
    hcol = dim // 2
    wrows = vocab // STEPS

    def remote(src, dst, ssem, rsem, who):
        return pltpu.make_async_remote_copy(
            src_ref=src, dst_ref=dst, send_sem=ssem, recv_sem=rsem,
            device_id={"tp": who}, device_id_type=MESH,
        )

    hid_cp = pltpu.make_async_copy(hid_ref, hall.at[:, pl.ds(k * rows, rows), :], loc.at[0])
    hid_cp.start()
    tok_cp = pltpu.make_async_copy(tok_in, tok_ref, loc.at[6])
    tok_cp.start()

    def stage_cp(g):
        part = pl.ds(g * 8 * pitch, 8 * pitch)
        return pltpu.make_async_copy(q_ref.at[part], stage.at[part], loc.at[1 + g])

    def w_cp(t, slot):
        return pltpu.make_async_copy(
            w_ref.at[pl.ds(pl.multiple_of(t * wrows, 8), wrows)], wbuf.at[slot], wsem.at[slot]
        )

    barrier = pltpu.get_barrier_semaphore()
    for who in (2 * right + c, 2 * left + c, mate):
        pl.semaphore_signal(barrier, inc=1, device_id={"tp": who}, device_id_type=MESH)
    pl.semaphore_wait(barrier, 3)

    def hpiece(src, half):
        return hall.at[:, pl.ds(pl.multiple_of(src * rows, rows), rows), pl.ds(half * hcol, hcol)]

    def hcopy(src, half, ssem, who):
        return remote(hpiece(src, half), hpiece(src, half), ssem, h_recv.at[src * 2 + half], who)

    def hwait(src, half):
        hcopy(src, half, h_send.at[0], mate).wait_recv()

    hid_cp.wait()
    own_sends = []
    for idx, (who, half) in enumerate(
        [(2 * right + c, 0), (2 * left + c, 1), (2 * right + c, 1), (2 * left + c, 0), (mate, 0), (mate, 1)]
    ):
        cp = hcopy(k, half, h_send.at[idx], who)
        cp.start()
        own_sends.append(cp)
    for g in range(rows // 8):
        stage_cp(g).start()
    w_cp(0, 0).start()
    w_cp(1, 1).start()

    z[:, 0:96, :] = jnp.zeros((positions, 96, batch), F32)
    z[:, width - 96:width, :] = jnp.zeros((positions, 96, batch), F32)

    tok_cp.wait()
    for g in range(rows // 8):
        stage_cp(g).wait()

    def qrows(g, i, j):
        return stage[pl.ds(g * 8 * pitch + drafts * j + i, 8, stride=pitch), :]

    groups = [(i, g) for i in range(drafts) for g in range(rows // 8)]
    lane_b = lax.broadcasted_iota(jnp.int32, (8, batch), 1)
    sub_b = lax.broadcasted_iota(jnp.int32, (8, batch), 0)
    lane_t = lax.broadcasted_iota(jnp.int32, (8, LANES), 1)
    mine = [lane_b == k * rows + 8 * g + sub_b for g in range(rows // 8)]
    tok_col = []
    for i, g in groups:
        t = jnp.where(mine[g], jnp.broadcast_to(tok_ref[i:i + 1, :].astype(F32), (8, batch)), 0.0)
        tok_col.append(jnp.broadcast_to(jnp.sum(t, axis=1, keepdims=True), (8, LANES)).astype(jnp.int32))

    def scan(j, carry):
        top, got = carry
        new_top, new_got = [], []
        col = lane_t + j * LANES
        for a, (i, g) in enumerate(groups):
            v = qrows(g, i, j)
            new_top.append(jnp.maximum(top[a], v))
            new_got.append(jnp.where(col == tok_col[a], v, got[a]))
        return tuple(new_top), tuple(new_got)

    zero8 = tuple(jnp.zeros((8, LANES), F32) for _ in groups)
    top, got = lax.fori_loop(0, all_tiles, scan, (zero8, zero8))
    qtop_row, qgot_row = [], []
    for i in range(drafts):
        acc_t = jnp.zeros((8, batch), F32)
        acc_g = jnp.zeros((8, batch), F32)
        for a, (ii, g) in enumerate(groups):
            if ii != i:
                continue
            tcol = jnp.max(top[a], axis=1, keepdims=True)
            gcol = jnp.sum(got[a], axis=1, keepdims=True)
            rowc[a] = jnp.broadcast_to(jnp.log(TOP) - 0.25 * jnp.log(tcol), (8, LANES))
            acc_t = acc_t + jnp.where(mine[g], jnp.broadcast_to(tcol, (8, batch)), 0.0)
            acc_g = acc_g + jnp.where(mine[g], jnp.broadcast_to(gcol, (8, batch)), 0.0)
        qtop_row.append(jnp.sum(acc_t, axis=0, keepdims=True))
        qgot_row.append(jnp.sum(acc_g, axis=0, keepdims=True))
    msgs[k] = jnp.zeros(msgs.shape[1:], F32)
    for i in range(drafts):
        msgs[k, 8 + i:9 + i, :] = qgot_row[i]
        msgs[k, 10 + i:11 + i, :] = qtop_row[i]

    def encode(dest, put):
        first = (dest * vocab) // LANES

        def body(j, _):
            for i in range(drafts):
                for gg in range(rows // 16):
                    parts = []
                    for g in (2 * gg, 2 * gg + 1):
                        v = qrows(g, i, first + j)
                        y = jnp.exp(0.25 * jnp.log(v) + rowc[i * (rows // 8) + g])
                        parts.append((y + 0.5).astype(jnp.int32) - HALF)
                    code = jnp.concatenate(parts, axis=0).astype(jnp.int16)
                    put(i, gg, j // per, pl.ds(pl.multiple_of((j % per) * LANES, LANES), LANES), code)
            return 0

        lax.fori_loop(0, tiles, body, 0)

    def to_slot(r):
        def put(i, gg, s, cols, code):
            scode[r, i, s, 16 * gg:16 * gg + 16, cols] = code

        return put

    def to_self(i, gg, s, cols, code):
        qall[i, s, pl.ds(pl.multiple_of(k * rows + 16 * gg, 16), 16), cols] = code

    encode(2 * far, to_slot(0))
    encode(2 * far + 1, to_slot(1))

    fwd = []

    def forward(src, half):
        cp = hcopy(src, half, h_fwd.at[len(fwd)], mate)
        cp.start()
        fwd.append(cp)

    hwait(2 * left + c, 0)
    rel_r = hcopy(2 * left + c, 0, h_send.at[6], 2 * right + c)
    rel_r.start()
    forward(2 * left + c, 0)
    hwait(2 * right + c, 1)
    rel_l = hcopy(2 * right + c, 1, h_send.at[7], 2 * left + c)
    rel_l.start()
    forward(2 * right + c, 1)

    def unit(buf_i, i, s):
        return buf_i.at[i, s]

    def landing(src, i, s):
        return qall.at[i, s, pl.ds(pl.multiple_of(src * rows, rows), rows)]

    def direct(slot, i, s, who):
        return remote(
            unit(scode.at[slot], i, s), landing(k, i, s),
            q_send.at[slot * units + i * SEGS + s], q_recv.at[k * units + i * SEGS + s], who,
        )

    def core_of(way):
        return c if way == 0 else 1 - c

    def out_far(way, v):
        i, s, cc = v // SEGS, v % SEGS, core_of(way)
        who = 2 * (right if way == 0 else left) + c
        return remote(
            unit(scode.at[cc], i, s), rbuf.at[way, v],
            q_send.at[cc * units + i * SEGS + s], r_recv.at[way * units + v], who,
        )

    def relay(way, v):
        i, s, cc = v // SEGS, v % SEGS, core_of(way)
        src = 2 * (left if way == 0 else right) + c
        who = 2 * (right if way == 0 else left) + cc
        return remote(
            rbuf.at[way, v], landing(src, i, s),
            r_send.at[way * units + v], q_recv.at[src * units + i * SEGS + s], who,
        )

    def near(way, u):
        i, s, cc = u // (2 * SEGS), (u // 2) % SEGS, u % 2
        who = 2 * (right if way == 0 else left) + cc
        return direct(2 + 2 * way + cc, i, s, who)

    def send_far(v):
        out_far(0, v).start()
        out_far(1, v).start()

    def send_near(u):
        near(0, u).start()
        near(1, u).start()

    def pass_on(v):
        for way in range(2):
            out_far(way, v).wait_recv()
            relay(way, v).start()

    encode(2 * right, to_slot(2))
    encode(2 * right + 1, to_slot(3))
    encode(2 * left, to_slot(4))
    encode(2 * left + 1, to_slot(5))

    hwait(2 * left + c, 1)
    forward(2 * left + c, 1)
    hwait(2 * right + c, 0)
    forward(2 * right + c, 0)

    def first_far(v, _):
        send_far(v)
        return 0

    def first_near(u, _):
        send_near(u)
        return 0

    lax.fori_loop(0, SEGS, first_far, 0)
    lax.fori_loop(0, 2 * SEGS, first_near, 0)
    encode(mate, to_slot(6))
    encode(k, to_self)

    def to_mate(u, _):
        direct(6, u // SEGS, u % SEGS, mate).start()
        return 0

    lax.fori_loop(0, drafts * SEGS, to_mate, 0)

    hwait(2 * far + c, 0)
    forward(2 * far + c, 0)
    hwait(2 * far + c, 1)
    forward(2 * far + c, 1)
    for chip in (x, left, right, far):
        for half in range(2):
            hwait(2 * chip + 1 - c, half)

    def step(t, top):
        slot = t % 2

        @pl.when((t >= 2) & (t < 4))
        def _():
            for e in range(SEGS // 2):
                pass_on((SEGS // 2) * (t - 2) + e)

        @pl.when((t >= 4) & (t < 6))
        def _():
            for e in range(SEGS // 2):
                send_far(SEGS + (SEGS // 2) * (t - 4) + e)

        @pl.when(t >= 6)
        def _():
            for e in range(SEGS // 2):
                send_near(2 * SEGS + (SEGS // 2) * (t - 6) + e)

        w_cp(t, slot).wait()
        prod = INV_TEMP * lax.dot_general(
            wbuf[slot], hall[...].reshape(positions * batch, dim), (((1,), (1,)), ((), ())), preferred_element_type=F32
        )
        base = pl.multiple_of(off + t * wrows, 8)
        for i in range(positions):
            z[i, pl.ds(base, wrows), :] = prod[:, i * batch:(i + 1) * batch]

        @pl.when(t + 2 < STEPS)
        def _():
            w_cp(t + 2, slot).start()

        return jnp.maximum(top, jnp.max(prod.reshape(wrows // 8, 8, positions * batch), axis=0))

    top = lax.fori_loop(0, STEPS, step, jnp.full((8, positions * batch), -jnp.inf, F32))
    own_max = jnp.max(top, axis=0, keepdims=True)

    chunk = 160
    row_i = lax.broadcasted_iota(jnp.int32, (chunk, batch), 0)
    for i in range(positions):
        m_i = own_max[:, i * batch:(i + 1) * batch]
        want = tok_ref[i:i + 1, :] - k * vocab if i < drafts else None

        def expo(t, carry, i=i, m_i=m_i, want=want):
            total, got = carry
            at = pl.ds(pl.multiple_of(off + t * chunk, 8), chunk)
            e = jnp.exp(z[i, at, :] - m_i)
            z[i, at, :] = e
            total = total + jnp.sum(e.reshape(chunk // 8, 8, batch), axis=0)
            if want is not None:
                pick = jnp.where(row_i + t * chunk == want, e, 0.0)
                got = got + jnp.sum(pick.reshape(chunk // 8, 8, batch), axis=0)
            return total, got

        zero = jnp.zeros((8, batch), F32)
        total, got = lax.fori_loop(0, vocab // chunk, expo, (zero, zero))
        msgs[k, i:i + 1, :] = m_i
        msgs[k, 3 + i:4 + i, :] = jnp.sum(total, axis=0, keepdims=True)
        if i < drafts:
            msgs[k, 6 + i:7 + i, :] = jnp.sum(got, axis=0, keepdims=True)

    def msg(p, src):
        return remote(msgs.at[src], msgs.at[src], m_send.at[p], m_recv.at[src], (k + p) % n)

    for p in range(1, n):
        msg(p, k).start()

    for v in range(SEGS, 2 * SEGS):
        pass_on(v)
    for p in range(1, n):
        msg(p, (k + p) % n).wait_recv()

    allm = msgs[...]
    peak = jnp.max(allm[:, 0:3, :], axis=0)
    part = jnp.exp(allm[:, 0:3, :] - peak[None])
    inv = 1.0 / jnp.sum(part * allm[:, 3:6, :], axis=0)
    p_pick = jnp.sum(part[:, 0:drafts, :] * allm[:, 6:8, :], axis=0) * inv[0:drafts]
    q_pick = jnp.sum(allm[:, 8:10, :], axis=0)
    q_scale = jnp.sum(allm[:, 10:12, :], axis=0) * (1.0 / (TOP * TOP * TOP * TOP))
    fac = jnp.exp(msgs[k, 0:3, :] - peak) * inv

    def scale(t, _):
        at = pl.ds(pl.multiple_of(off + t * chunk, 8), chunk)
        z[drafts, at, :] = z[drafts, at, :] * fac[drafts:drafts + 1, :]
        return 0

    lax.fori_loop(0, vocab // chunk, scale, 0)

    def xmsg(p, i, src):
        return remote(mass.at[i, src], mass.at[i, src], x_send.at[i * n + p], x_recv.at[i * n + src], (k + p) % n)

    def drain(u, _):
        direct(u // units, (u % units) // SEGS, u % SEGS, mate).wait_send()
        return 0

    def drain_relay(v, _):
        relay(0, v).wait_send()
        relay(1, v).wait_send()
        return 0

    for i in range(drafts):
        acc = [jnp.zeros((8, LANES), F32) for _ in range(batch // LANES)]
        for s in range(SEGS):
            if i == drafts - 1 and s == SEGS - 1:
                for cp in own_sends + [rel_r, rel_l] + fwd:
                    cp.wait_send()
                for p in range(1, n):
                    msg(p, k).wait_send()
                lax.fori_loop(0, (n - 1) * units, drain, 0)
            for p in range(1, n):
                src = (k + p) % n
                remote(
                    landing(src, i, s), landing(src, i, s), q_send.at[0],
                    q_recv.at[src * units + i * SEGS + s], mate,
                ).wait_recv()

            def body(t, acc, i=i, s=s):
                at = pl.ds(pl.multiple_of((s * (tiles // SEGS) + t) * LANES, LANES), LANES)
                out = []
                for h in range(batch // LANES):
                    ls = slice(h * LANES, (h + 1) * LANES)
                    code = qall[i, s, ls, pl.ds(pl.multiple_of(t * LANES, LANES), LANES)].astype(jnp.int32).astype(F32)
                    y = code.T + float(HALF)
                    y = y * y
                    qt = y * y * q_scale[i:i + 1, ls]
                    ex = jnp.maximum(z[i, at, ls] * fac[i:i + 1, ls] - qt, 0.0)
                    z[i, at, ls] = ex
                    out.append(acc[h] + jnp.sum(ex.reshape(LANES // 8, 8, LANES), axis=0))
                return tuple(out)

            acc = lax.fori_loop(0, tiles // SEGS, body, tuple(acc))
        for h in range(batch // LANES):
            mass[i, k, :, h * LANES:(h + 1) * LANES] = jnp.sum(acc[h], axis=0, keepdims=True)
        for p in range(1, n):
            xmsg(p, i, k).start()
    lax.fori_loop(0, units, drain_relay, 0)
    small_ref[...] = jnp.zeros(small_ref.shape, F32)
    small_ref[2:4, :] = p_pick
    small_ref[4:6, :] = q_pick
    for i in range(drafts):
        for p in range(1, n):
            xmsg(p, i, (k + p) % n).wait_recv()
        total = jnp.sum(mass[i], axis=0)
        small_ref[i:i + 1, :] = 1.0 / total

    for p in range(1, n):
        for i in range(drafts):
            xmsg(p, i, k).wait_send()


def finish(n, z, small, res_ref, bonus_ref, acc_out, exp_out, buf, acc_ref, exp_ref, sem):
    drafts, vocab, _ = res_ref.shape
    off = pl.multiple_of((lax.axis_index("tp") * vocab) % LANES, 8)
    part = vocab // PARTS
    copies = []
    for t in range(PARTS):
        at = pl.ds(pl.multiple_of(off + t * part, 8), part)
        cp = pltpu.make_async_copy(z.at[drafts, at, :], bonus_ref.at[pl.ds(t * part, part)], sem.at[t])
        cp.start()
        copies.append(cp)
    accept = jnp.minimum(small[2:4, :] / small[4:6, :], 1.0)
    acc_ref[...] = accept
    exp_ref[...] = accept[0:1] + accept[0:1] * accept[1:2]
    for i in range(drafts):
        scale = small[i:i + 1, :]
        for t in range(PARTS):
            to = pl.ds(t * part, part)
            buf[i, to, :] = z[i, pl.ds(pl.multiple_of(off + t * part, 8), part), :] * scale
            cp = pltpu.make_async_copy(buf.at[i, to], res_ref.at[i, to], sem.at[len(copies)])
            cp.start()
            copies.append(cp)
        if i == 0:
            for src, dst in ((acc_ref, acc_out), (exp_ref, exp_out)):
                cp = pltpu.make_async_copy(src, dst, sem.at[len(copies)])
                cp.start()
                copies.append(cp)
    for cp in copies:
        cp.wait()


def solution(mesh):
    n = mesh.shape["tp"]

    def local(hid, w, q, tok):
        rows, positions, dim = hid.shape
        vocab = w.shape[1]
        drafts = positions - 1
        batch = rows * n
        q_tiles = q.shape[2] // LANES
        width = -(-vocab // LANES) * LANES
        q_view = q.reshape(rows, drafts, q_tiles, LANES).transpose(0, 2, 1, 3)
        q_view = with_layout_constraint(q_view, Layout((0, 1, 2, 3))).reshape(-1, LANES)
        dma = pltpu.SemaphoreType.DMA
        vmem, anywhere = pl.BlockSpec(memory_space=pltpu.VMEM), pl.BlockSpec(memory_space=pltpu.HBM)
        z, small = pl.pallas_call(
            functools.partial(kernel, n),
            out_shape=(
                jax.ShapeDtypeStruct((positions, width, batch), F32),
                jax.ShapeDtypeStruct((8, batch), F32),
            ),
            in_specs=[anywhere] * 4,
            out_specs=(vmem, vmem),
            scratch_shapes=[
                pltpu.VMEM((drafts, batch), jnp.int32),
                pltpu.VMEM((positions, batch, dim), jnp.bfloat16),
                pltpu.VMEM((rows * q_tiles * drafts, LANES), F32),
                pltpu.VMEM((n - 1, drafts, SEGS, rows, width // SEGS), jnp.int16),
                pltpu.VMEM((drafts, SEGS, batch, width // SEGS), jnp.int16),
                pltpu.VMEM((2, drafts * SEGS, rows, width // SEGS), jnp.int16),
                pltpu.VMEM((2, vocab // STEPS, dim), jnp.bfloat16),
                pltpu.VMEM((n, 16, batch), F32),
                pltpu.VMEM((drafts, n, 1, batch), F32),
                pltpu.VMEM((drafts * (rows // 8), 8, LANES), F32),
                dma((8,)), dma((8,)), dma((2 * n,)),
                dma((n * drafts * SEGS,)), dma((n * drafts * SEGS,)), dma((2 * drafts * SEGS,)), dma((2 * drafts * SEGS,)),
                dma((n,)), dma((n,)), dma((2 * n,)), dma((2 * n,)),
                dma((8,)), dma((2,)),
            ],
            compiler_params=pltpu.CompilerParams(
                collective_id=0, has_side_effects=True, vmem_limit_bytes=40 * 2**20
            ),
        )(*[pltpu.with_memory_space_constraint(a, pltpu.HBM) for a in (tok.T, hid.transpose(1, 0, 2), w.T, q_view)])
        residual, bonus, accept, expected = pl.pallas_call(
            functools.partial(finish, n),
            out_shape=(
                jax.ShapeDtypeStruct((drafts, vocab, batch), F32),
                jax.ShapeDtypeStruct((vocab, batch), F32),
                jax.ShapeDtypeStruct((drafts, batch), F32),
                jax.ShapeDtypeStruct((1, batch), F32),
            ),
            in_specs=[vmem, vmem],
            out_specs=(anywhere,) * 4,
            scratch_shapes=[
                pltpu.VMEM((drafts, vocab, batch), F32),
                pltpu.VMEM((drafts, batch), F32),
                pltpu.VMEM((1, batch), F32),
                dma(((drafts + 1) * PARTS + 2,)),
            ],
            compiler_params=pltpu.CompilerParams(vmem_limit_bytes=24 * 2**20),
        )(z, small)
        return accept.T, expected[0], residual.transpose(2, 0, 1), bonus.T

    return jax.shard_map(
        local,
        mesh=mesh,
        in_specs=(P(("dp", "tp"), None, None), P(None, "tp"), P(("dp", "tp"), None, None), P("dp", None)),
        out_specs=(P("dp", None), P("dp"), P("dp", None, "tp"), P("dp", "tp")),
        check_vma=False,
    )
```

```python
import functools

import jax
import jax.numpy as jnp
from jax import lax
from jax.experimental import pallas as pl
from jax.experimental.pallas import tpu as pltpu
from jax.experimental.layout import Layout, with_layout_constraint
from jax.sharding import PartitionSpec as P

INV_TEMP = 1.25
TOP = 65535.0
HALF = 32768
LANES = 128
SEGS = 2
STEPS = 10
PARTS = 5
F32 = jnp.float32
MESH = pl.DeviceIdType.MESH


def kernel(
    n, tok_in, hid_ref, w_ref, q_ref,
    z, small_ref,
    tok_ref, hall, stage, scode, qall, rbuf, wbuf, msgs, mass, rowc,
    h_send, h_fwd, h_recv, q_send, q_recv, r_send, r_recv,
    m_send, m_recv, x_send, x_recv, loc, wsem,
):
    k = lax.axis_index("tp")
    x, c = k // 2, k % 2
    chips = n // 2
    right, left = (x + 1) % chips, (x + chips - 1) % chips
    far = (x + 2) % chips
    mate = 2 * x + 1 - c
    positions, batch, dim = hall.shape
    drafts = positions - 1
    rows = batch // n
    vocab = w_ref.shape[0]
    seg = qall.shape[3]
    width = seg * SEGS
    tiles = width // LANES
    units = drafts * SEGS
    per = seg // LANES
    pitch = q_ref.shape[0] // rows
    all_tiles = pitch // drafts
    off = (k * vocab) % LANES
    hcol = dim // 2
    wrows = vocab // STEPS

    def remote(src, dst, ssem, rsem, who):
        return pltpu.make_async_remote_copy(
            src_ref=src, dst_ref=dst, send_sem=ssem, recv_sem=rsem,
            device_id={"tp": who}, device_id_type=MESH,
        )

    hid_cp = pltpu.make_async_copy(hid_ref, hall.at[:, pl.ds(k * rows, rows), :], loc.at[0])
    hid_cp.start()
    tok_cp = pltpu.make_async_copy(tok_in, tok_ref, loc.at[6])
    tok_cp.start()

    def stage_cp(g):
        part = pl.ds(g * 8 * pitch, 8 * pitch)
        return pltpu.make_async_copy(q_ref.at[part], stage.at[part], loc.at[1 + g])

    def w_cp(t, slot):
        return pltpu.make_async_copy(
            w_ref.at[pl.ds(pl.multiple_of(t * wrows, 8), wrows)], wbuf.at[slot], wsem.at[slot]
        )

    barrier = pltpu.get_barrier_semaphore()
    for who in (2 * right + c, 2 * left + c, mate):
        pl.semaphore_signal(barrier, inc=1, device_id={"tp": who}, device_id_type=MESH)
    pl.semaphore_wait(barrier, 3)

    def hpiece(src, half):
        return hall.at[:, pl.ds(pl.multiple_of(src * rows, rows), rows), pl.ds(half * hcol, hcol)]

    def hcopy(src, half, ssem, who):
        return remote(hpiece(src, half), hpiece(src, half), ssem, h_recv.at[src * 2 + half], who)

    def hwait(src, half):
        hcopy(src, half, h_send.at[0], mate).wait_recv()

    hid_cp.wait()
    own_sends = []
    for idx, (who, half) in enumerate(
        [(2 * right + c, 0), (2 * left + c, 1), (2 * right + c, 1), (2 * left + c, 0), (mate, 0), (mate, 1)]
    ):
        cp = hcopy(k, half, h_send.at[idx], who)
        cp.start()
        own_sends.append(cp)
    for g in range(rows // 8):
        stage_cp(g).start()
    w_cp(0, 0).start()
    w_cp(1, 1).start()

    z[:, 0:96, :] = jnp.zeros((positions, 96, batch), F32)
    z[:, width - 96:width, :] = jnp.zeros((positions, 96, batch), F32)

    tok_cp.wait()
    for g in range(rows // 8):
        stage_cp(g).wait()

    def qrows(g, i, j):
        return stage[pl.ds(g * 8 * pitch + drafts * j + i, 8, stride=pitch), :]

    groups = [(i, g) for i in range(drafts) for g in range(rows // 8)]
    lane_b = lax.broadcasted_iota(jnp.int32, (8, batch), 1)
    sub_b = lax.broadcasted_iota(jnp.int32, (8, batch), 0)
    lane_t = lax.broadcasted_iota(jnp.int32, (8, LANES), 1)
    mine = [lane_b == k * rows + 8 * g + sub_b for g in range(rows // 8)]
    tok_col = []
    for i, g in groups:
        t = jnp.where(mine[g], jnp.broadcast_to(tok_ref[i:i + 1, :].astype(F32), (8, batch)), 0.0)
        tok_col.append(jnp.broadcast_to(jnp.sum(t, axis=1, keepdims=True), (8, LANES)).astype(jnp.int32))

    def scan(j, carry):
        top, got = carry
        new_top, new_got = [], []
        col = lane_t + j * LANES
        for a, (i, g) in enumerate(groups):
            v = qrows(g, i, j)
            new_top.append(jnp.maximum(top[a], v))
            new_got.append(jnp.where(col == tok_col[a], v, got[a]))
        return tuple(new_top), tuple(new_got)

    zero8 = tuple(jnp.zeros((8, LANES), F32) for _ in groups)
    top, got = lax.fori_loop(0, all_tiles, scan, (zero8, zero8))
    qtop_row, qgot_row = [], []
    for i in range(drafts):
        acc_t = jnp.zeros((8, batch), F32)
        acc_g = jnp.zeros((8, batch), F32)
        for a, (ii, g) in enumerate(groups):
            if ii != i:
                continue
            tcol = jnp.max(top[a], axis=1, keepdims=True)
            gcol = jnp.sum(got[a], axis=1, keepdims=True)
            rowc[a] = jnp.broadcast_to(jnp.log(TOP) - 0.25 * jnp.log(tcol), (8, LANES))
            acc_t = acc_t + jnp.where(mine[g], jnp.broadcast_to(tcol, (8, batch)), 0.0)
            acc_g = acc_g + jnp.where(mine[g], jnp.broadcast_to(gcol, (8, batch)), 0.0)
        qtop_row.append(jnp.sum(acc_t, axis=0, keepdims=True))
        qgot_row.append(jnp.sum(acc_g, axis=0, keepdims=True))
    msgs[k] = jnp.zeros(msgs.shape[1:], F32)
    for i in range(drafts):
        msgs[k, 8 + i:9 + i, :] = qgot_row[i]
        msgs[k, 10 + i:11 + i, :] = qtop_row[i]

    def encode(dest, put):
        first = (dest * vocab) // LANES

        def body(j, _):
            for i in range(drafts):
                for gg in range(rows // 16):
                    parts = []
                    for g in (2 * gg, 2 * gg + 1):
                        v = qrows(g, i, first + j)
                        y = jnp.exp(0.25 * jnp.log(v) + rowc[i * (rows // 8) + g])
                        parts.append((y + 0.5).astype(jnp.int32) - HALF)
                    code = jnp.concatenate(parts, axis=0).astype(jnp.int16)
                    put(i, gg, j // per, pl.ds(pl.multiple_of((j % per) * LANES, LANES), LANES), code)
            return 0

        lax.fori_loop(0, tiles, body, 0)

    def to_slot(r):
        def put(i, gg, s, cols, code):
            scode[r, i, s, 16 * gg:16 * gg + 16, cols] = code

        return put

    def to_self(i, gg, s, cols, code):
        qall[i, s, pl.ds(pl.multiple_of(k * rows + 16 * gg, 16), 16), cols] = code

    encode(2 * far, to_slot(0))
    encode(2 * far + 1, to_slot(1))

    fwd = []

    def forward(src, half):
        cp = hcopy(src, half, h_fwd.at[len(fwd)], mate)
        cp.start()
        fwd.append(cp)

    hwait(2 * left + c, 0)
    rel_r = hcopy(2 * left + c, 0, h_send.at[6], 2 * right + c)
    rel_r.start()
    forward(2 * left + c, 0)
    hwait(2 * right + c, 1)
    rel_l = hcopy(2 * right + c, 1, h_send.at[7], 2 * left + c)
    rel_l.start()
    forward(2 * right + c, 1)

    def unit(buf_i, i, s):
        return buf_i.at[i, s]

    def landing(src, i, s):
        return qall.at[i, s, pl.ds(pl.multiple_of(src * rows, rows), rows)]

    def whole(src, i):
        return qall.at[i, :, pl.ds(pl.multiple_of(src * rows, rows), rows)]

    def direct(slot, i, who):
        return remote(
            scode.at[slot, i], whole(k, i),
            q_send.at[slot * units + i * SEGS], q_recv.at[k * units + i * SEGS], who,
        )

    def core_of(way):
        return c if way == 0 else 1 - c

    def out_far(way, v):
        i, s, cc = v // SEGS, v % SEGS, core_of(way)
        who = 2 * (right if way == 0 else left) + c
        return remote(
            unit(scode.at[cc], i, s), rbuf.at[way, v],
            q_send.at[cc * units + i * SEGS + s], r_recv.at[way * units + v], who,
        )

    def relay(way, v):
        i, s, cc = v // SEGS, v % SEGS, core_of(way)
        src = 2 * (left if way == 0 else right) + c
        who = 2 * (right if way == 0 else left) + cc
        return remote(
            rbuf.at[way, v], landing(src, i, s),
            r_send.at[way * units + v], q_recv.at[src * units + i * SEGS + s], who,
        )

    def send_far(v):
        out_far(0, v).start()
        out_far(1, v).start()

    def send_near(i, cc):
        direct(2 + cc, i, 2 * right + cc).start()
        direct(4 + cc, i, 2 * left + cc).start()

    def pass_on(v):
        for way in range(2):
            out_far(way, v).wait_recv()
            relay(way, v).start()

    encode(2 * right, to_slot(2))
    encode(2 * right + 1, to_slot(3))
    encode(2 * left, to_slot(4))
    encode(2 * left + 1, to_slot(5))

    hwait(2 * left + c, 1)
    forward(2 * left + c, 1)
    hwait(2 * right + c, 0)
    forward(2 * right + c, 0)

    def first_far(v, _):
        send_far(v)
        return 0

    lax.fori_loop(0, SEGS, first_far, 0)
    send_near(0, c)
    encode(mate, to_slot(6))
    encode(k, to_self)

    for i in range(drafts):
        direct(6, i, mate).start()

    hwait(2 * far + c, 0)
    forward(2 * far + c, 0)
    hwait(2 * far + c, 1)
    forward(2 * far + c, 1)
    for chip in (x, left, right, far):
        for half in range(2):
            hwait(2 * chip + 1 - c, half)

    def step(t, top):
        slot = t % 2

        @pl.when((t >= 2) & (t < 4))
        def _():
            for e in range(SEGS // 2):
                pass_on((SEGS // 2) * (t - 2) + e)

        @pl.when((t >= 4) & (t < 6))
        def _():
            for e in range(SEGS // 2):
                send_far(SEGS + (SEGS // 2) * (t - 4) + e)

        pl.when(t == 1)(lambda: send_near(0, 1 - c))
        pl.when(t == 6)(lambda: send_near(1, c))
        pl.when(t == 8)(lambda: send_near(1, 1 - c))

        w_cp(t, slot).wait()
        prod = INV_TEMP * lax.dot_general(
            wbuf[slot], hall[...].reshape(positions * batch, dim), (((1,), (1,)), ((), ())), preferred_element_type=F32
        )
        base = pl.multiple_of(off + t * wrows, 8)
        for i in range(positions):
            z[i, pl.ds(base, wrows), :] = prod[:, i * batch:(i + 1) * batch]

        @pl.when(t + 2 < STEPS)
        def _():
            w_cp(t + 2, slot).start()

        return jnp.maximum(top, jnp.max(prod.reshape(wrows // 8, 8, positions * batch), axis=0))

    top = lax.fori_loop(0, STEPS, step, jnp.full((8, positions * batch), -jnp.inf, F32))
    own_max = jnp.max(top, axis=0, keepdims=True)

    chunk = 160
    row_i = lax.broadcasted_iota(jnp.int32, (chunk, batch), 0)
    for i in range(positions):
        m_i = own_max[:, i * batch:(i + 1) * batch]
        want = tok_ref[i:i + 1, :] - k * vocab if i < drafts else None

        def expo(t, carry, i=i, m_i=m_i, want=want):
            total, got = carry
            at = pl.ds(pl.multiple_of(off + t * chunk, 8), chunk)
            e = jnp.exp(z[i, at, :] - m_i)
            z[i, at, :] = e
            total = total + jnp.sum(e.reshape(chunk // 8, 8, batch), axis=0)
            if want is not None:
                pick = jnp.where(row_i + t * chunk == want, e, 0.0)
                got = got + jnp.sum(pick.reshape(chunk // 8, 8, batch), axis=0)
            return total, got

        zero = jnp.zeros((8, batch), F32)
        total, got = lax.fori_loop(0, vocab // chunk, expo, (zero, zero))
        msgs[k, i:i + 1, :] = m_i
        msgs[k, 3 + i:4 + i, :] = jnp.sum(total, axis=0, keepdims=True)
        if i < drafts:
            msgs[k, 6 + i:7 + i, :] = jnp.sum(got, axis=0, keepdims=True)

    def msg(p, src):
        return remote(msgs.at[src], msgs.at[src], m_send.at[p], m_recv.at[src], (k + p) % n)

    for p in range(1, n):
        msg(p, k).start()

    for v in range(SEGS, 2 * SEGS):
        pass_on(v)
    for p in range(1, n):
        msg(p, (k + p) % n).wait_recv()

    allm = msgs[...]
    peak = jnp.max(allm[:, 0:3, :], axis=0)
    part = jnp.exp(allm[:, 0:3, :] - peak[None])
    inv = 1.0 / jnp.sum(part * allm[:, 3:6, :], axis=0)
    p_pick = jnp.sum(part[:, 0:drafts, :] * allm[:, 6:8, :], axis=0) * inv[0:drafts]
    q_pick = jnp.sum(allm[:, 8:10, :], axis=0)
    q_scale = jnp.sum(allm[:, 10:12, :], axis=0) * (1.0 / (TOP * TOP * TOP * TOP))
    fac = jnp.exp(msgs[k, 0:3, :] - peak) * inv

    def scale(t, _):
        at = pl.ds(pl.multiple_of(off + t * chunk, 8), chunk)
        z[drafts, at, :] = z[drafts, at, :] * fac[drafts:drafts + 1, :]
        return 0

    lax.fori_loop(0, vocab // chunk, scale, 0)

    def xmsg(p, i, src):
        return remote(mass.at[i, src], mass.at[i, src], x_send.at[i * n + p], x_recv.at[i * n + src], (k + p) % n)

    def drain_relay(v, _):
        relay(0, v).wait_send()
        relay(1, v).wait_send()
        return 0

    for i in range(drafts):
        acc = [jnp.zeros((8, LANES), F32) for _ in range(batch // LANES)]
        for src in (2 * left, 2 * left + 1, 2 * right, 2 * right + 1, mate):
            remote(whole(src, i), whole(src, i), q_send.at[0], q_recv.at[src * units + i * SEGS], mate).wait_recv()
        for s in range(SEGS):
            if i == drafts - 1 and s == SEGS - 1:
                for cp in own_sends + [rel_r, rel_l] + fwd:
                    cp.wait_send()
                for p in range(1, n):
                    msg(p, k).wait_send()
                for v in range(units):
                    for way in range(2):
                        out_far(way, v).wait_send()
                for slot in range(2, n - 1):
                    for ii in range(drafts):
                        direct(slot, ii, mate).wait_send()
            for src in (2 * far, 2 * far + 1):
                remote(
                    landing(src, i, s), landing(src, i, s), q_send.at[0],
                    q_recv.at[src * units + i * SEGS + s], mate,
                ).wait_recv()

            def body(t, acc, i=i, s=s):
                at = pl.ds(pl.multiple_of((s * (tiles // SEGS) + t) * LANES, LANES), LANES)
                out = []
                for h in range(batch // LANES):
                    ls = slice(h * LANES, (h + 1) * LANES)
                    code = qall[i, s, ls, pl.ds(pl.multiple_of(t * LANES, LANES), LANES)].astype(jnp.int32).astype(F32)
                    y = code.T + float(HALF)
                    y = y * y
                    qt = y * y * q_scale[i:i + 1, ls]
                    ex = jnp.maximum(z[i, at, ls] * fac[i:i + 1, ls] - qt, 0.0)
                    z[i, at, ls] = ex
                    out.append(acc[h] + jnp.sum(ex.reshape(LANES // 8, 8, LANES), axis=0))
                return tuple(out)

            acc = lax.fori_loop(0, tiles // SEGS, body, tuple(acc))
        for h in range(batch // LANES):
            mass[i, k, :, h * LANES:(h + 1) * LANES] = jnp.sum(acc[h], axis=0, keepdims=True)
        for p in range(1, n):
            xmsg(p, i, k).start()
    lax.fori_loop(0, units, drain_relay, 0)
    small_ref[...] = jnp.zeros(small_ref.shape, F32)
    small_ref[2:4, :] = p_pick
    small_ref[4:6, :] = q_pick
    for i in range(drafts):
        for p in range(1, n):
            xmsg(p, i, (k + p) % n).wait_recv()
        total = jnp.sum(mass[i], axis=0)
        small_ref[i:i + 1, :] = 1.0 / total

    for p in range(1, n):
        for i in range(drafts):
            xmsg(p, i, k).wait_send()


def finish(n, z, small, res_ref, bonus_ref, acc_out, exp_out, buf, acc_ref, exp_ref, sem):
    drafts, vocab, _ = res_ref.shape
    off = pl.multiple_of((lax.axis_index("tp") * vocab) % LANES, 8)
    part = vocab // PARTS
    last = pltpu.make_async_copy(z.at[drafts, pl.ds(off, vocab), :], bonus_ref, sem.at[0])
    last.start()
    copies = [last]
    accept = jnp.minimum(small[2:4, :] / small[4:6, :], 1.0)
    acc_ref[...] = accept
    exp_ref[...] = accept[0:1] + accept[0:1] * accept[1:2]
    for i in range(drafts):
        scale = small[i:i + 1, :]
        for t in range(PARTS):
            to = pl.ds(t * part, part)
            buf[i, to, :] = z[i, pl.ds(pl.multiple_of(off + t * part, 8), part), :] * scale
            cp = pltpu.make_async_copy(buf.at[i, to], res_ref.at[i, to], sem.at[len(copies)])
            cp.start()
            copies.append(cp)
        if i == 0:
            for src, dst in ((acc_ref, acc_out), (exp_ref, exp_out)):
                cp = pltpu.make_async_copy(src, dst, sem.at[len(copies)])
                cp.start()
                copies.append(cp)
    for cp in copies:
        cp.wait()


def solution(mesh):
    n = mesh.shape["tp"]

    def local(hid, w, q, tok):
        rows, positions, dim = hid.shape
        vocab = w.shape[1]
        drafts = positions - 1
        batch = rows * n
        q_tiles = q.shape[2] // LANES
        width = -(-vocab // LANES) * LANES
        q_view = q.reshape(rows, drafts, q_tiles, LANES).transpose(0, 2, 1, 3)
        q_view = with_layout_constraint(q_view, Layout((0, 1, 2, 3))).reshape(-1, LANES)
        dma = pltpu.SemaphoreType.DMA
        vmem, anywhere = pl.BlockSpec(memory_space=pltpu.VMEM), pl.BlockSpec(memory_space=pltpu.HBM)
        z, small = pl.pallas_call(
            functools.partial(kernel, n),
            out_shape=(
                jax.ShapeDtypeStruct((positions, width, batch), F32),
                jax.ShapeDtypeStruct((8, batch), F32),
            ),
            in_specs=[anywhere] * 4,
            out_specs=(vmem, vmem),
            scratch_shapes=[
                pltpu.VMEM((drafts, batch), jnp.int32),
                pltpu.VMEM((positions, batch, dim), jnp.bfloat16),
                pltpu.VMEM((rows * q_tiles * drafts, LANES), F32),
                pltpu.VMEM((n - 1, drafts, SEGS, rows, width // SEGS), jnp.int16),
                pltpu.VMEM((drafts, SEGS, batch, width // SEGS), jnp.int16),
                pltpu.VMEM((2, drafts * SEGS, rows, width // SEGS), jnp.int16),
                pltpu.VMEM((2, vocab // STEPS, dim), jnp.bfloat16),
                pltpu.VMEM((n, 16, batch), F32),
                pltpu.VMEM((drafts, n, 1, batch), F32),
                pltpu.VMEM((drafts * (rows // 8), 8, LANES), F32),
                dma((8,)), dma((8,)), dma((2 * n,)),
                dma((n * drafts * SEGS,)), dma((n * drafts * SEGS,)), dma((2 * drafts * SEGS,)), dma((2 * drafts * SEGS,)),
                dma((n,)), dma((n,)), dma((2 * n,)), dma((2 * n,)),
                dma((8,)), dma((2,)),
            ],
            compiler_params=pltpu.CompilerParams(
                collective_id=0, has_side_effects=True, vmem_limit_bytes=40 * 2**20
            ),
        )(*[pltpu.with_memory_space_constraint(a, pltpu.HBM) for a in (tok.T, hid.transpose(1, 0, 2), w.T, q_view)])
        residual, bonus, accept, expected = pl.pallas_call(
            functools.partial(finish, n),
            out_shape=(
                jax.ShapeDtypeStruct((drafts, vocab, batch), F32),
                jax.ShapeDtypeStruct((vocab, batch), F32),
                jax.ShapeDtypeStruct((drafts, batch), F32),
                jax.ShapeDtypeStruct((1, batch), F32),
            ),
            in_specs=[vmem, vmem],
            out_specs=(anywhere,) * 4,
            scratch_shapes=[
                pltpu.VMEM((drafts, vocab, batch), F32),
                pltpu.VMEM((drafts, batch), F32),
                pltpu.VMEM((1, batch), F32),
                dma(((drafts + 1) * PARTS + 2,)),
            ],
            compiler_params=pltpu.CompilerParams(vmem_limit_bytes=24 * 2**20),
        )(z, small)
        return accept.T, expected[0], residual.transpose(2, 0, 1), bonus.T

    return jax.shard_map(
        local,
        mesh=mesh,
        in_specs=(P(("dp", "tp"), None, None), P(None, "tp"), P(("dp", "tp"), None, None), P("dp", None)),
        out_specs=(P("dp", None), P("dp"), P("dp", None, "tp"), P("dp", "tp")),
        check_vma=False,
    )
```

```python
import functools

import jax
import jax.numpy as jnp
from jax import lax
from jax.experimental import pallas as pl
from jax.experimental.pallas import tpu as pltpu
from jax.experimental.layout import Layout, with_layout_constraint
from jax.sharding import PartitionSpec as P

INV_TEMP = 1.25
TOP = 65535.0
HALF = 32768
LANES = 128
SEGS = 2
STEPS = 10
PARTS = 5
F32 = jnp.float32
MESH = pl.DeviceIdType.MESH


def kernel(
    n, tok_in, hid_ref, w_ref, q_ref,
    z, small_ref,
    tok_ref, hall, stage, scode, qall, rbuf, wbuf, msgs, mass, rowc,
    h_send, h_fwd, h_recv, q_send, q_recv, r_send, r_recv,
    m_send, m_recv, x_send, x_recv, loc, wsem,
):
    k = lax.axis_index("tp")
    x, c = k // 2, k % 2
    chips = n // 2
    right, left = (x + 1) % chips, (x + chips - 1) % chips
    far = (x + 2) % chips
    mate = 2 * x + 1 - c
    positions, batch, dim = hall.shape
    drafts = positions - 1
    rows = batch // n
    vocab = w_ref.shape[0]
    seg = qall.shape[3]
    width = seg * SEGS
    tiles = width // LANES
    units = drafts * SEGS
    per = seg // LANES
    pitch = q_ref.shape[0] // rows
    all_tiles = pitch // drafts
    off = (k * vocab) % LANES
    hcol = dim // 2
    wrows = vocab // STEPS

    def remote(src, dst, ssem, rsem, who):
        return pltpu.make_async_remote_copy(
            src_ref=src, dst_ref=dst, send_sem=ssem, recv_sem=rsem,
            device_id={"tp": who}, device_id_type=MESH,
        )

    hid_cp = pltpu.make_async_copy(hid_ref, hall.at[:, pl.ds(k * rows, rows), :], loc.at[0])
    hid_cp.start()
    tok_cp = pltpu.make_async_copy(tok_in, tok_ref, loc.at[6])
    tok_cp.start()

    def stage_cp(g):
        part = pl.ds(g * 8 * pitch, 8 * pitch)
        return pltpu.make_async_copy(q_ref.at[part], stage.at[part], loc.at[1 + g])

    def w_cp(t, slot):
        return pltpu.make_async_copy(
            w_ref.at[pl.ds(pl.multiple_of(t * wrows, 8), wrows)], wbuf.at[slot], wsem.at[slot]
        )

    barrier = pltpu.get_barrier_semaphore()
    for who in (2 * right + c, 2 * left + c, mate):
        pl.semaphore_signal(barrier, inc=1, device_id={"tp": who}, device_id_type=MESH)
    pl.semaphore_wait(barrier, 3)

    def hpiece(src, half):
        return hall.at[:, pl.ds(pl.multiple_of(src * rows, rows), rows), pl.ds(half * hcol, hcol)]

    def hcopy(src, half, ssem, who):
        return remote(hpiece(src, half), hpiece(src, half), ssem, h_recv.at[src * 2 + half], who)

    def hwait(src, half):
        hcopy(src, half, h_send.at[0], mate).wait_recv()

    hid_cp.wait()
    own_sends = []
    for idx, (who, half) in enumerate(
        [(2 * right + c, 0), (2 * left + c, 1), (mate, 0), (mate, 1), (2 * right + c, 1), (2 * left + c, 0)]
    ):
        own_sends.append(hcopy(k, half, h_send.at[idx], who))
    for cp in own_sends[:4]:
        cp.start()
    for g in range(rows // 8):
        stage_cp(g).start()
    w_cp(0, 0).start()
    w_cp(1, 1).start()

    z[:, 0:96, :] = jnp.zeros((positions, 96, batch), F32)
    z[:, width - 96:width, :] = jnp.zeros((positions, 96, batch), F32)

    tok_cp.wait()
    for g in range(rows // 8):
        stage_cp(g).wait()

    def qrows(g, i, j):
        return stage[pl.ds(g * 8 * pitch + drafts * j + i, 8, stride=pitch), :]

    groups = [(i, g) for i in range(drafts) for g in range(rows // 8)]
    lane_b = lax.broadcasted_iota(jnp.int32, (8, batch), 1)
    sub_b = lax.broadcasted_iota(jnp.int32, (8, batch), 0)
    lane_t = lax.broadcasted_iota(jnp.int32, (8, LANES), 1)
    mine = [lane_b == k * rows + 8 * g + sub_b for g in range(rows // 8)]
    tok_col = []
    for i, g in groups:
        t = jnp.where(mine[g], jnp.broadcast_to(tok_ref[i:i + 1, :].astype(F32), (8, batch)), 0.0)
        tok_col.append(jnp.broadcast_to(jnp.sum(t, axis=1, keepdims=True), (8, LANES)).astype(jnp.int32))

    def scan(j, carry):
        top, got = carry
        new_top, new_got = [], []
        col = lane_t + j * LANES
        for a, (i, g) in enumerate(groups):
            v = qrows(g, i, j)
            new_top.append(jnp.maximum(top[a], v))
            new_got.append(jnp.where(col == tok_col[a], v, got[a]))
        return tuple(new_top), tuple(new_got)

    zero8 = tuple(jnp.zeros((8, LANES), F32) for _ in groups)
    top, got = lax.fori_loop(0, all_tiles, scan, (zero8, zero8))
    qtop_row, qgot_row = [], []
    for i in range(drafts):
        acc_t = jnp.zeros((8, batch), F32)
        acc_g = jnp.zeros((8, batch), F32)
        for a, (ii, g) in enumerate(groups):
            if ii != i:
                continue
            tcol = jnp.max(top[a], axis=1, keepdims=True)
            gcol = jnp.sum(got[a], axis=1, keepdims=True)
            rowc[a] = jnp.broadcast_to(jnp.log(TOP) - 0.25 * jnp.log(tcol), (8, LANES))
            acc_t = acc_t + jnp.where(mine[g], jnp.broadcast_to(tcol, (8, batch)), 0.0)
            acc_g = acc_g + jnp.where(mine[g], jnp.broadcast_to(gcol, (8, batch)), 0.0)
        qtop_row.append(jnp.sum(acc_t, axis=0, keepdims=True))
        qgot_row.append(jnp.sum(acc_g, axis=0, keepdims=True))
    msgs[k] = jnp.zeros(msgs.shape[1:], F32)
    for i in range(drafts):
        msgs[k, 8 + i:9 + i, :] = qgot_row[i]
        msgs[k, 10 + i:11 + i, :] = qtop_row[i]

    def encode(dest, put):
        first = (dest * vocab) // LANES

        def body(j, _):
            for i in range(drafts):
                for gg in range(rows // 16):
                    parts = []
                    for g in (2 * gg, 2 * gg + 1):
                        v = qrows(g, i, first + j)
                        y = jnp.exp(0.25 * jnp.log(v) + rowc[i * (rows // 8) + g])
                        parts.append((y + 0.5).astype(jnp.int32) - HALF)
                    code = jnp.concatenate(parts, axis=0).astype(jnp.int16)
                    put(i, gg, j // per, pl.ds(pl.multiple_of((j % per) * LANES, LANES), LANES), code)
            return 0

        lax.fori_loop(0, tiles, body, 0)

    def to_slot(r):
        def put(i, gg, s, cols, code):
            scode[r, i, s, 16 * gg:16 * gg + 16, cols] = code

        return put

    def to_self(i, gg, s, cols, code):
        qall[i, s, pl.ds(pl.multiple_of(k * rows + 16 * gg, 16), 16), cols] = code

    encode(2 * far, to_slot(0))
    encode(2 * far + 1, to_slot(1))

    fwd = []

    def forward(src, half):
        cp = hcopy(src, half, h_fwd.at[len(fwd)], mate)
        cp.start()
        fwd.append(cp)

    for way in range(2):
        own_sends[way].wait_send()
        own_sends[4 + way].start()
    hwait(2 * left + c, 0)
    rel_r = hcopy(2 * left + c, 0, h_send.at[6], 2 * right + c)
    rel_r.start()
    forward(2 * left + c, 0)
    hwait(2 * right + c, 1)
    rel_l = hcopy(2 * right + c, 1, h_send.at[7], 2 * left + c)
    rel_l.start()
    forward(2 * right + c, 1)

    def unit(buf_i, i, s):
        return buf_i.at[i, s]

    def landing(src, i, s):
        return qall.at[i, s, pl.ds(pl.multiple_of(src * rows, rows), rows)]

    def whole(src, i):
        return qall.at[i, :, pl.ds(pl.multiple_of(src * rows, rows), rows)]

    def direct(slot, i, who):
        return remote(
            scode.at[slot, i], whole(k, i),
            q_send.at[slot * units + i * SEGS], q_recv.at[k * units + i * SEGS], who,
        )

    def core_of(way):
        return c if way == 0 else 1 - c

    def out_far(way, v):
        i, s, cc = v // SEGS, v % SEGS, core_of(way)
        who = 2 * (right if way == 0 else left) + c
        return remote(
            unit(scode.at[cc], i, s), rbuf.at[way, v],
            q_send.at[cc * units + i * SEGS + s], r_recv.at[way * units + v], who,
        )

    def relay(way, v):
        i, s, cc = v // SEGS, v % SEGS, core_of(way)
        src = 2 * (left if way == 0 else right) + c
        who = 2 * (right if way == 0 else left) + cc
        return remote(
            rbuf.at[way, v], landing(src, i, s),
            r_send.at[way * units + v], q_recv.at[src * units + i * SEGS + s], who,
        )

    def send_far(v):
        out_far(0, v).start()
        out_far(1, v).start()

    def send_near(i, cc):
        direct(2 + cc, i, 2 * right + cc).start()
        direct(4 + cc, i, 2 * left + cc).start()

    def pass_on(v):
        for way in range(2):
            out_far(way, v).wait_recv()
            relay(way, v).start()

    encode(2 * right, to_slot(2))
    encode(2 * right + 1, to_slot(3))
    encode(2 * left, to_slot(4))
    encode(2 * left + 1, to_slot(5))

    hwait(2 * left + c, 1)
    forward(2 * left + c, 1)
    hwait(2 * right + c, 0)
    forward(2 * right + c, 0)

    def first_far(v, _):
        send_far(v)
        return 0

    lax.fori_loop(0, SEGS, first_far, 0)
    send_near(0, c)
    encode(mate, to_slot(6))
    encode(k, to_self)

    for i in range(drafts):
        direct(6, i, mate).start()

    hwait(2 * far + c, 0)
    forward(2 * far + c, 0)
    hwait(2 * far + c, 1)
    forward(2 * far + c, 1)
    for chip in (x, left, right, far):
        for half in range(2):
            hwait(2 * chip + 1 - c, half)

    def step(t, top):
        slot = t % 2

        @pl.when((t >= 2) & (t < 4))
        def _():
            for e in range(SEGS // 2):
                pass_on((SEGS // 2) * (t - 2) + e)

        @pl.when((t >= 4) & (t < 6))
        def _():
            for e in range(SEGS // 2):
                send_far(SEGS + (SEGS // 2) * (t - 4) + e)

        pl.when(t == 1)(lambda: send_near(0, 1 - c))
        pl.when(t == 6)(lambda: send_near(1, c))
        pl.when(t == 8)(lambda: send_near(1, 1 - c))

        w_cp(t, slot).wait()
        prod = INV_TEMP * lax.dot_general(
            wbuf[slot], hall[...].reshape(positions * batch, dim), (((1,), (1,)), ((), ())), preferred_element_type=F32
        )
        base = pl.multiple_of(off + t * wrows, 8)
        for i in range(positions):
            z[i, pl.ds(base, wrows), :] = prod[:, i * batch:(i + 1) * batch]

        @pl.when(t + 2 < STEPS)
        def _():
            w_cp(t + 2, slot).start()

        return jnp.maximum(top, jnp.max(prod.reshape(wrows // 8, 8, positions * batch), axis=0))

    top = lax.fori_loop(0, STEPS, step, jnp.full((8, positions * batch), -jnp.inf, F32))
    own_max = jnp.max(top, axis=0, keepdims=True)

    chunk = 160
    row_i = lax.broadcasted_iota(jnp.int32, (chunk, batch), 0)
    for i in range(positions):
        m_i = own_max[:, i * batch:(i + 1) * batch]
        want = tok_ref[i:i + 1, :] - k * vocab if i < drafts else None

        def expo(t, carry, i=i, m_i=m_i, want=want):
            total, got = carry
            at = pl.ds(pl.multiple_of(off + t * chunk, 8), chunk)
            e = jnp.exp(z[i, at, :] - m_i)
            z[i, at, :] = e
            total = total + jnp.sum(e.reshape(chunk // 8, 8, batch), axis=0)
            if want is not None:
                pick = jnp.where(row_i + t * chunk == want, e, 0.0)
                got = got + jnp.sum(pick.reshape(chunk // 8, 8, batch), axis=0)
            return total, got

        zero = jnp.zeros((8, batch), F32)
        total, got = lax.fori_loop(0, vocab // chunk, expo, (zero, zero))
        msgs[k, i:i + 1, :] = m_i
        msgs[k, 3 + i:4 + i, :] = jnp.sum(total, axis=0, keepdims=True)
        if i < drafts:
            msgs[k, 6 + i:7 + i, :] = jnp.sum(got, axis=0, keepdims=True)

    def msg(p, src):
        return remote(msgs.at[src], msgs.at[src], m_send.at[p], m_recv.at[src], (k + p) % n)

    for p in range(1, n):
        msg(p, k).start()

    for v in range(SEGS, 2 * SEGS):
        pass_on(v)
    for p in range(1, n):
        msg(p, (k + p) % n).wait_recv()

    allm = msgs[...]
    peak = jnp.max(allm[:, 0:3, :], axis=0)
    part = jnp.exp(allm[:, 0:3, :] - peak[None])
    inv = 1.0 / jnp.sum(part * allm[:, 3:6, :], axis=0)
    p_pick = jnp.sum(part[:, 0:drafts, :] * allm[:, 6:8, :], axis=0) * inv[0:drafts]
    q_pick = jnp.sum(allm[:, 8:10, :], axis=0)
    q_scale = jnp.sum(allm[:, 10:12, :], axis=0) * (1.0 / (TOP * TOP * TOP * TOP))
    fac = jnp.exp(msgs[k, 0:3, :] - peak) * inv

    def scale(t, _):
        at = pl.ds(pl.multiple_of(off + t * chunk, 8), chunk)
        z[drafts, at, :] = z[drafts, at, :] * fac[drafts:drafts + 1, :]
        return 0

    lax.fori_loop(0, vocab // chunk, scale, 0)

    def xmsg(p, i, src):
        return remote(mass.at[i, src], mass.at[i, src], x_send.at[i * n + p], x_recv.at[i * n + src], (k + p) % n)

    def drain_relay(v, _):
        relay(0, v).wait_send()
        relay(1, v).wait_send()
        return 0

    for i in range(drafts):
        acc = [jnp.zeros((8, LANES), F32) for _ in range(batch // LANES)]
        for src in (2 * left, 2 * left + 1, 2 * right, 2 * right + 1, mate):
            remote(whole(src, i), whole(src, i), q_send.at[0], q_recv.at[src * units + i * SEGS], mate).wait_recv()
        for s in range(SEGS):
            if i == drafts - 1 and s == SEGS - 1:
                for cp in own_sends[2:] + [rel_r, rel_l] + fwd:
                    cp.wait_send()
                for p in range(1, n):
                    msg(p, k).wait_send()
                for v in range(units):
                    for way in range(2):
                        out_far(way, v).wait_send()
                for slot in range(2, n - 1):
                    for ii in range(drafts):
                        direct(slot, ii, mate).wait_send()
            for src in (2 * far, 2 * far + 1):
                remote(
                    landing(src, i, s), landing(src, i, s), q_send.at[0],
                    q_recv.at[src * units + i * SEGS + s], mate,
                ).wait_recv()

            def body(t, acc, i=i, s=s):
                at = pl.ds(pl.multiple_of((s * (tiles // SEGS) + t) * LANES, LANES), LANES)
                out = []
                for h in range(batch // LANES):
                    ls = slice(h * LANES, (h + 1) * LANES)
                    code = qall[i, s, ls, pl.ds(pl.multiple_of(t * LANES, LANES), LANES)].astype(jnp.int32).astype(F32)
                    y = code.T + float(HALF)
                    y = y * y
                    qt = y * y * q_scale[i:i + 1, ls]
                    ex = jnp.maximum(z[i, at, ls] * fac[i:i + 1, ls] - qt, 0.0)
                    z[i, at, ls] = ex
                    out.append(acc[h] + jnp.sum(ex.reshape(LANES // 8, 8, LANES), axis=0))
                return tuple(out)

            acc = lax.fori_loop(0, tiles // SEGS, body, tuple(acc))
        for h in range(batch // LANES):
            mass[i, k, :, h * LANES:(h + 1) * LANES] = jnp.sum(acc[h], axis=0, keepdims=True)
        for p in range(1, n):
            xmsg(p, i, k).start()
    lax.fori_loop(0, units, drain_relay, 0)
    small_ref[...] = jnp.zeros(small_ref.shape, F32)
    small_ref[2:4, :] = p_pick
    small_ref[4:6, :] = q_pick
    for i in range(drafts):
        for p in range(1, n):
            xmsg(p, i, (k + p) % n).wait_recv()
        total = jnp.sum(mass[i], axis=0)
        small_ref[i:i + 1, :] = 1.0 / total

    for p in range(1, n):
        for i in range(drafts):
            xmsg(p, i, k).wait_send()


def finish(n, z, small, res_ref, bonus_ref, acc_out, exp_out, buf, acc_ref, exp_ref, sem):
    drafts, vocab, _ = res_ref.shape
    off = pl.multiple_of((lax.axis_index("tp") * vocab) % LANES, 8)
    part = vocab // PARTS
    last = pltpu.make_async_copy(z.at[drafts, pl.ds(off, vocab), :], bonus_ref, sem.at[0])
    last.start()
    copies = [last]
    accept = jnp.minimum(small[2:4, :] / small[4:6, :], 1.0)
    acc_ref[...] = accept
    exp_ref[...] = accept[0:1] + accept[0:1] * accept[1:2]
    for i in range(drafts):
        scale = small[i:i + 1, :]
        for t in range(PARTS):
            to = pl.ds(t * part, part)
            buf[i, to, :] = z[i, pl.ds(pl.multiple_of(off + t * part, 8), part), :] * scale
            cp = pltpu.make_async_copy(buf.at[i, to], res_ref.at[i, to], sem.at[len(copies)])
            cp.start()
            copies.append(cp)
        if i == 0:
            for src, dst in ((acc_ref, acc_out), (exp_ref, exp_out)):
                cp = pltpu.make_async_copy(src, dst, sem.at[len(copies)])
                cp.start()
                copies.append(cp)
    for cp in copies:
        cp.wait()


def solution(mesh):
    n = mesh.shape["tp"]

    def local(hid, w, q, tok):
        rows, positions, dim = hid.shape
        vocab = w.shape[1]
        drafts = positions - 1
        batch = rows * n
        q_tiles = q.shape[2] // LANES
        width = -(-vocab // LANES) * LANES
        q_view = q.reshape(rows, drafts, q_tiles, LANES).transpose(0, 2, 1, 3)
        q_view = with_layout_constraint(q_view, Layout((0, 1, 2, 3))).reshape(-1, LANES)
        dma = pltpu.SemaphoreType.DMA
        vmem, anywhere = pl.BlockSpec(memory_space=pltpu.VMEM), pl.BlockSpec(memory_space=pltpu.HBM)
        z, small = pl.pallas_call(
            functools.partial(kernel, n),
            out_shape=(
                jax.ShapeDtypeStruct((positions, width, batch), F32),
                jax.ShapeDtypeStruct((8, batch), F32),
            ),
            in_specs=[anywhere] * 4,
            out_specs=(vmem, vmem),
            scratch_shapes=[
                pltpu.VMEM((drafts, batch), jnp.int32),
                pltpu.VMEM((positions, batch, dim), jnp.bfloat16),
                pltpu.VMEM((rows * q_tiles * drafts, LANES), F32),
                pltpu.VMEM((n - 1, drafts, SEGS, rows, width // SEGS), jnp.int16),
                pltpu.VMEM((drafts, SEGS, batch, width // SEGS), jnp.int16),
                pltpu.VMEM((2, drafts * SEGS, rows, width // SEGS), jnp.int16),
                pltpu.VMEM((2, vocab // STEPS, dim), jnp.bfloat16),
                pltpu.VMEM((n, 16, batch), F32),
                pltpu.VMEM((drafts, n, 1, batch), F32),
                pltpu.VMEM((drafts * (rows // 8), 8, LANES), F32),
                dma((8,)), dma((8,)), dma((2 * n,)),
                dma((n * drafts * SEGS,)), dma((n * drafts * SEGS,)), dma((2 * drafts * SEGS,)), dma((2 * drafts * SEGS,)),
                dma((n,)), dma((n,)), dma((2 * n,)), dma((2 * n,)),
                dma((8,)), dma((2,)),
            ],
            compiler_params=pltpu.CompilerParams(
                collective_id=0, has_side_effects=True, vmem_limit_bytes=40 * 2**20
            ),
        )(*[pltpu.with_memory_space_constraint(a, pltpu.HBM) for a in (tok.T, hid.transpose(1, 0, 2), w.T, q_view)])
        residual, bonus, accept, expected = pl.pallas_call(
            functools.partial(finish, n),
            out_shape=(
                jax.ShapeDtypeStruct((drafts, vocab, batch), F32),
                jax.ShapeDtypeStruct((vocab, batch), F32),
                jax.ShapeDtypeStruct((drafts, batch), F32),
                jax.ShapeDtypeStruct((1, batch), F32),
            ),
            in_specs=[vmem, vmem],
            out_specs=(anywhere,) * 4,
            scratch_shapes=[
                pltpu.VMEM((drafts, vocab, batch), F32),
                pltpu.VMEM((drafts, batch), F32),
                pltpu.VMEM((1, batch), F32),
                dma(((drafts + 1) * PARTS + 2,)),
            ],
            compiler_params=pltpu.CompilerParams(vmem_limit_bytes=24 * 2**20),
        )(z, small)
        return accept.T, expected[0], residual.transpose(2, 0, 1), bonus.T

    return jax.shard_map(
        local,
        mesh=mesh,
        in_specs=(P(("dp", "tp"), None, None), P(None, "tp"), P(("dp", "tp"), None, None), P("dp", None)),
        out_specs=(P("dp", None), P("dp"), P("dp", None, "tp"), P("dp", "tp")),
        check_vma=False,
    )
```
